128 devices in a mesh: seq: 32 (over x, z, core), mp: 4 (over y).
Axes of the slice: x: 4, y: 4, z: 4, core: 2. Of those that a mesh axis runs over, the one named last changes fastest.
Arguments:
- layer_in: bfloat16 [24576, 2560], P('seq'), may hold values from -6 to 6
- ssm_input: bfloat16 [24576, 5120], P('seq', 'mp'), may hold values from -6 to 6
- b_matrix: bfloat16 [24576, 128], P('seq'), may hold values from -1.796875 to 1.796875
- c_matrix: bfloat16 [24576, 128], P('seq'), may hold values from -1.796875 to 1.796875
- dt_raw: float32 [24576, 80], P('seq', 'mp'), may hold values from -2.8 to 2.8
- dt_bias: float32 [80], P('mp'), may hold values from -7 to 0
- a_log: float32 [80], P('mp'), may hold values from -8 to 3
- d_skip: float32 [80], P('mp'), may hold values from 0.5 to 1.5
- grad_out: bfloat16 [24576, 5120], P('seq', 'mp'), may hold values from -1 to 1
Outputs:
- grad_wx: float32 [2560, 5120], P('seq', 'mp')
- grad_wbc: float32 [2560, 256], P('seq', 'mp')
- grad_alog: float32 [80], P('mp')
- grad_dtbias: float32 [80], P('mp')
- grad_dskip: float32 [80], P('mp')
The draws below stay inside these ranges and needn't reach their ends.
All inputs are finite; a program needn't handle non-finite values.
Results may differ from the reference program's by a relative error of at most 0.0063.
Values sent between devices are 32-bit elements; how exact they have to be, the bound alone decides.
A program may use at most 192 MiB of HBM per device.

```python
import math
from functools import partial
import jax
import jax.numpy as jnp
from jax import lax

D = 2560
HEADS = 80
HEAD_DIM = 64
STATE = 128
GROUP = 256
TOK_DEV = 768
TOKENS = 24576
N_SEQ = 32


def draw_dt_bias(key, part):
    centre = -0.5 * jnp.log(jnp.float32(TOKENS))
    offset = jax.random.uniform(key, (HEADS,), jnp.float32, -0.5, 0.5)
    return centre + offset


def draw_a_log(key, part):
    key_pick = jax.random.fold_in(key, 11)
    key_slow = jax.random.fold_in(key, 12)
    key_fast = jax.random.fold_in(key, 13)
    seq_root = jnp.sqrt(jnp.float32(TOKENS))
    is_slow = jax.random.bernoulli(key_pick, 0.5, (HEADS,))
    slow_rate = jnp.exp(jax.random.uniform(key_slow, (HEADS,), jnp.float32, math.log(0.15), 0.0)) / seq_root
    fast_rate = seq_root / (1.28 * jax.random.uniform(key_fast, (HEADS,), jnp.float32, 30.0, 50.0))
    return jnp.log(jnp.where(is_slow, slow_rate, fast_rate))


def draw_grad_out(key, part):
    key_main = jax.random.fold_in(key, 21)
    row_width = HEADS * HEAD_DIM
    position = jnp.arange(TOKENS, dtype=jnp.float32)[:, None]
    ramp_scale = (0.5 + 1.5 * position / TOKENS) / jnp.sqrt(jnp.float32(TOKENS))
    noise_field = jnp.clip(jax.random.normal(key_main, (TOKENS, row_width), jnp.float32), -4.0, 4.0)
    return (noise_field * ramp_scale).astype(jnp.bfloat16)


def level_of(stream_key, dims, cuts, low, top_value):
    def one(axis_at, shards_of):
        heights = jax.random.uniform(jax.random.fold_in(jax.random.fold_in(stream_key, 6), axis_at), (shards_of,), jnp.float32, low / len(cuts), top_value / len(cuts))
        return jnp.repeat(jnp.exp(heights), dims[axis_at] // shards_of).reshape((-1,) + (1,) * (len(dims) - axis_at - 1))

    gain = one(*cuts[0])
    for cut in cuts[1:]:
        gain = gain * one(*cut)
    return gain


def bell_draw(rng, extent, width, bound, split=(), held_as=jnp.bfloat16):
    values = jax.random.normal(rng, extent, jnp.float32) * width
    if len(split) > 0:
        values = level_of(rng, extent, split, -0.22, 0.18) * values
    return jnp.clip(values, min=-bound, max=bound).astype(held_as)


def setup_inputs(seed: int = 0) -> dict:
    splits = jax.random.split(jax.random.key(seed), 10)
    return {
        "layer_in": bell_draw(splits[0], (TOKENS, D), 1.0, 6.0, ((0, 32),)),
        "ssm_input": bell_draw(splits[1], (TOKENS, HEADS * HEAD_DIM), 1.0, 6.0, ((0, 32), (1, 4))),
        "b_matrix": bell_draw(splits[2], (TOKENS, STATE), 0.3, 1.796875, ((0, 32),)),
        "c_matrix": bell_draw(splits[3], (TOKENS, STATE), 0.3, 1.796875, ((0, 32),)),
        "dt_raw": bell_draw(splits[4], (TOKENS, HEADS), 0.7, 2.8, ((0, 32), (1, 4)), jnp.float32),
        "dt_bias": draw_dt_bias(jax.random.fold_in(splits[9], 71), 0),
        "a_log": draw_a_log(jax.random.fold_in(splits[9], 71), 0),
        "d_skip": jnp.clip(0.5 + 1.0 * jax.random.uniform(splits[7], (HEADS,), jnp.float32) ** level_of(splits[7], (HEADS,), ((0, 4),), -0.2, 0.2), 0.5, 1.5),
        "grad_out": draw_grad_out(jax.random.fold_in(splits[9], 71), 0),
    }


def contract(form, left, right):
    return jnp.einsum(form, left.astype(jnp.float32), right.astype(jnp.float32), precision=lax.Precision.HIGHEST)


def matmul(left, right):
    return jnp.dot(left, right, preferred_element_type=jnp.float32)


def inner_first(left, right):
    return jnp.dot(left.T, right, preferred_element_type=jnp.float32)


def inner_last(left, right):
    return jnp.dot(left, right.T, preferred_element_type=jnp.float32)


def reverse_sum(values):
    return jnp.flip(jnp.cumsum(jnp.flip(values, 0), axis=0), 0)


def exclusive_sum(values):
    return jnp.cumsum(values, axis=0) - values


def head_rates(dt_raw, dt_bias, a_log):
    shifted = dt_raw + dt_bias[None, :]
    dt_step = jax.nn.softplus(shifted)
    gate_slope = jax.nn.sigmoid(shifted)
    decay_rate = -jnp.exp(a_log)
    return dt_step, gate_slope, decay_rate, dt_step * decay_rate[None, :]


def block_states(ssm_input, grad_out, b_matrix, c_matrix, dt_step, log_step):
    tok_count, head_count = dt_step.shape
    head_dim = ssm_input.shape[1] // head_count
    state_width = b_matrix.shape[1]
    groups = tok_count // GROUP
    within = jnp.cumsum(log_step.reshape(groups, GROUP, head_count), axis=1)
    totals = within[:, -1, :]
    group_steps = dt_step.reshape(groups, GROUP, head_count)
    x_four = ssm_input.reshape(groups, GROUP, head_count, head_dim)
    dy_four = grad_out.reshape(groups, GROUP, head_count, head_dim)
    x_scaled = (x_four * (group_steps * jnp.exp(totals[:, None, :] - within))[..., None]).astype(jnp.bfloat16)
    y_scaled = (dy_four * jnp.exp(within)[..., None]).astype(jnp.bfloat16)
    b_three = b_matrix.reshape(groups, GROUP, state_width)
    c_three = c_matrix.reshape(groups, GROUP, state_width)
    state_parts = contract("kqhp,kqn->khpn", x_scaled, b_three)
    grad_parts = contract("kqhp,kqn->khpn", y_scaled, c_three)
    carry_state = jnp.zeros((head_count, head_dim, state_width), jnp.float32)
    starts = []
    for group_id in range(groups):
        starts.append(carry_state)
        carry_state = jnp.exp(totals[group_id])[:, None, None] * carry_state + state_parts[group_id]
    carry_grad = jnp.zeros((head_count, head_dim, state_width), jnp.float32)
    end_grads = [carry_grad] * groups
    for group_id in range(groups - 1, -1, -1):
        end_grads[group_id] = carry_grad
        carry_grad = grad_parts[group_id] + jnp.exp(totals[group_id])[:, None, None] * carry_grad
    cumulative = jnp.cumsum(log_step, axis=0)
    block_decay = jnp.exp(cumulative[-1])
    packed = (within, totals, x_scaled, y_scaled, jnp.stack(starts), jnp.stack(end_grads), cumulative)
    return block_decay, carry_state, carry_grad, packed


def one_group(d_skip, group_item):
    x_c, dy_c, b_c, c_c, dt_c, within_c, total_c, start_c, end_c, xw_c, yw_c = group_item
    size_q = x_c.shape[0]
    state_width = b_c.shape[1]
    cross_bc = inner_last(c_c, b_c)
    positions = jnp.arange(size_q)
    lower_mask = positions[:, None] >= positions[None, :]
    strict = positions[:, None] > positions[None, :]
    lagged = within_c.T[:, :, None] - within_c.T[:, None, :]
    decayed = jnp.where(lower_mask[None], jnp.exp(jnp.where(lower_mask[None], lagged, 0.0)), 0.0)
    mix_matrix = (cross_bc[None] * decayed).astype(jnp.bfloat16)
    gb_intra = contract("hrs,rhp->shp", mix_matrix, dy_c)
    paired = contract("rhp,shp->hrs", dy_c, x_c) * decayed
    paired_dt = paired * dt_c.T[:, None, :]
    mixed_sum = jnp.sum(paired_dt, axis=0).astype(jnp.bfloat16)
    box_terms = jnp.where(strict[None], cross_bc[None] * paired_dt, 0.0)
    box_flow = jnp.sum(box_terms, axis=1) - jnp.sum(box_terms, axis=2)
    da_intra = (jnp.cumsum(box_flow, axis=1) - box_flow).T
    start_low = start_c.astype(jnp.bfloat16)
    end_low = end_c.astype(jnp.bfloat16)
    y_start = contract("hpn,qn->qhp", start_low, c_c) * jnp.exp(within_c)[:, :, None]
    gb_end = contract("hpn,qn->qhp", end_low, b_c) * jnp.exp(total_c[None, :] - within_c)[:, :, None]
    gb_local = gb_intra + gb_end
    dx_local = (dt_c[:, :, None] * gb_local + d_skip[None, :, None] * dy_c).astype(jnp.bfloat16)
    x_wide = x_c.astype(jnp.float32)
    dy_wide = dy_c.astype(jnp.float32)
    x_gb = jnp.sum(x_wide * gb_local, axis=2)
    backward_part = jnp.sum(dy_wide * y_start, axis=2)
    forward_part = dt_c * jnp.sum(x_wide * gb_end, axis=2)
    meeting = jnp.exp(total_c) * jnp.sum(end_c * start_c, axis=(1, 2))
    da_local = da_intra + reverse_sum(backward_part) + exclusive_sum(forward_part) + meeting[None, :]
    dc_part = matmul(mixed_sum, b_c) + matmul(yw_c.reshape(size_q, -1), start_low.reshape(-1, state_width))
    db_part = inner_first(mixed_sum, c_c) + matmul(xw_c.reshape(size_q, -1), end_low.reshape(-1, state_width))
    return dx_local, jnp.concatenate([db_part, dc_part], axis=1), x_gb, da_local


def group_local(ssm_input, grad_out, b_matrix, c_matrix, dt_step, d_skip, packed):
    within, totals, x_scaled, y_scaled, starts, end_grads, cumulative = packed
    tok_count, head_count = dt_step.shape
    groups = within.shape[0]
    head_dim = ssm_input.shape[1] // head_count
    group_items = (ssm_input.reshape(groups, GROUP, head_count, head_dim),
                   grad_out.reshape(groups, GROUP, head_count, head_dim),
                   b_matrix.reshape(groups, GROUP, -1), c_matrix.reshape(groups, GROUP, -1),
                   dt_step.reshape(groups, GROUP, head_count), within, totals, starts, end_grads,
                   x_scaled, y_scaled)
    dx_local, dbc_local, x_gb, da_local = lax.map(partial(one_group, d_skip), group_items)
    return (dx_local.reshape(tok_count, -1), dbc_local.reshape(tok_count, -1),
            x_gb.reshape(tok_count, head_count), da_local.reshape(tok_count, head_count))


def device_terms(ssm_input, grad_out, b_matrix, c_matrix, dt_step, cumulative, state_in, grad_in):
    tok_count, head_count = dt_step.shape
    head_dim = ssm_input.shape[1] // head_count
    state_width = b_matrix.shape[1]
    block_end = cumulative[-1]
    state_low = state_in.astype(jnp.bfloat16)
    grad_low = grad_in.astype(jnp.bfloat16)
    rise_factor = jnp.exp(cumulative)
    fall_factor = jnp.exp(block_end[None, :] - cumulative)
    x_three = ssm_input.reshape(tok_count, head_count, head_dim)
    dy_three = grad_out.reshape(tok_count, head_count, head_dim)
    y_dev = contract("hpn,tn->thp", state_low, c_matrix) * rise_factor[:, :, None]
    gb_dev = contract("hpn,tn->thp", grad_low, b_matrix) * fall_factor[:, :, None]
    dx_carry = (dt_step[:, :, None] * gb_dev).astype(jnp.bfloat16).reshape(tok_count, -1)
    x_gb = jnp.sum(x_three.astype(jnp.float32) * gb_dev, axis=2)
    backward_part = jnp.sum(dy_three.astype(jnp.float32) * y_dev, axis=2)
    forward_part = dt_step * x_gb
    meeting = jnp.exp(block_end) * jnp.sum(grad_in * state_in, axis=(1, 2))
    da_dev = reverse_sum(backward_part) + exclusive_sum(forward_part) + meeting[None, :]
    y_rise = (dy_three * rise_factor[:, :, None]).astype(jnp.bfloat16).reshape(tok_count, -1)
    x_fall = (x_three * (dt_step * fall_factor)[:, :, None]).astype(jnp.bfloat16).reshape(tok_count, -1)
    dc_dev = matmul(y_rise, state_low.reshape(-1, state_width))
    db_dev = matmul(x_fall, grad_low.reshape(-1, state_width))
    return dx_carry, jnp.concatenate([db_dev, dc_dev], axis=1), x_gb, da_dev


def head_totals(ssm_input, grad_out, dt_step, gate_slope, decay_rate, x_gb, da_all):
    tok_count, head_count = dt_step.shape
    derivative = x_gb + decay_rate[None, :] * da_all
    skip_terms = jnp.sum((ssm_input.astype(jnp.float32) * grad_out.astype(jnp.float32)).reshape(tok_count, head_count, -1), axis=2)
    return jnp.sum(dt_step * da_all, axis=0), jnp.sum(gate_slope * derivative, axis=0), jnp.sum(skip_terms, axis=0)


def reference(layer_in, ssm_input, b_matrix, c_matrix, dt_raw, dt_bias, a_log, d_skip, grad_out):
    dt_step, gate_slope, decay_rate, log_step = head_rates(dt_raw, dt_bias, a_log)

    def block_piece(array, block_id):
        return lax.dynamic_slice_in_dim(array, (block_id * TOK_DEV).astype(jnp.int32), TOK_DEV, 0)

    def pieces(block_id):
        return tuple(block_piece(array, block_id) for array in (ssm_input, grad_out, b_matrix, c_matrix, dt_step, log_step))

    def summary(block_id):
        block_decay, block_state, block_grad, packed = block_states(*pieces(block_id))
        return block_decay, block_state, block_grad

    block_ids = jnp.arange(N_SEQ, dtype=jnp.int32)
    decays, states, grads = lax.map(summary, block_ids)

    def forward(running_state, entry):
        return entry[0][:, None, None] * running_state + entry[1], running_state

    def backward(running_state, entry):
        return entry[1] + entry[0][:, None, None] * running_state, running_state

    zero_state = jnp.zeros_like(states[0])
    final_state, states_in = lax.scan(forward, zero_state, (decays, states))
    first_grad, grads_in = lax.scan(backward, zero_state, (decays, grads), reverse=True)

    def accumulate(running, block_id):
        wx_total, wbc_total, rate_total, bias_total, skip_total = running
        x_blk, dy_blk, b_blk, c_blk, dt_blk, log_blk = pieces(block_id)
        block_decay, block_state, block_grad, packed = block_states(x_blk, dy_blk, b_blk, c_blk, dt_blk, log_blk)
        local_part = group_local(x_blk, dy_blk, b_blk, c_blk, dt_blk, d_skip, packed)
        carried = device_terms(x_blk, dy_blk, b_blk, c_blk, dt_blk, packed[6], states_in[block_id], grads_in[block_id])
        u_blk = block_piece(layer_in, block_id)
        wx_total = wx_total + (inner_first(u_blk, local_part[0]) + inner_first(u_blk, carried[0]))
        dbc_low = (local_part[1] + carried[1]).astype(jnp.bfloat16)
        wbc_total = wbc_total + inner_first(u_blk, dbc_low)
        slope_blk = block_piece(gate_slope, block_id)
        rate_part, bias_part, skip_part = head_totals(x_blk, dy_blk, dt_blk, slope_blk, decay_rate,
                                                      local_part[2] + carried[2], local_part[3] + carried[3])
        return (wx_total, wbc_total, rate_total + rate_part, bias_total + bias_part, skip_total + skip_part), None

    start = (jnp.zeros((D, HEADS * HEAD_DIM), jnp.float32), jnp.zeros((D, 2 * STATE), jnp.float32),
             jnp.zeros((HEADS,), jnp.float32), jnp.zeros((HEADS,), jnp.float32), jnp.zeros((HEADS,), jnp.float32))
    totals_out, unused = lax.scan(accumulate, start, block_ids)
    grad_wx, grad_wbc, rate_sum, bias_sum, skip_sum = totals_out
    return grad_wx, grad_wbc, decay_rate * rate_sum, bias_sum, skip_sum
```

```python
import functools
import math

import jax
import jax.numpy as jnp
from jax import lax
from jax.experimental import pallas as pl
from jax.experimental.pallas import tpu as pltpu
from jax.sharding import Mesh
from jax.sharding import PartitionSpec as P

GROUP = 256
HEAD_DIM = 64
STATE = 128
LOG2E = 1.0 / math.log(2.0)
SEQ = ("seq_0", "seq_1", "seq_2")
F32 = jnp.float32
BF16 = jnp.bfloat16
VMEM = pltpu.VMEM


def dot(left, right):
    return jnp.dot(left, right, preferred_element_type=F32)


def dot_nt(left, right):
    return lax.dot_general(left, right, (((1,), (1,)), ((), ())), preferred_element_type=F32)


def dot_tn(left, right):
    return lax.dot_general(left, right, (((0,), (0,)), ((), ())), preferred_element_type=F32)


def dot_exact(left, right):
    return jnp.dot(left, right, preferred_element_type=F32, precision=lax.Precision.HIGHEST)


def lane_iota(shape, dim):
    return lax.broadcasted_iota(jnp.int32, shape, dim)


def spread_matrix(heads, dtype):
    rows = lane_iota((heads, heads * HEAD_DIM), 0)
    cols = lane_iota((heads, heads * HEAD_DIM), 1)
    inside = (cols >= rows * HEAD_DIM) & (cols < (rows + 1) * HEAD_DIM)
    return jnp.where(inside, 1.0, 0.0).astype(dtype)


def gather_matrix(heads, dtype):
    rows = lane_iota((heads * HEAD_DIM, heads), 0)
    cols = lane_iota((heads * HEAD_DIM, heads), 1)
    inside = (rows >= cols * HEAD_DIM) & (rows < (cols + 1) * HEAD_DIM)
    return jnp.where(inside, 1.0, 0.0).astype(dtype)


def lower_ones(size):
    return jnp.where(lane_iota((size, size), 0) >= lane_iota((size, size), 1), 1.0, 0.0)


def spread(values, matrix):
    high = values.astype(BF16)
    low = (values - high.astype(F32)).astype(BF16)
    return dot(high, matrix) + dot(low, matrix)


def states_kernel(x_ref, dy_ref, b_ref, c_ref, dt_ref, a_ref, parts_ref, ends_ref, total_s, total_g):
    groups = x_ref.shape[0] // GROUP
    heads = dt_ref.shape[1]
    width = heads * HEAD_DIM
    tri = lower_ones(GROUP)
    spread_m = spread_matrix(heads, BF16)
    spread_e = spread_matrix(heads, F32)
    decays = []
    block_end = jnp.zeros((1, heads), F32)
    for g in range(groups):
        rows = slice(g * GROUP, (g + 1) * GROUP)
        within = dot_exact(tri, a_ref[rows, :])
        last = within[GROUP - 1 : GROUP, :]
        block_end = block_end + last
        decays.append(dot_exact(jnp.broadcast_to(jnp.exp(last), (8, heads)), spread_e)[0:1, :])
        fall = spread(dt_ref[rows, :] * jnp.exp(last - within), spread_m)
        xw = (x_ref[rows, :].astype(F32) * fall).astype(BF16)
        state = dot_tn(b_ref[rows, :], xw)
        rise = spread(jnp.exp(within), spread_m)
        yw = (dy_ref[rows, :].astype(F32) * rise).astype(BF16)
        grad = dot_tn(c_ref[rows, :], yw)
        if g < groups - 1:
            parts_ref[g] = state
        if g > 0:
            parts_ref[groups - 2 + g] = grad
        if g == 0:
            total_s[...] = state
            total_g[...] = grad
            gain = decays[0]
        else:
            total_s[...] = decays[g] * total_s[...] + state
            total_g[...] = total_g[...] + gain * grad
            gain = gain * decays[g]
    ends_ref[0:STATE, 0:width] = total_s[...]
    ends_ref[STATE : 2 * STATE, 0:width] = total_g[...]
    pad = jnp.concatenate([jnp.exp(block_end), jnp.zeros((1, 128 - heads), F32)], axis=1)
    ends_ref[:, width : width + 128] = jnp.broadcast_to(pad, (2 * STATE, 128))


def scan_kernel(half_ref, in_ref, out_ref, gain_ref):
    devices, rows, full = in_ref.shape
    width = full - 128
    heads = width // HEAD_DIM
    gains = in_ref[:, 0, width : width + 128][:, 0:heads]
    gain_ref[...] = dot_exact(gains, spread_matrix(heads, F32))
    backward = half_ref[0]

    def step(i, running):
        b = jnp.where(backward == 1, devices - 1 - i, i)
        out_ref[b] = running
        return gain_ref[pl.ds(b, 1), :] * running + in_ref[b, :, 0:width]

    lax.fori_loop(0, devices, step, jnp.zeros((rows, width), F32))


def intra_kernel(x_ref, dy_ref, b_ref, c_ref, dt_ref, slope_ref, a_ref, gi_ref, dbc_ref, stat_ref, v_ref, mix_ref):
    heads = dt_ref.shape[1]
    half = GROUP // 2
    tri = lower_ones(GROUP)
    dt = dt_ref[...]
    within = dot_exact(tri, a_ref[...])
    sums = dot_exact(tri, jnp.concatenate([dt, slope_ref[...]], axis=1))
    rise2 = within * LOG2E
    start2 = rise2 - jnp.log2(dt)
    rise_rows = jnp.transpose(rise2)
    sum_rows = jnp.transpose(sums)
    cross = dot_nt(b_ref[...], c_ref[...])
    v_ref[...] = jnp.zeros_like(v_ref)
    mix_ref[:, half:GROUP, 0:half] = jnp.zeros((2, half, half), BF16)
    strip = 64
    for pair in range(heads // 2):
        lanes = slice(pair * 128, (pair + 1) * 128)
        halves = []
        zs = []
        for sub in range(2):
            h = 2 * pair + sub
            cols = slice(h * HEAD_DIM, (h + 1) * HEAD_DIM)
            x_h = x_ref[:, cols]
            dy_h = dy_ref[:, cols]
            top = dot_nt(x_h[0:half], dy_h)
            low = dot_nt(x_h[half:GROUP], dy_h[half:GROUP])
            acc = [jnp.zeros((8, GROUP), F32) for _ in range(3)]
            z_strips = []
            for k in range(GROUP // strip):
                first = (k * strip // half) * half
                rows = slice(k * strip, (k + 1) * strip)
                wide = GROUP - first
                gap = rise_rows[h : h + 1, first:GROUP] - start2[rows, h : h + 1]
                reach = lane_iota((strip, wide), 1) + first >= lane_iota((strip, wide), 0) + k * strip
                decay = jnp.where(reach, jnp.exp2(gap), 0.0)
                bc = cross[rows, first:GROUP]
                mix_ref[sub, rows, first:GROUP] = (decay * bc).astype(BF16)
                pairs = top[rows, :] if first == 0 else low[k * strip - half : (k + 1) * strip - half, :]
                z = decay * pairs
                z_strips.append(z)
                box = z * bc
                w_dt = sums[rows, h : h + 1]
                w_sl = sums[rows, heads + h : heads + h + 1]
                for n, term in enumerate((box, box * w_dt, box * w_sl)):
                    part = jnp.sum(term.reshape(strip // 8, 8, wide), axis=0)
                    if first > 0:
                        acc[n] = jnp.concatenate([acc[n][:, 0:first], acc[n][:, first:GROUP] + part], axis=1)
                    else:
                        acc[n] = acc[n] + part
            zs.append(z_strips)
            halves.append(dot(mix_ref[sub], dy_h))
            flow_dt = acc[0] * sum_rows[h : h + 1, :] - acc[1]
            flow_sl = acc[0] * sum_rows[heads + h : heads + h + 1, :] - acc[2]
            stat_ref[0, h : h + 1, :] = jnp.sum(flow_dt, axis=0, keepdims=True)
            stat_ref[0, heads + h : heads + h + 1, :] = jnp.sum(flow_sl, axis=0, keepdims=True)
        for k in range(GROUP // strip):
            first = (k * strip // half) * half
            rows = slice(k * strip, (k + 1) * strip)
            v_ref[rows, first:GROUP] += zs[0][k] + zs[1][k]
        gi_ref[:, lanes] = jnp.concatenate(halves, axis=1).astype(BF16)
    mixed = v_ref[...].astype(BF16)
    dbc_ref[:, 0:STATE] = dot(mixed, c_ref[...])
    dbc_ref[:, STATE : 2 * STATE] = dot_tn(mixed, b_ref[...])


def final_kernel(x_ref, dy_ref, b_ref, c_ref, dt_ref, slope_ref, a_ref, skip_ref, rate_ref, gi_ref, dbc_ref,
                 flow_ref, parts_ref, carry_ref, dx_ref, dbc_out, stat_ref, sp_ref, gp_ref):
    heads = dt_ref.shape[1]
    groups = x_ref.shape[0] // GROUP
    tri = lower_ones(GROUP)
    spread_m = spread_matrix(heads, BF16)
    spread_e = spread_matrix(heads, F32)
    gather_m = gather_matrix(heads, BF16)
    gather_e = gather_matrix(heads, F32)
    rate = rate_ref[...]
    within, last, decays = [], [], []
    for g in range(groups):
        rows = slice(g * GROUP, (g + 1) * GROUP)
        within.append(dot_exact(tri, a_ref[rows, :]))
        last.append(within[g][GROUP - 1 : GROUP, :])
        decays.append(dot_exact(jnp.broadcast_to(jnp.exp(last[g]), (8, heads)), spread_e)[0:1, :])
    sp_ref[0] = carry_ref[0:STATE, :]
    gp_ref[groups - 1] = carry_ref[STATE : 2 * STATE, :]
    for g in range(groups - 1):
        sp_ref[g + 1] = decays[g] * sp_ref[g] + parts_ref[g]
    for g in range(groups - 1, 0, -1):
        gp_ref[g - 1] = parts_ref[groups - 2 + g] + decays[g] * gp_ref[g]
    flow_dt_all = jnp.zeros((1, heads), F32)
    flow_sl_all = jnp.zeros((1, heads), F32)
    bias_all = jnp.zeros((1, heads), F32)
    skip_all = jnp.zeros((1, heads), F32)
    for g in range(groups):
        rows = slice(g * GROUP, (g + 1) * GROUP)
        dt = dt_ref[rows, :]
        slope = slope_ref[rows, :]
        rise = jnp.exp(within[g])
        fall = dt * jnp.exp(last[g] - within[g])
        x = x_ref[rows, :].astype(F32)
        dy = dy_ref[rows, :].astype(F32)
        b = b_ref[rows, :]
        c = c_ref[rows, :]
        sp = sp_ref[g]
        gp = gp_ref[g]
        sp_low = sp.astype(BF16)
        gp_low = gp.astype(BF16)
        fall_wide = spread(fall, spread_m)
        xw = (x * fall_wide).astype(BF16)
        from_end = dot(b, gp_low)
        dx_raw = gi_ref[rows, :].astype(F32) + fall_wide * from_end
        dx_ref[rows, :] = (dx_raw + skip_ref[...] * dy).astype(BF16)
        x_gb = dot((x * dx_raw).astype(BF16), gather_m)
        fore = fall * dot((x * from_end).astype(BF16), gather_m)
        skips = dot((x * dy).astype(BF16), gather_m)
        rise_wide = spread(rise, spread_m)
        yw = (dy * rise_wide).astype(BF16)
        from_start = dot(c, sp_low)
        back = rise * dot((dy * from_start).astype(BF16), gather_m)
        dbc_out[rows, 0:STATE] = dbc_ref[rows, 0:STATE] + dot_nt(xw, gp_low)
        dbc_out[rows, STATE : 2 * STATE] = dbc_ref[rows, STATE : 2 * STATE] + dot_nt(yw, sp_low)
        sum_dt = dot_exact(tri, dt)
        sum_sl = dot_exact(tri, slope)
        all_dt = sum_dt[GROUP - 1 : GROUP, :]
        all_sl = sum_sl[GROUP - 1 : GROUP, :]
        inner = jnp.sum(sp * gp, axis=0, keepdims=True)
        meet = jnp.exp(last[g]) * dot_exact(jnp.broadcast_to(inner, (8, inner.shape[1])), gather_e)[0:1, :]
        flow_dt_all += jnp.sum(back * sum_dt + fore * (all_dt - sum_dt), axis=0, keepdims=True) + meet * all_dt
        flow_sl_all += jnp.sum(back * sum_sl + fore * (all_sl - sum_sl), axis=0, keepdims=True) + meet * all_sl
        bias_all += jnp.sum(slope / dt * x_gb, axis=0, keepdims=True)
        skip_all += jnp.sum(skips, axis=0, keepdims=True)
    intra = flow_ref[0]
    for g in range(1, groups):
        intra = intra + flow_ref[g]
    totals = jnp.transpose(jnp.sum(intra, axis=1, keepdims=True) + jnp.zeros((2 * heads, 128), F32))[0:1, :]
    flow_dt_all += totals[:, 0:heads]
    flow_sl_all += totals[:, heads : 2 * heads]
    stat_ref[...] = jnp.zeros_like(stat_ref)
    stat_ref[0:1, 0:heads] = rate * flow_dt_all
    stat_ref[1:2, 0:heads] = bias_all + rate * flow_sl_all
    stat_ref[2:3, 0:heads] = skip_all


def full(shape):
    return pl.BlockSpec(shape, lambda *_: (0,) * len(shape))


def by_group(width):
    return pl.BlockSpec((GROUP, width), lambda g: (g, 0))


def call(kernel, out, name, flops, nbytes, **options):
    params = pltpu.CompilerParams(vmem_limit_bytes=options.pop("vmem", 56 * 1024 * 1024))
    cost = pl.CostEstimate(flops=flops, bytes_accessed=nbytes, transcendentals=0)
    return pl.pallas_call(kernel, out_shape=out, name=name, cost_estimate=cost, compiler_params=params, **options)


def on_device(layer_in, ssm_input, b_matrix, c_matrix, dt_raw, dt_bias, a_log, d_skip, grad_out):
    tokens, heads = dt_raw.shape
    width = heads * HEAD_DIM
    groups = tokens // GROUP
    devices = math.prod(lax.axis_size(axis) for axis in SEQ)
    rows = 2 * STATE // devices
    shifted = dt_raw + dt_bias[None, :]
    dt = jax.nn.softplus(shifted)
    slope = jax.nn.sigmoid(shifted)
    rate = -jnp.exp(a_log)
    log_step = dt * rate[None, :]
    sds = jax.ShapeDtypeStruct

    parts, ends = call(
        states_kernel,
        (sds((2 * groups - 2, STATE, width), F32), sds((2 * STATE, width + 128), F32)),
        "block_states", 10**9, 10**7,
        scratch_shapes=[VMEM((STATE, width), F32), VMEM((STATE, width), F32)],
    )(ssm_input, grad_out, b_matrix, c_matrix, dt, log_step)

    sent = ends.reshape(devices, rows, width + 128)
    got = lax.all_to_all(sent, SEQ, split_axis=0, concat_axis=0, tiled=True)
    position = lax.axis_index(SEQ)
    backward = (position >= devices // 2).astype(jnp.int32).reshape(1)
    scanned = call(
        scan_kernel, sds((devices, rows, width), F32), "carry_scan", 10**8, 3 * 10**6,
        in_specs=[pl.BlockSpec(memory_space=pltpu.SMEM), full((devices, rows, width + 128))],
        out_specs=full((devices, rows, width)),
        grid=(1,),
        scratch_shapes=[VMEM((devices, width), F32)],
    )(backward, got)
    carry = lax.all_to_all(scanned, SEQ, split_axis=0, concat_axis=0, tiled=True).reshape(2 * STATE, width)

    gi, dbc_local, flows = call(
        intra_kernel,
        (sds((tokens, width), BF16), sds((tokens, 2 * STATE), F32), sds((groups, 2 * heads, GROUP), F32)),
        "intra", 3 * 10**10, 8 * 10**6,
        grid=(groups,),
        in_specs=[by_group(width), by_group(width), by_group(STATE), by_group(STATE),
                  by_group(heads), by_group(heads), by_group(heads)],
        out_specs=(by_group(width), by_group(2 * STATE), pl.BlockSpec((1, 2 * heads, GROUP), lambda g: (g, 0, 0))),
        scratch_shapes=[VMEM((GROUP, GROUP), F32), VMEM((2, GROUP, GROUP), BF16)],
    )(ssm_input, grad_out, b_matrix, c_matrix, dt, slope, log_step)

    skip_wide = jnp.repeat(d_skip, HEAD_DIM)[None, :]
    dx, dbc, stats = call(
        final_kernel,
        (sds((tokens, width), BF16), sds((tokens, 2 * STATE), F32), sds((8, 128), F32)),
        "combine", 2 * 10**9, 2 * 10**7,
        scratch_shapes=[VMEM((groups, STATE, width), F32), VMEM((groups, STATE, width), F32)],
    )(ssm_input, grad_out, b_matrix, c_matrix, dt, slope, log_step, skip_wide, rate[None, :], gi, dbc_local,
      flows, parts, carry)

    grad_wx = lax.psum_scatter(
        lax.dot_general(layer_in, dx, (((0,), (0,)), ((), ())), preferred_element_type=F32),
        SEQ, scatter_dimension=0, tiled=True,
    )
    owned = lax.psum_scatter(dbc, "mp", scatter_dimension=1, tiled=True).astype(BF16)
    partial = lax.dot_general(layer_in, owned, (((0,), (0,)), ((), ())), preferred_element_type=F32)
    blocks = partial.reshape(devices, -1, owned.shape[1])
    extra = stats.reshape(-1, owned.shape[1])
    extra = jnp.broadcast_to(extra[None], (devices, *extra.shape))
    arrived = lax.all_to_all(
        jnp.concatenate([blocks, extra], axis=1), SEQ, split_axis=0, concat_axis=0, tiled=True
    ).sum(axis=0)
    grad_wbc = arrived[: blocks.shape[1]]
    totals = arrived[blocks.shape[1] :].reshape(8, 128)
    return (grad_wx, grad_wbc, totals[0, :heads], totals[1, :heads], totals[2, :heads])


def solution(mesh):
    n_seq, n_mp = mesh.shape["seq"], mesh.shape["mp"]
    split = Mesh(mesh.devices.reshape(n_seq // 8, 4, 2, n_mp), SEQ + ("mp",))
    in_specs = (
        P(SEQ, None),
        P(SEQ, "mp"),
        P(SEQ, None),
        P(SEQ, None),
        P(SEQ, "mp"),
        P("mp"),
        P("mp"),
        P("mp"),
        P(SEQ, "mp"),
    )
    out_specs = (P(SEQ, "mp"), P(SEQ, "mp"), P("mp"), P("mp"), P("mp"))
    return jax.shard_map(
        on_device, mesh=split, in_specs=in_specs, out_specs=out_specs, check_vma=False
    )
```

```python
import functools
import math

import jax
import jax.numpy as jnp
from jax import lax
from jax.experimental import pallas as pl
from jax.experimental.pallas import tpu as pltpu
from jax.sharding import Mesh
from jax.sharding import PartitionSpec as P

GROUP = 256
HEAD_DIM = 64
STATE = 128
LOG2E = 1.0 / math.log(2.0)
SEQ = ("seq_0", "seq_1", "seq_2")
F32 = jnp.float32
BF16 = jnp.bfloat16
VMEM = pltpu.VMEM


def dot(left, right):
    return jnp.dot(left, right, preferred_element_type=F32)


def dot_nt(left, right):
    return lax.dot_general(left, right, (((1,), (1,)), ((), ())), preferred_element_type=F32)


def dot_tn(left, right):
    return lax.dot_general(left, right, (((0,), (0,)), ((), ())), preferred_element_type=F32)


def dot_exact(left, right):
    return jnp.dot(left, right, preferred_element_type=F32, precision=lax.Precision.HIGHEST)


def lane_iota(shape, dim):
    return lax.broadcasted_iota(jnp.int32, shape, dim)


def spread_matrix(heads, dtype):
    rows = lane_iota((heads, heads * HEAD_DIM), 0)
    cols = lane_iota((heads, heads * HEAD_DIM), 1)
    inside = (cols >= rows * HEAD_DIM) & (cols < (rows + 1) * HEAD_DIM)
    return jnp.where(inside, 1.0, 0.0).astype(dtype)


def gather_matrix(heads, dtype):
    rows = lane_iota((heads * HEAD_DIM, heads), 0)
    cols = lane_iota((heads * HEAD_DIM, heads), 1)
    inside = (rows >= cols * HEAD_DIM) & (rows < (cols + 1) * HEAD_DIM)
    return jnp.where(inside, 1.0, 0.0).astype(dtype)


def lower_ones(size):
    return jnp.where(lane_iota((size, size), 0) >= lane_iota((size, size), 1), 1.0, 0.0)


def spread(values, matrix):
    high = values.astype(BF16)
    low = (values - high.astype(F32)).astype(BF16)
    return dot(high, matrix) + dot(low, matrix)


def states_kernel(x_ref, dy_ref, b_ref, c_ref, dt_ref, a_ref, parts_ref, ends_ref, total_s, total_g):
    groups = x_ref.shape[0] // GROUP
    heads = dt_ref.shape[1]
    width = heads * HEAD_DIM
    tri = lower_ones(GROUP)
    spread_m = spread_matrix(heads, BF16)
    spread_e = spread_matrix(heads, F32)
    decays = []
    block_end = jnp.zeros((1, heads), F32)
    for g in range(groups):
        rows = slice(g * GROUP, (g + 1) * GROUP)
        within = dot_exact(tri, a_ref[rows, :])
        last = within[GROUP - 1 : GROUP, :]
        block_end = block_end + last
        decays.append(dot_exact(jnp.broadcast_to(jnp.exp(last), (8, heads)), spread_e)[0:1, :])
        fall = spread(dt_ref[rows, :] * jnp.exp(last - within), spread_m)
        xw = (x_ref[rows, :].astype(F32) * fall).astype(BF16)
        state = dot_tn(b_ref[rows, :], xw)
        rise = spread(jnp.exp(within), spread_m)
        yw = (dy_ref[rows, :].astype(F32) * rise).astype(BF16)
        grad = dot_tn(c_ref[rows, :], yw)
        if g < groups - 1:
            parts_ref[g] = state
        if g > 0:
            parts_ref[groups - 2 + g] = grad
        if g == 0:
            total_s[...] = state
            total_g[...] = grad
            gain = decays[0]
        else:
            total_s[...] = decays[g] * total_s[...] + state
            total_g[...] = total_g[...] + gain * grad
            gain = gain * decays[g]
    ends_ref[0:STATE, 0:width] = total_s[...]
    ends_ref[STATE : 2 * STATE, 0:width] = total_g[...]
    pad = jnp.concatenate([jnp.exp(block_end), jnp.zeros((1, 128 - heads), F32)], axis=1)
    ends_ref[:, width : width + 128] = jnp.broadcast_to(pad, (2 * STATE, 128))


def scan_kernel(half_ref, in_ref, out_ref, gain_ref):
    devices, rows, full = in_ref.shape
    width = full - 128
    heads = width // HEAD_DIM
    gains = in_ref[:, 0, width : width + 128][:, 0:heads]
    gain_ref[...] = dot_exact(gains, spread_matrix(heads, F32))
    backward = half_ref[0]

    def step(i, running):
        b = jnp.where(backward == 1, devices - 1 - i, i)
        out_ref[b] = running
        return gain_ref[pl.ds(b, 1), :] * running + in_ref[b, :, 0:width]

    lax.fori_loop(0, devices, step, jnp.zeros((rows, width), F32))


def intra_kernel(x_ref, dy_ref, b_ref, c_ref, dt_ref, slope_ref, a_ref, gi_ref, dbc_ref, stat_ref, v_ref, mix_ref):
    heads = dt_ref.shape[1]
    half = GROUP // 2
    tri = lower_ones(GROUP)
    dt = dt_ref[...]
    within = dot_exact(tri, a_ref[...])
    sums = dot_exact(tri, jnp.concatenate([dt, slope_ref[...]], axis=1))
    rise2 = within * LOG2E
    start2 = rise2 - jnp.log2(dt)
    rise_rows = jnp.transpose(rise2)
    sum_rows = jnp.transpose(sums)
    cross = dot_nt(b_ref[...], c_ref[...])
    v_ref[...] = jnp.zeros_like(v_ref)
    mix_ref[:, half:GROUP, 0:half] = jnp.zeros((2, half, half), BF16)
    strip = 64
    for pair in range(heads // 2):
        lanes = slice(pair * 128, (pair + 1) * 128)
        halves = []
        zs = []
        for sub in range(2):
            h = 2 * pair + sub
            cols = slice(h * HEAD_DIM, (h + 1) * HEAD_DIM)
            x_h = x_ref[:, cols]
            dy_h = dy_ref[:, cols]
            top = dot_nt(x_h[0:half], dy_h)
            low = dot_nt(x_h[half:GROUP], dy_h[half:GROUP])
            acc = [jnp.zeros((8, GROUP), F32) for _ in range(3)]
            z_strips = []
            for k in range(GROUP // strip):
                first = (k * strip // half) * half
                rows = slice(k * strip, (k + 1) * strip)
                wide = GROUP - first
                gap = rise_rows[h : h + 1, first:GROUP] - start2[rows, h : h + 1]
                reach = lane_iota((strip, wide), 1) + first >= lane_iota((strip, wide), 0) + k * strip
                decay = jnp.where(reach, jnp.exp2(gap), 0.0)
                bc = cross[rows, first:GROUP]
                mix_ref[sub, rows, first:GROUP] = (decay * bc).astype(BF16)
                pairs = top[rows, :] if first == 0 else low[k * strip - half : (k + 1) * strip - half, :]
                z = decay * pairs
                z_strips.append(z)
                box = z * bc
                w_dt = sums[rows, h : h + 1]
                w_sl = sums[rows, heads + h : heads + h + 1]
                for n, term in enumerate((box, box * w_dt, box * w_sl)):
                    part = jnp.sum(term.reshape(strip // 8, 8, wide), axis=0)
                    if first > 0:
                        acc[n] = jnp.concatenate([acc[n][:, 0:first], acc[n][:, first:GROUP] + part], axis=1)
                    else:
                        acc[n] = acc[n] + part
            zs.append(z_strips)
            halves.append(dot(mix_ref[sub], dy_h))
            flow_dt = acc[0] * sum_rows[h : h + 1, :] - acc[1]
            flow_sl = acc[0] * sum_rows[heads + h : heads + h + 1, :] - acc[2]
            stat_ref[0, h : h + 1, :] = jnp.sum(flow_dt, axis=0, keepdims=True)
            stat_ref[0, heads + h : heads + h + 1, :] = jnp.sum(flow_sl, axis=0, keepdims=True)
        for k in range(GROUP // strip):
            first = (k * strip // half) * half
            rows = slice(k * strip, (k + 1) * strip)
            v_ref[rows, first:GROUP] += zs[0][k] + zs[1][k]
        gi_ref[:, lanes] = jnp.concatenate(halves, axis=1).astype(BF16)
    mixed = v_ref[...].astype(BF16)
    dbc_ref[:, 0:STATE] = dot(mixed, c_ref[...])
    dbc_ref[:, STATE : 2 * STATE] = dot_tn(mixed, b_ref[...])


def final_kernel(x_ref, dy_ref, b_ref, c_ref, dt_ref, slope_ref, a_ref, skip_ref, rate_ref, gi_ref, dbc_ref,
                 flow_ref, parts_ref, carry_ref, dx_ref, dbc_out, stat_ref, sp_ref, gp_ref):
    heads = dt_ref.shape[1]
    groups = x_ref.shape[0] // GROUP
    tri = lower_ones(GROUP)
    spread_m = spread_matrix(heads, BF16)
    spread_e = spread_matrix(heads, F32)
    gather_m = gather_matrix(heads, BF16)
    gather_e = gather_matrix(heads, F32)
    rate = rate_ref[...]
    within, last, decays = [], [], []
    for g in range(groups):
        rows = slice(g * GROUP, (g + 1) * GROUP)
        within.append(dot_exact(tri, a_ref[rows, :]))
        last.append(within[g][GROUP - 1 : GROUP, :])
        decays.append(dot_exact(jnp.broadcast_to(jnp.exp(last[g]), (8, heads)), spread_e)[0:1, :])
    sp_ref[0] = carry_ref[0:STATE, :]
    gp_ref[groups - 1] = carry_ref[STATE : 2 * STATE, :]
    for g in range(groups - 1):
        sp_ref[g + 1] = decays[g] * sp_ref[g] + parts_ref[g]
    for g in range(groups - 1, 0, -1):
        gp_ref[g - 1] = parts_ref[groups - 2 + g] + decays[g] * gp_ref[g]
    flow_dt_all = jnp.zeros((1, heads), F32)
    flow_sl_all = jnp.zeros((1, heads), F32)
    bias_all = jnp.zeros((1, heads), F32)
    skip_all = jnp.zeros((1, heads), F32)
    for g in range(groups):
        rows = slice(g * GROUP, (g + 1) * GROUP)
        dt = dt_ref[rows, :]
        slope = slope_ref[rows, :]
        rise = jnp.exp(within[g])
        fall = dt * jnp.exp(last[g] - within[g])
        x = x_ref[rows, :].astype(F32)
        dy = dy_ref[rows, :].astype(F32)
        b = b_ref[rows, :]
        c = c_ref[rows, :]
        sp = sp_ref[g]
        gp = gp_ref[g]
        sp_low = sp.astype(BF16)
        gp_low = gp.astype(BF16)
        fall_wide = spread(fall, spread_m)
        xw = (x * fall_wide).astype(BF16)
        from_end = dot(b, gp_low)
        dx_raw = gi_ref[rows, :].astype(F32) + fall_wide * from_end
        dx_ref[rows, :] = (dx_raw + skip_ref[...] * dy).astype(BF16)
        x_gb = dot((x * dx_raw).astype(BF16), gather_m)
        fore = fall * dot((x * from_end).astype(BF16), gather_m)
        skips = dot((x * dy).astype(BF16), gather_m)
        rise_wide = spread(rise, spread_m)
        yw = (dy * rise_wide).astype(BF16)
        from_start = dot(c, sp_low)
        back = rise * dot((dy * from_start).astype(BF16), gather_m)
        grads = (dbc_ref[rows, 0:STATE] + dot_nt(xw, gp_low), dbc_ref[rows, STATE : 2 * STATE] + dot_nt(yw, sp_low))
        for piece in range(GROUP // 128):
            at = g * (GROUP // 128) + piece
            side, base = divmod(at * 128, dbc_out.shape[1])
            for m in range(dbc_out.shape[0]):
                source, left = divmod(m * 64, STATE)
                dbc_out[m, base : base + 128, side * 64 : side * 64 + 64] = grads[source][
                    piece * 128 : (piece + 1) * 128, left : left + 64
                ]
        sum_dt = dot_exact(tri, dt)
        sum_sl = dot_exact(tri, slope)
        all_dt = sum_dt[GROUP - 1 : GROUP, :]
        all_sl = sum_sl[GROUP - 1 : GROUP, :]
        inner = jnp.sum(sp * gp, axis=0, keepdims=True)
        meet = jnp.exp(last[g]) * dot_exact(jnp.broadcast_to(inner, (8, inner.shape[1])), gather_e)[0:1, :]
        flow_dt_all += jnp.sum(back * sum_dt + fore * (all_dt - sum_dt), axis=0, keepdims=True) + meet * all_dt
        flow_sl_all += jnp.sum(back * sum_sl + fore * (all_sl - sum_sl), axis=0, keepdims=True) + meet * all_sl
        bias_all += jnp.sum(slope / dt * x_gb, axis=0, keepdims=True)
        skip_all += jnp.sum(skips, axis=0, keepdims=True)
    intra = flow_ref[0]
    for g in range(1, groups):
        intra = intra + flow_ref[g]
    totals = jnp.transpose(jnp.sum(intra, axis=1, keepdims=True) + jnp.zeros((2 * heads, 128), F32))[0:1, :]
    flow_dt_all += totals[:, 0:heads]
    flow_sl_all += totals[:, heads : 2 * heads]
    stat_ref[...] = jnp.zeros_like(stat_ref)
    stat_ref[0:1, 0:heads] = rate * flow_dt_all
    stat_ref[1:2, 0:heads] = bias_all + rate * flow_sl_all
    stat_ref[2:3, 0:heads] = skip_all


MESH = pl.DeviceIdType.MESH
W_ROWS = 48


def around(axis, shift):
    return {axis: lax.rem(lax.axis_index(axis) + shift, 4)}


def remote(source, target, send, recv, device):
    return pltpu.make_async_remote_copy(
        src_ref=source, dst_ref=target, send_sem=send, recv_sem=recv, device_id=device, device_id_type=MESH
    )


class RingSum:
    def __init__(self, axis, part, relay, final, send, recv, base):
        self.axis, self.part, self.relay, self.final = axis, part, relay, final
        self.send, self.recv, self.base = send, recv, base
        me = lax.axis_index(axis)
        self.me = me
        self.ahead, self.behind, self.across = (lax.rem(me + k, 4) for k in (1, 3, 2))
        self.up, self.down = around(axis, 1), around(axis, 3)
        self.copies = {}

    def copy(self, n, source, target, device):
        at = self.base + n
        self.copies[n] = remote(source, target, self.send(at), self.recv(at), device)
        self.copies[n].start()

    def first(self):
        self.copy(0, self.part(self.across, 0), self.relay(0), self.up)
        self.copy(1, self.part(self.across, 1), self.relay(1), self.down)
        self.copy(2, self.part(self.ahead, 1), self.final(0, 1), self.up)
        self.copy(3, self.part(self.behind, 0), self.final(1, 0), self.down)

    def second(self):
        self.copies[0].wait_recv()
        ahead = self.part(self.ahead, 0)
        ahead[...] += self.relay(0)[...]
        self.copy(4, ahead, self.final(0, 0), self.up)
        self.copies[1].wait_recv()
        behind = self.part(self.behind, 1)
        behind[...] += self.relay(1)[...]
        self.copy(5, behind, self.final(1, 1), self.down)

    def result(self, half):
        (self.copies[4] if half == 0 else self.copies[2]).wait_recv()
        (self.copies[3] if half == 0 else self.copies[5]).wait_recv()
        return self.part(self.me, half)[...] + self.final(0, half)[...] + self.final(1, half)[...]

    def drain(self):
        for copy in self.copies.values():
            copy.wait_send()


class PlaneSum:
    def __init__(self, first_axis, second_axis, swap, own, relay, final, mid, relay2, final2, send, recv, store):
        rows = mid.shape[1]
        self.store, self.mid, self.rows = store, mid, rows

        def part(d, half):
            pair = pl.ds(2 * half, 2)
            return own.at[pair, d] if swap else own.at[d, pair]

        def part2(d, half):
            return mid.at[d, pl.ds(half * (rows // 2), rows // 2)]

        self.one = RingSum(first_axis, part, lambda h: relay.at[h], lambda w, h: final.at[w, pl.ds(2 * h, 2)],
                           send, recv, 0)
        self.two = RingSum(second_axis, part2, lambda h: relay2.at[h],
                           lambda w, h: final2.at[w, pl.ds(h * (rows // 2), rows // 2)], send, recv, 6)

    def run(self, stage):
        if stage == 0:
            self.one.first()
        elif stage == 1:
            self.one.second()
        elif stage == 2:
            for half in range(2):
                self.mid[pl.ds(2 * half, 2)] = self.one.result(half)
            self.two.first()
        elif stage == 3:
            self.two.second()
        elif stage == 4:
            for half in range(2):
                self.store(half, self.two.result(half))

    def drain(self):
        self.one.drain()
        self.two.drain()


def project_kernel(lt_hbm, dx_hbm, dbc_ref, stats_ref, wx_ref, wbc_ref, total_ref,
                   lt, dx, dbc_in, work, relay, final, mid, relay2, final2,
                   w_work, w_relay, w_final, w_mid, w_relay2, w_final2,
                   load_sem, mp_send, mp_recv, core_send, core_recv, send, recv):
    block = wx_ref.shape[0]
    chunks = work.shape[1]
    core = lax.axis_index("seq_2")
    mp = lax.axis_index("mp")
    other = {"seq_2": 1 - core}

    loads = [pltpu.make_async_copy(dx_hbm, dx, load_sem.at[32])]
    loads[0].start()
    for slot in range(2):
        kind = 1 - core if slot == 0 else core
        for k in range(16):
            start = pl.multiple_of((2 * k + kind) * block, 16)
            load = pltpu.make_async_copy(
                lt_hbm.at[pl.ds(start, block)], lt.at[slot, pl.ds(k * block, block)], load_sem.at[slot * 16 + k]
            )
            load.start()
            loads.append(load)

    partners = [other] + [around(axis, k) for axis in ("seq_0", "seq_1") for k in (1, 3)]
    partners += [around("mp", k) for k in (1, 2, 3)]
    barrier = pltpu.get_barrier_semaphore()
    for partner in partners:
        pl.semaphore_signal(barrier, inc=1, device_id=partner, device_id_type=MESH)
    pl.semaphore_wait(barrier, len(partners))

    mp_copies = []
    for k in (1, 2, 3):
        target = around("mp", k)
        copy = remote(dbc_ref.at[target["mp"]], dbc_in.at[k - 1], mp_send.at[k - 1], mp_recv.at[k - 1], target)
        copy.start()
        mp_copies.append(copy)

    for load in loads:
        load.wait()

    send_own, got, own = (work.at[i] for i in range(3))
    core_copies = {}

    def give(j):
        cols = dx[:, j * 256 : (j + 1) * 256]

        def body(i, unused):
            start = pl.multiple_of(i * 4 * block, 16)
            res = dot(lt[0, pl.ds(start, 4 * block), :], cols)
            for side in range(2):
                send_own[j, side, i] = res[:, side * 128 : (side + 1) * 128].reshape(4, block, 128)
            return unused

        lax.fori_loop(0, 4, body, 0)
        core_copies[j] = remote(send_own.at[j], got.at[j], core_send.at[j], core_recv.at[j], other)
        core_copies[j].start()

    def keep(j):
        core_copies[j].wait_recv()
        cols = dx[:, j * 256 : (j + 1) * 256]

        def body(i, unused):
            start = pl.multiple_of(i * 4 * block, 16)
            res = dot(lt[1, pl.ds(start, 4 * block), :], cols)
            for side in range(2):
                own[j, side, i] = got[j, side, i] + res[:, side * 128 : (side + 1) * 128].reshape(4, block, 128)
            return unused

        lax.fori_loop(0, 4, body, 0)

    def narrow(slot, i, cols):
        start = pl.multiple_of(i * 4 * block, 16)
        res = dot(lt[slot, pl.ds(start, 4 * block), :], cols).reshape(4, block, 64)
        grads = jnp.concatenate([res[:, 0 : block // 2], res[:, block // 2 : block]], axis=2)
        stats = jnp.broadcast_to(stats_ref[...][None], (4, 8, 128))
        return jnp.concatenate([grads, stats], axis=1)

    def owned_cols():
        for copy in mp_copies:
            copy.wait_recv()
        owned = dbc_ref[mp] + dbc_in[0] + dbc_in[1] + dbc_in[2]
        return jnp.concatenate([owned[:, 0:64], owned[:, 64:128]], axis=0).astype(BF16)

    def give_narrow(cols):
        def body(i, unused):
            w_work[0, i] = narrow(0, i, cols)
            return unused

        lax.fori_loop(0, 4, body, 0)
        core_copies[chunks] = remote(
            w_work.at[0], w_work.at[1], core_send.at[chunks], core_recv.at[chunks], other
        )
        core_copies[chunks].start()

    def keep_narrow(cols):
        core_copies[chunks].wait_recv()

        def body(i, unused):
            w_work[2, i] = w_work[1, i] + narrow(1, i, cols)
            return unused

        lax.fori_loop(0, 4, body, 0)

    def store_wide(j, side):
        def store(half, value):
            wx_ref[half * (block // 2) : (half + 1) * (block // 2), j * 256 + side * 128 : j * 256 + side * 128 + 128] = value

        return store

    def store_narrow(half, value):
        w_work[0, 0, 0, half * (W_ROWS // 2) : (half + 1) * (W_ROWS // 2)] = value

    def stream(j, side):
        axes = ("seq_0", "seq_1") if side == 0 else ("seq_1", "seq_0")
        n = 2 * j + side
        return PlaneSum(*axes, side == 1, own.at[j, side], relay.at[:, j, side], final.at[:, j, side],
                        mid.at[j, side], relay2.at[:, j, side], final2.at[:, j, side],
                        lambda k: send.at[n, k], lambda k: recv.at[n, k], store_wide(j, side))

    streams = [[stream(j, 0), stream(j, 1)] for j in range(chunks)]
    last = 2 * chunks
    streams.append([PlaneSum("seq_0", "seq_1", False, w_work.at[2], w_relay, w_final, w_mid, w_relay2, w_final2,
                             lambda k: send.at[last, k], lambda k: recv.at[last, k], store_narrow)])

    cols_low = []
    give(0)
    for t in range(chunks + 6):
        if t + 1 < chunks:
            give(t + 1)
        elif t + 1 == chunks:
            cols_low.append(owned_cols())
            give_narrow(cols_low[0])
        if t < chunks:
            keep(t)
        elif t == chunks:
            keep_narrow(cols_low[0])
        for stage in range(5):
            j = t - stage
            if 0 <= j <= chunks:
                if stage == 4 and j == chunks:
                    core_copies[chunks].wait_send()
                for one in streams[j]:
                    one.run(stage)

    half = block // 2
    wbc_ref[0:half, :] = w_work[0, 0, 0, 0:half, 0:64]
    wbc_ref[half:block, :] = w_work[0, 0, 0, 0:half, 64:128]
    total_ref[...] = w_work[0, 0, 0, half : half + 8, :]
    for copy in mp_copies:
        copy.wait_send()
    for j in range(chunks):
        core_copies[j].wait_send()
    for group in streams:
        for one in group:
            one.drain()


def full(shape):
    return pl.BlockSpec(shape, lambda *_: (0,) * len(shape))


def by_group(width):
    return pl.BlockSpec((GROUP, width), lambda g: (g, 0))


def call(kernel, out, name, flops, nbytes, **options):
    params = pltpu.CompilerParams(vmem_limit_bytes=options.pop("vmem", 56 * 1024 * 1024))
    cost = pl.CostEstimate(flops=flops, bytes_accessed=nbytes, transcendentals=0)
    return pl.pallas_call(kernel, out_shape=out, name=name, cost_estimate=cost, compiler_params=params, **options)


def on_device(layer_in, ssm_input, b_matrix, c_matrix, dt_raw, dt_bias, a_log, d_skip, grad_out):
    tokens, heads = dt_raw.shape
    width = heads * HEAD_DIM
    groups = tokens // GROUP
    devices = math.prod(lax.axis_size(axis) for axis in SEQ)
    rows = 2 * STATE // devices
    shifted = dt_raw + dt_bias[None, :]
    dt = jax.nn.softplus(shifted)
    slope = jax.nn.sigmoid(shifted)
    rate = -jnp.exp(a_log)
    log_step = dt * rate[None, :]
    sds = jax.ShapeDtypeStruct

    parts, ends = call(
        states_kernel,
        (sds((2 * groups - 2, STATE, width), F32), sds((2 * STATE, width + 128), F32)),
        "block_states", 10**9, 10**7,
        scratch_shapes=[VMEM((STATE, width), F32), VMEM((STATE, width), F32)],
    )(ssm_input, grad_out, b_matrix, c_matrix, dt, log_step)

    sent = ends.reshape(devices, rows, width + 128)
    got = lax.all_to_all(sent, SEQ, split_axis=0, concat_axis=0, tiled=True)
    position = lax.axis_index(SEQ)
    backward = (position >= devices // 2).astype(jnp.int32).reshape(1)
    scanned = call(
        scan_kernel, sds((devices, rows, width), F32), "carry_scan", 10**8, 3 * 10**6,
        in_specs=[pl.BlockSpec(memory_space=pltpu.SMEM), full((devices, rows, width + 128))],
        out_specs=full((devices, rows, width)),
        grid=(1,),
        scratch_shapes=[VMEM((devices, width), F32)],
    )(backward, got)
    carry = lax.all_to_all(scanned, SEQ, split_axis=0, concat_axis=0, tiled=True).reshape(2 * STATE, width)

    gi, dbc_local, flows = call(
        intra_kernel,
        (sds((tokens, width), BF16), sds((tokens, 2 * STATE), F32), sds((groups, 2 * heads, GROUP), F32)),
        "intra", 3 * 10**10, 8 * 10**6,
        grid=(groups,),
        in_specs=[by_group(width), by_group(width), by_group(STATE), by_group(STATE),
                  by_group(heads), by_group(heads), by_group(heads)],
        out_specs=(by_group(width), by_group(2 * STATE), pl.BlockSpec((1, 2 * heads, GROUP), lambda g: (g, 0, 0))),
        scratch_shapes=[VMEM((GROUP, GROUP), F32), VMEM((2, GROUP, GROUP), BF16)],
    )(ssm_input, grad_out, b_matrix, c_matrix, dt, slope, log_step)

    skip_wide = jnp.repeat(d_skip, HEAD_DIM)[None, :]
    dx, dbc, stats = call(
        final_kernel,
        (sds((tokens, width), BF16), sds((4, tokens // 2, 128), F32), sds((8, 128), F32)),
        "combine", 2 * 10**9, 2 * 10**7,
        scratch_shapes=[VMEM((groups, STATE, width), F32), VMEM((groups, STATE, width), F32)],
    )(ssm_input, grad_out, b_matrix, c_matrix, dt, slope, log_step, skip_wide, rate[None, :], gi, dbc_local,
      flows, parts, carry)

    flipped = layer_in.T
    block = flipped.shape[0] // devices
    chunks = width // 256
    grad_wx, grad_wbc, totals = pl.pallas_call(
        project_kernel,
        out_shape=(sds((block, width), F32), sds((block, 64), F32), sds((8, 128), F32)),
        in_specs=[pl.BlockSpec(memory_space=pl.ANY), pl.BlockSpec(memory_space=pl.ANY),
                  pl.BlockSpec(memory_space=VMEM), pl.BlockSpec(memory_space=VMEM)],
        out_specs=(pl.BlockSpec(memory_space=VMEM),) * 3,
        scratch_shapes=[
            VMEM((2, 16 * block, tokens), BF16),
            VMEM((tokens, width), BF16),
            VMEM((3, tokens // 2, 128), F32),
            VMEM((3, chunks, 2, 4, 4, block, 128), F32),
            VMEM((2, chunks, 2, 2, block, 128), F32),
            VMEM((2, chunks, 2, 4, block, 128), F32),
            VMEM((chunks, 2, 4, block, 128), F32),
            VMEM((2, chunks, 2, block // 2, 128), F32),
            VMEM((2, chunks, 2, block, 128), F32),
            VMEM((3, 4, 4, W_ROWS, 128), F32),
            VMEM((2, 2, W_ROWS, 128), F32),
            VMEM((2, 4, W_ROWS, 128), F32),
            VMEM((4, W_ROWS, 128), F32),
            VMEM((2, W_ROWS // 2, 128), F32),
            VMEM((2, W_ROWS, 128), F32),
            pltpu.SemaphoreType.DMA((33,)),
            pltpu.SemaphoreType.DMA((3,)),
            pltpu.SemaphoreType.DMA((3,)),
            pltpu.SemaphoreType.DMA((chunks + 1,)),
            pltpu.SemaphoreType.DMA((chunks + 1,)),
            pltpu.SemaphoreType.DMA((2 * chunks + 1, 12)),
            pltpu.SemaphoreType.DMA((2 * chunks + 1, 12)),
        ],
        name="project",
        cost_estimate=pl.CostEstimate(flops=5 * 10**9, bytes_accessed=10**7, transcendentals=0),
        compiler_params=pltpu.CompilerParams(
            collective_id=0, has_side_effects=True, vmem_limit_bytes=60 * 1024 * 1024
        ),
    )(flipped, dx, dbc, stats)
    return (grad_wx, grad_wbc, totals[0, :heads], totals[1, :heads], totals[2, :heads])


def solution(mesh):
    n_seq, n_mp = mesh.shape["seq"], mesh.shape["mp"]
    split = Mesh(mesh.devices.reshape(n_seq // 8, 4, 2, n_mp), SEQ + ("mp",))
    in_specs = (
        P(SEQ, None),
        P(SEQ, "mp"),
        P(SEQ, None),
        P(SEQ, None),
        P(SEQ, "mp"),
        P("mp"),
        P("mp"),
        P("mp"),
        P(SEQ, "mp"),
    )
    out_specs = (P(SEQ, "mp"), P(SEQ, "mp"), P("mp"), P("mp"), P("mp"))
    return jax.shard_map(
        on_device, mesh=split, in_specs=in_specs, out_specs=out_specs, check_vma=False
    )
```

```python
import functools
import math

import jax
import jax.numpy as jnp
from jax import lax
from jax.experimental import pallas as pl
from jax.experimental.pallas import tpu as pltpu
from jax.sharding import Mesh
from jax.sharding import PartitionSpec as P

GROUP = 256
HEAD_DIM = 64
STATE = 128
LOG2E = 1.0 / math.log(2.0)
SEQ = ("seq_0", "seq_1", "seq_2")
F32 = jnp.float32
BF16 = jnp.bfloat16
VMEM = pltpu.VMEM


def dot(left, right):
    return jnp.dot(left, right, preferred_element_type=F32)


def dot_nt(left, right):
    return lax.dot_general(left, right, (((1,), (1,)), ((), ())), preferred_element_type=F32)


def dot_tn(left, right):
    return lax.dot_general(left, right, (((0,), (0,)), ((), ())), preferred_element_type=F32)


def dot_exact(left, right):
    return jnp.dot(left, right, preferred_element_type=F32, precision=lax.Precision.HIGHEST)


def lane_iota(shape, dim):
    return lax.broadcasted_iota(jnp.int32, shape, dim)


def spread_matrix(heads, dtype):
    rows = lane_iota((heads, heads * HEAD_DIM), 0)
    cols = lane_iota((heads, heads * HEAD_DIM), 1)
    inside = (cols >= rows * HEAD_DIM) & (cols < (rows + 1) * HEAD_DIM)
    return jnp.where(inside, 1.0, 0.0).astype(dtype)


def gather_matrix(heads, dtype):
    rows = lane_iota((heads * HEAD_DIM, heads), 0)
    cols = lane_iota((heads * HEAD_DIM, heads), 1)
    inside = (rows >= cols * HEAD_DIM) & (rows < (cols + 1) * HEAD_DIM)
    return jnp.where(inside, 1.0, 0.0).astype(dtype)


def lower_ones(size):
    return jnp.where(lane_iota((size, size), 0) >= lane_iota((size, size), 1), 1.0, 0.0)


def spread(values, matrix):
    high = values.astype(BF16)
    low = (values - high.astype(F32)).astype(BF16)
    return dot(high, matrix) + dot(low, matrix)


MESH = pl.DeviceIdType.MESH
W_ROWS = 48


def around(axis, shift):
    return {axis: lax.rem(lax.axis_index(axis) + shift, 4)}


def remote(source, target, send, recv, device):
    return pltpu.make_async_remote_copy(
        src_ref=source, dst_ref=target, send_sem=send, recv_sem=recv, device_id=device, device_id_type=MESH
    )


class RingSum:
    def __init__(self, axis, part, relay, final, send, recv, base):
        self.axis, self.part, self.relay, self.final = axis, part, relay, final
        self.send, self.recv, self.base = send, recv, base
        me = lax.axis_index(axis)
        self.me = me
        self.ahead, self.behind, self.across = (lax.rem(me + k, 4) for k in (1, 3, 2))
        self.up, self.down = around(axis, 1), around(axis, 3)
        self.copies = {}

    def copy(self, n, source, target, device):
        at = self.base + n
        self.copies[n] = remote(source, target, self.send(at), self.recv(at), device)
        self.copies[n].start()

    def first(self):
        self.copy(0, self.part(self.across, 0), self.relay(0), self.up)
        self.copy(1, self.part(self.across, 1), self.relay(1), self.down)
        self.copy(2, self.part(self.ahead, 1), self.final(0, 1), self.up)
        self.copy(3, self.part(self.behind, 0), self.final(1, 0), self.down)

    def second(self):
        self.copies[0].wait_recv()
        ahead = self.part(self.ahead, 0)
        ahead[...] += self.relay(0)[...]
        self.copy(4, ahead, self.final(0, 0), self.up)
        self.copies[1].wait_recv()
        behind = self.part(self.behind, 1)
        behind[...] += self.relay(1)[...]
        self.copy(5, behind, self.final(1, 1), self.down)

    def result(self, half):
        (self.copies[4] if half == 0 else self.copies[2]).wait_recv()
        (self.copies[3] if half == 0 else self.copies[5]).wait_recv()
        return self.part(self.me, half)[...] + self.final(0, half)[...] + self.final(1, half)[...]

    def drain(self):
        for copy in self.copies.values():
            copy.wait_send()


class PlaneSum:
    def __init__(self, first_axis, second_axis, swap, own, relay, final, mid, relay2, final2, send, recv, store):
        rows = mid.shape[1]
        self.store, self.mid, self.rows = store, mid, rows

        def part(d, half):
            pair = pl.ds(2 * half, 2)
            return own.at[pair, d] if swap else own.at[d, pair]

        def part2(d, half):
            return mid.at[d, pl.ds(half * (rows // 2), rows // 2)]

        self.one = RingSum(first_axis, part, lambda h: relay.at[h], lambda w, h: final.at[w, pl.ds(2 * h, 2)],
                           send, recv, 0)
        self.two = RingSum(second_axis, part2, lambda h: relay2.at[h],
                           lambda w, h: final2.at[w, pl.ds(h * (rows // 2), rows // 2)], send, recv, 6)

    def run(self, stage):
        if stage == 0:
            self.one.first()
        elif stage == 1:
            self.one.second()
        elif stage == 2:
            for half in range(2):
                self.mid[pl.ds(2 * half, 2)] = self.one.result(half)
            self.two.first()
        elif stage == 3:
            self.two.second()
        elif stage == 4:
            for half in range(2):
                self.store(half, self.two.result(half))

    def drain(self):
        self.one.drain()
        self.two.drain()


STRIP = 64


def scalars(raw_ref, bias_ref, log_ref, dt_ref, slope_ref, a_ref):
    shifted = raw_ref[...] + bias_ref[...]
    small = jnp.exp(-jnp.abs(shifted))
    one = 1.0 + small
    log_one = jnp.where(one == 1.0, small, jnp.log(one) * small / jnp.where(one == 1.0, 1.0, one - 1.0))
    dt = jnp.maximum(shifted, 0.0) + log_one
    dt_ref[...] = dt
    slope_ref[...] = jnp.where(shifted >= 0.0, 1.0, small) / one
    a_ref[...] = dt * -jnp.exp(log_ref[...])


def states(x, dy, b_ref, c_ref, dt_ref, slope_ref, a_ref, within_ref, last_ref, cols_ref, rows_ref, cross_ref,
           decay_ref, spread_ref, parts, ends):
    tokens, heads = dt_ref.shape
    groups = tokens // GROUP
    width = heads * HEAD_DIM
    tri = lower_ones(GROUP)
    spread_m = spread_matrix(heads, BF16)
    spread_ref[...] = spread_m
    spread_e = spread_matrix(heads, F32)
    block_end = jnp.zeros((1, heads), F32)
    for g in range(groups):
        rows = slice(g * GROUP, (g + 1) * GROUP)
        dt = dt_ref[rows, :]
        sums = dot_exact(tri, jnp.concatenate([a_ref[rows, :], dt, slope_ref[rows, :]], axis=1))
        within = sums[:, 0:heads]
        last = within[GROUP - 1 : GROUP, :]
        block_end = block_end + last
        within_ref[rows, :] = within
        last_ref[g : g + 1, :] = last
        decay = dot_exact(jnp.broadcast_to(jnp.exp(last), (8, heads)), spread_e)[0:1, :]
        decay_ref[g : g + 1, :] = decay
        fall = spread(dt * jnp.exp(last - within), spread_m)
        xw = (x[rows, :].astype(F32) * fall).astype(BF16)
        state = dot_tn(b_ref[rows, :], xw)
        rise = spread(jnp.exp(within), spread_m)
        yw = (dy[rows, :].astype(F32) * rise).astype(BF16)
        grad = dot_tn(c_ref[rows, :], yw)
        if g < groups - 1:
            parts[g] = state
        if g > 0:
            parts[groups - 2 + g] = grad
        if g == 0:
            ends[0:STATE, 0:width] = state
            ends[STATE : 2 * STATE, 0:width] = grad
            gain = decay
        else:
            ends[0:STATE, 0:width] = decay * ends[0:STATE, 0:width] + state
            ends[STATE : 2 * STATE, 0:width] = ends[STATE : 2 * STATE, 0:width] + gain * grad
            gain = gain * decay
        packed = jnp.concatenate([within * LOG2E - jnp.log2(dt), sums[:, heads : 3 * heads]], axis=1)
        cols_ref[rows, :] = packed
        rows_ref[g] = jnp.transpose(jnp.concatenate([within * LOG2E, sums[:, heads : 3 * heads]], axis=1))
        cross_ref[g] = dot_nt(b_ref[rows, :], c_ref[rows, :])
    pad = jnp.concatenate([jnp.exp(block_end), jnp.zeros((1, 128 - heads), F32)], axis=1)
    ends[:, width : width + 128] = jnp.broadcast_to(pad, (2 * STATE, 128))


class Carry:
    def __init__(self, ends, pair, out, got, scanned, back, mine, yours, carry, gains, core_sems, sems):
        self.ends, self.pair, self.out, self.got, self.scanned = ends, pair, out, got, scanned
        self.back, self.mine, self.yours, self.carry, self.gains = back, mine, yours, carry, gains
        self.core_sems, self.sems = core_sems, sems
        self.core = lax.axis_index("seq_2")
        self.other = {"seq_2": 1 - self.core}
        self.me = lax.axis_index("seq_0") * 4 + lax.axis_index("seq_1")
        self.width = carry.shape[1]
        self.heads = self.width // HEAD_DIM

    def own_rows(self, kind, core):
        return pl.ds(pl.multiple_of(kind * STATE + core * (STATE // 2), STATE // 2), STATE // 2)

    def chip(self, offset):
        index = lax.rem(self.me + offset, 16)
        return index, {"seq_0": index // 4, "seq_1": lax.rem(index, 4)}

    def give_pair(self):
        self.pair_copies = []
        for kind in range(2):
            copy = remote(self.ends.at[self.own_rows(kind, 1 - self.core)], self.pair.at[kind],
                          self.core_sems.at[0, kind], self.core_sems.at[1, kind], self.other)
            copy.start()
            self.pair_copies.append(copy)

    def both(self, kind):
        own = self.ends[self.own_rows(kind, self.core), 0 : self.width]
        other = self.pair[kind, :, 0 : self.width]
        first = self.core == 0
        return jnp.where(first, own, other), jnp.where(first, other, own)

    def gains_of(self, tile):
        return dot_exact(tile[:, 0 : self.heads], spread_matrix(self.heads, F32))

    def give_chips(self):
        width, heads = self.width, self.heads
        half = STATE // 2
        for copy in self.pair_copies:
            copy.wait_recv()
        mine, theirs = self.ends[0:8, width : width + 128], self.pair[0, 0:8, width : width + 128]
        first = self.core == 0
        tile0, tile1 = jnp.where(first, mine, theirs), jnp.where(first, theirs, mine)
        self.gains[0:8, :] = self.gains_of(tile0)
        self.gains[8:16, :] = self.gains_of(tile1)
        s0, s1 = self.both(0)
        chip_s = self.gains[8:9, :] * s0 + s1
        self.out[0:8, :, 0:width] = chip_s.reshape(8, 8, width)
        g0, g1 = self.both(1)
        chip_g = g0 + self.gains[0:1, :] * g1
        self.out[8:16, :, 0:width] = chip_g.reshape(8, 8, width)
        self.out[:, :, width : width + 128] = jnp.broadcast_to((tile0 * tile1)[None], (16, 8, 128))
        self.got[0] = self.out[self.me]
        self.copies = []
        for k in range(1, 16):
            index, device = self.chip(k)
            copy = remote(self.out.at[index], self.got.at[k], self.sems.at[0, k], self.sems.at[1, k], device)
            copy.start()
            self.copies.append(copy)

    def scan(self):
        width = self.width
        for copy in self.copies:
            copy.wait_recv()
        self.gains[16:32, :] = self.gains_of(self.got[:, 0, width : width + 128])
        backward = self.me >= 8

        def step(i, running):
            chip = jnp.where(backward, 15 - i, i)
            slot = lax.rem(self.me - chip + 16, 16)
            self.scanned[slot] = running
            return self.gains[pl.ds(16 + slot, 1), :] * running + self.got[slot, :, 0:width]

        lax.fori_loop(0, 16, step, jnp.zeros((8, width), F32))
        self.back[self.me] = self.scanned[0]
        self.back_copies = []
        for k in range(1, 16):
            index, device = self.chip(16 - k)
            copy = remote(self.scanned.at[k], self.back.at[self.me], self.sems.at[2, k], self.sems.at[3, k], device)
            copy.start()
            self.back_copies.append(copy)

    def give_back(self):
        width = self.width
        half = STATE // 2
        for copy in self.back_copies:
            copy.wait_recv()
        first = self.core == 0
        s_in = self.back[0:8].reshape(half, width)
        s0, _ = self.both(0)
        s_next = self.gains[0:1, :] * s_in + s0
        self.carry[self.own_rows(0, self.core), :] = jnp.where(first, s_in, s_next)
        self.mine[0] = jnp.where(first, s_next, s_in)
        g_in = self.back[8:16].reshape(half, width)
        _, g1 = self.both(1)
        g_before = g1 + self.gains[8:9, :] * g_in
        self.carry[self.own_rows(1, self.core), :] = jnp.where(first, g_before, g_in)
        self.mine[1] = jnp.where(first, g_in, g_before)
        self.last = remote(self.mine, self.yours, self.core_sems.at[0, 2], self.core_sems.at[1, 2], self.other)
        self.last.start()

    def finish(self):
        self.last.wait_recv()
        for kind in range(2):
            self.carry[self.own_rows(kind, 1 - self.core), :] = self.yours[kind]

    def drain(self):
        for copy in self.pair_copies + self.copies + self.back_copies + [self.last]:
            copy.wait_send()


def intra(j, x, dy, cols_ref, rows_ref, cross_ref, v_ref, mix_ref, gi, flow_ref, heads):
    half = GROUP // 2

    def group(g, unused):
        at = pl.multiple_of(g * GROUP, GROUP)
        for pair in range(2 * j, 2 * j + 2):
            zs, sides = [], []
            for sub in range(2):
                h = 2 * pair + sub
                lanes = slice(h * HEAD_DIM, (h + 1) * HEAD_DIM)
                x_h = x[pl.ds(at, GROUP), lanes]
                dy_h = dy[pl.ds(at, GROUP), lanes]
                top = dot_nt(x_h[0:half], dy_h)
                low = dot_nt(x_h[half:GROUP], dy_h[half:GROUP])
                acc = [jnp.zeros((8, GROUP), F32) for _ in range(3)]
                z_strips = []
                for k in range(GROUP // STRIP):
                    first = (k * STRIP // half) * half
                    wide = GROUP - first
                    rows = slice(k * STRIP, (k + 1) * STRIP)
                    here = pl.ds(at + k * STRIP, STRIP)
                    gap = rows_ref[g, h : h + 1, first:GROUP] - cols_ref[here, h : h + 1]
                    reach = lane_iota((STRIP, wide), 1) + first >= lane_iota((STRIP, wide), 0) + k * STRIP
                    decay = jnp.where(reach, jnp.exp2(gap), 0.0)
                    bc = cross_ref[g, rows, first:GROUP]
                    mix_ref[sub, rows, first:GROUP] = (decay * bc).astype(BF16)
                    z = decay * (top[rows, :] if first == 0 else low[k * STRIP - half : (k + 1) * STRIP - half, :])
                    z_strips.append(z)
                    box = z * bc
                    w_dt = cols_ref[here, heads + h : heads + h + 1]
                    w_sl = cols_ref[here, 2 * heads + h : 2 * heads + h + 1]
                    for n, term in enumerate((box, box * w_dt, box * w_sl)):
                        part = jnp.sum(term.reshape(STRIP // 8, 8, wide), axis=0)
                        if first > 0:
                            acc[n] = jnp.concatenate([acc[n][:, 0:first], acc[n][:, first:GROUP] + part], axis=1)
                        else:
                            acc[n] = acc[n] + part
                zs.append(z_strips)
                sides.append(dot(mix_ref[sub], dy_h))
                flow_dt = acc[0] * rows_ref[g, heads + h : heads + h + 1, :] - acc[1]
                flow_sl = acc[0] * rows_ref[g, 2 * heads + h : 2 * heads + h + 1, :] - acc[2]
                flow_ref[g, h : h + 1, :] = jnp.sum(flow_dt, axis=0, keepdims=True)
                flow_ref[g, heads + h : heads + h + 1, :] = jnp.sum(flow_sl, axis=0, keepdims=True)
            for k in range(GROUP // STRIP):
                first = (k * STRIP // half) * half
                rows = slice(k * STRIP, (k + 1) * STRIP)
                both = zs[0][k] + zs[1][k]
                if pair == 0:
                    v_ref[g, rows, first:GROUP] = both
                else:
                    v_ref[g, rows, first:GROUP] += both
            gi[pl.ds(at, GROUP), pair * 128 : (pair + 1) * 128] = jnp.concatenate(sides, axis=1).astype(BF16)
        return unused

    lax.fori_loop(0, x.shape[0] // GROUP, group, 0)


def combine(j, x, dy, b_ref, c_ref, dt_ref, within_ref, last_ref, decay_ref, spread_ref, skip_ref, parts, carry,
            sp_ref, gp_ref, dx, dbc, sums_ref, inner_ref):
    tokens, heads = dt_ref.shape
    groups = tokens // GROUP
    cols = slice(j * 256, (j + 1) * 256)
    sp_ref[0] = carry[0:STATE, cols]
    gp_ref[groups - 1] = carry[STATE : 2 * STATE, cols]
    for g in range(groups - 1):
        sp_ref[g + 1] = decay_ref[g : g + 1, cols] * sp_ref[g] + parts[g, :, cols]
    for g in range(groups - 1, 0, -1):
        gp_ref[g - 1] = parts[groups - 2 + g, :, cols] + decay_ref[g : g + 1, cols] * gp_ref[g]
    spread_m = spread_ref[:, cols]
    head = (lane_iota((256, 128), 0) + j * 256) // HEAD_DIM
    lane = lane_iota((256, 128), 1)

    def gather(k):
        return jnp.where(lane == head + k * heads, 1.0, 0.0).astype(BF16)

    for g in range(groups):
        rows = slice(g * GROUP, (g + 1) * GROUP)
        within = within_ref[rows, :]
        fall = spread(dt_ref[rows, :] * jnp.exp(last_ref[g : g + 1, :] - within), spread_m)
        rise = spread(jnp.exp(within), spread_m)
        xs = x[rows, cols].astype(F32)
        dys = dy[rows, cols].astype(F32)
        sp = sp_ref[g]
        gp = gp_ref[g]
        inner_ref[g : g + 1, cols] = jnp.sum(sp * gp, axis=0, keepdims=True)
        sp_low = sp.astype(BF16)
        gp_low = gp.astype(BF16)
        from_end = dot(b_ref[rows, :], gp_low)
        from_start = dot(c_ref[rows, :], sp_low)
        raw = dx[rows, cols].astype(F32) + fall * from_end
        total = dot((xs * raw).astype(BF16), gather(0))
        total += dot((xs * from_end).astype(BF16), gather(1))
        total += dot((xs * dys).astype(BF16), gather(2))
        total += dot((dys * from_start).astype(BF16), gather(3))
        dx[rows, cols] = (raw + skip_ref[:, cols] * dys).astype(BF16)
        d_b = dot_nt((xs * fall).astype(BF16), gp_low)
        d_c = dot_nt((dys * rise).astype(BF16), sp_low)
        if j == 0:
            sums_ref[rows, :] = total
            dbc[rows, 0:STATE] = d_b
            dbc[rows, STATE : 2 * STATE] = d_c
        else:
            sums_ref[rows, :] += total
            dbc[rows, 0:STATE] += d_b
            dbc[rows, STATE : 2 * STATE] += d_c


def mixed_grads(b_ref, c_ref, v_ref, dbc, packed):
    groups = v_ref.shape[0]
    for g in range(groups):
        rows = slice(g * GROUP, (g + 1) * GROUP)
        mixed = v_ref[g].astype(BF16)
        grads = (dbc[rows, 0:STATE] + dot(mixed, c_ref[rows, :]),
                 dbc[rows, STATE : 2 * STATE] + dot_tn(mixed, b_ref[rows, :]))
        for piece in range(GROUP // 128):
            at = g * (GROUP // 128) + piece
            side, base = divmod(at * 128, packed.shape[1])
            for m in range(packed.shape[0]):
                source, left = divmod(m * 64, STATE)
                packed[m, base : base + 128, side * 64 : side * 64 + 64] = grads[source][
                    piece * 128 : (piece + 1) * 128, left : left + 64
                ]


def statistics(dt_ref, slope_ref, log_ref, within_ref, last_ref, cols_ref, sums_ref, inner_ref, flow_ref, stat_ref):
    tokens, heads = dt_ref.shape
    groups = tokens // GROUP
    gather_e = gather_matrix(heads, F32)
    rate = -jnp.exp(log_ref[...])
    flow_dt = jnp.zeros((1, heads), F32)
    flow_sl = jnp.zeros((1, heads), F32)
    bias = jnp.zeros((1, heads), F32)
    skips = jnp.zeros((1, heads), F32)
    inner = dot_exact(inner_ref[...], gather_e)
    for g in range(groups):
        rows = slice(g * GROUP, (g + 1) * GROUP)
        dt = dt_ref[rows, :]
        within = within_ref[rows, :]
        last = last_ref[g : g + 1, :]
        back = jnp.exp(within) * sums_ref[rows, 3 * heads : 4 * heads]
        fore = dt * jnp.exp(last - within) * sums_ref[rows, heads : 2 * heads]
        meet = jnp.exp(last) * inner[g : g + 1, :]
        for which in range(2):
            sums = cols_ref[rows, (which + 1) * heads : (which + 2) * heads]
            whole = sums[GROUP - 1 : GROUP, :]
            flow = jnp.sum(back * sums + fore * (whole - sums), axis=0, keepdims=True) + meet * whole
            if which == 0:
                flow_dt += flow
            else:
                flow_sl += flow
        bias += jnp.sum(slope_ref[rows, :] / dt * sums_ref[rows, 0:heads], axis=0, keepdims=True)
        skips += jnp.sum(sums_ref[rows, 2 * heads : 3 * heads], axis=0, keepdims=True)
    flows = flow_ref[0]
    for g in range(1, groups):
        flows = flows + flow_ref[g]
    totals = jnp.transpose(jnp.sum(flows, axis=1, keepdims=True) + jnp.zeros((2 * heads, 128), F32))[0:1, :]
    stat_ref[...] = jnp.zeros_like(stat_ref)
    stat_ref[0:1, 0:heads] = rate * (flow_dt + totals[:, 0:heads])
    stat_ref[1:2, 0:heads] = bias + rate * (flow_sl + totals[:, heads : 2 * heads])
    stat_ref[2:3, 0:heads] = skips


def flip(li, lt, block):
    def group(g, unused):
        at = pl.multiple_of(g * GROUP, GROUP)
        wide = 8 * block
        for q in range(li.shape[1] // wide):
            turned = jnp.transpose(li[pl.ds(at, GROUP), q * wide : (q + 1) * wide])
            for k in range(8):
                n = q * 8 + k
                lt[n % 2, (n // 2) * block : (n // 2 + 1) * block, pl.ds(at, GROUP)] = turned[
                    k * block : (k + 1) * block, :
                ]
        return unused

    lax.fori_loop(0, li.shape[0] // GROUP, group, 0)


def whole_kernel(refs_in, refs_out, s):
    x_hbm, dy_hbm, li_hbm, b_ref, c_ref, raw_ref, bias_ref, log_ref, skip_ref = refs_in
    wx_ref, wbc_ref, total_ref = refs_out
    block = wx_ref.shape[0]
    heads = raw_ref.shape[1]
    x, dy, li, dx, lt = s["x"], s["dy"], s["li"], s["dx"], s["lt"]
    work, got_sems = s["work"], s["core_sems"]
    chunks = work.shape[1]
    core = lax.axis_index("seq_2")
    mp = lax.axis_index("mp")
    other = {"seq_2": 1 - core}

    loads = []
    for n, (source, target) in enumerate(((x_hbm, x), (dy_hbm, dy), (li_hbm, li))):
        load = pltpu.make_async_copy(source, target, s["load_sems"].at[n])
        load.start()
        loads.append(load)

    carry = Carry(s["ends"], s["pair"], s["out"], s["got"], s["scanned"], s["back"], s["mine"], s["yours"],
                  s["carry"], s["gains"], s["pair_sems"], s["chip_sems"])
    partners = [other] + [carry.chip(k)[1] for k in range(1, 16)] + [around("mp", k) for k in (1, 2, 3)]
    barrier = pltpu.get_barrier_semaphore()
    for partner in partners:
        pl.semaphore_signal(barrier, inc=1, device_id=partner, device_id_type=MESH)

    scalars(raw_ref, bias_ref, log_ref, s["dt"], s["slope"], s["a"])
    s["mix"][:, GROUP // 2 : GROUP, 0 : GROUP // 2] = jnp.zeros((2, GROUP // 2, GROUP // 2), BF16)
    s["v"][:, GROUP // 2 : GROUP, 0 : GROUP // 2] = jnp.zeros((s["v"].shape[0], GROUP // 2, GROUP // 2), F32)
    s["inner"][...] = jnp.zeros_like(s["inner"])
    loads[0].wait()
    loads[1].wait()
    states(x, dy, b_ref, c_ref, s["dt"], s["slope"], s["a"], s["within"], s["last"], s["cols"], s["rows"],
           s["cross"], s["decay"], s["spread"], s["parts"], s["ends"])
    pl.semaphore_wait(barrier, len(partners))
    carry.give_pair()

    def intra_part(j):
        intra(j, x, dy, s["cols"], s["rows"], s["cross"], s["v"], s["mix"], dx, s["flow"], heads)

    def combine_part(j):
        combine(j, x, dy, b_ref, c_ref, s["dt"], s["within"], s["last"], s["decay"], s["spread"], skip_ref,
                s["parts"], s["carry"], s["sp"], s["gp"], dx, s["dbc"], s["sums"], s["inner"])

    carry.give_chips()
    loads[2].wait()
    flip(li, lt, block)
    intra_part(0)
    carry.scan()
    for j in range(1, min(3, chunks)):
        intra_part(j)
    carry.give_back()
    carry.finish()

    send_own, got, own = (work.at[i] for i in range(3))
    core_copies = {}

    def give(j):
        cols = dx[:, j * 256 : (j + 1) * 256]

        def body(i, unused):
            start = pl.multiple_of(i * 4 * block, 16)
            res = dot(lt[1 - core, pl.ds(start, 4 * block), :], cols)
            for side in range(2):
                send_own[j, side, i] = res[:, side * 128 : (side + 1) * 128].reshape(4, block, 128)
            return unused

        lax.fori_loop(0, 4, body, 0)
        core_copies[j] = remote(send_own.at[j], got.at[j], got_sems.at[0, j], got_sems.at[1, j], other)
        core_copies[j].start()

    def keep(j):
        core_copies[j].wait_recv()
        cols = dx[:, j * 256 : (j + 1) * 256]

        def body(i, unused):
            start = pl.multiple_of(i * 4 * block, 16)
            res = dot(lt[core, pl.ds(start, 4 * block), :], cols)
            for side in range(2):
                own[j, side, i] = got[j, side, i] + res[:, side * 128 : (side + 1) * 128].reshape(4, block, 128)
            return unused

        lax.fori_loop(0, 4, body, 0)

    w_work = s["w_work"]
    dbc_in, packed = s["dbc_in"], s["packed"]

    def narrow(kind, i, cols):
        start = pl.multiple_of(i * 4 * block, 16)
        res = dot(lt[kind, pl.ds(start, 4 * block), :], cols).reshape(4, block, 64)
        grads = jnp.concatenate([res[:, 0 : block // 2], res[:, block // 2 : block]], axis=2)
        stats = jnp.broadcast_to(s["stats"][...][None], (4, 8, 128))
        return jnp.concatenate([grads, stats], axis=1)

    mp_copies = []

    def give_mp():
        mixed_grads(b_ref, c_ref, s["v"], s["dbc"], packed)
        for k in (1, 2, 3):
            target = around("mp", k)
            copy = remote(packed.at[target["mp"]], dbc_in.at[k - 1], s["mp_sems"].at[0, k - 1],
                          s["mp_sems"].at[1, k - 1], target)
            copy.start()
            mp_copies.append(copy)
        statistics(s["dt"], s["slope"], log_ref, s["within"], s["last"], s["cols"], s["sums"], s["inner"],
                   s["flow"], s["stats"])

    def owned_cols():
        for copy in mp_copies:
            copy.wait_recv()
        owned = packed[mp] + dbc_in[0] + dbc_in[1] + dbc_in[2]
        return jnp.concatenate([owned[:, 0:64], owned[:, 64:128]], axis=0).astype(BF16)

    def give_narrow(cols):
        def body(i, unused):
            w_work[0, i] = narrow(1 - core, i, cols)
            return unused

        lax.fori_loop(0, 4, body, 0)
        core_copies[chunks] = remote(
            w_work.at[0], w_work.at[1], got_sems.at[0, chunks], got_sems.at[1, chunks], other
        )
        core_copies[chunks].start()

    def keep_narrow(cols):
        core_copies[chunks].wait_recv()

        def body(i, unused):
            w_work[2, i] = w_work[1, i] + narrow(core, i, cols)
            return unused

        lax.fori_loop(0, 4, body, 0)

    def store_wide(j, side):
        left = j * 256 + side * 128

        def store(half, value):
            wx_ref[half * (block // 2) : (half + 1) * (block // 2), left : left + 128] = value

        return store

    def store_narrow(half, value):
        w_work[0, 0, 0, half * (W_ROWS // 2) : (half + 1) * (W_ROWS // 2)] = value

    send, recv = s["ring_send"], s["ring_recv"]

    def stream(j, side):
        axes = ("seq_0", "seq_1") if side == 0 else ("seq_1", "seq_0")
        n = 2 * j + side
        return PlaneSum(*axes, side == 1, own.at[j, side], s["relay"].at[:, j, side], s["final"].at[:, j, side],
                        s["mid"].at[j, side], s["relay2"].at[:, j, side], s["final2"].at[:, j, side],
                        lambda k: send.at[n, k], lambda k: recv.at[n, k], store_wide(j, side))

    streams = [[stream(j, 0), stream(j, 1)] for j in range(chunks)]
    end = 2 * chunks
    streams.append([PlaneSum("seq_0", "seq_1", False, w_work.at[2], s["w_relay"], s["w_final"], s["w_mid"],
                             s["w_relay2"], s["w_final2"],
                             lambda k: send.at[end, k], lambda k: recv.at[end, k], store_narrow)])

    combine_part(0)
    give(0)
    cols_low = []
    for t in range(chunks + 6):
        if t + 1 < chunks:
            if t + 1 >= 3:
                intra_part(t + 1)
            combine_part(t + 1)
            give(t + 1)
        elif t + 1 == chunks:
            give_mp()
        if t < chunks:
            keep(t)
        if t + 1 == chunks:
            cols_low.append(owned_cols())
            give_narrow(cols_low[0])
        elif t == chunks:
            keep_narrow(cols_low[0])
        for stage in range(5):
            j = t - stage
            if 0 <= j <= chunks:
                if stage == 4 and j == chunks:
                    core_copies[chunks].wait_send()
                for one in streams[j]:
                    one.run(stage)

    half = block // 2
    wbc_ref[0:half, :] = w_work[0, 0, 0, 0:half, 0:64]
    wbc_ref[half:block, :] = w_work[0, 0, 0, 0:half, 64:128]
    total_ref[...] = w_work[0, 0, 0, half : half + 8, :]
    carry.drain()
    for copy in mp_copies:
        copy.wait_send()
    for j in range(chunks):
        core_copies[j].wait_send()
    for group in streams:
        for one in group:
            one.drain()


def scratch(tokens, heads, block, wide):
    width = heads * HEAD_DIM
    chunks = width // 256
    groups = tokens // GROUP
    half = STATE // 2
    dma = pltpu.SemaphoreType.DMA
    return {
        "x": VMEM((tokens, width), BF16), "dy": VMEM((tokens, width), BF16), "li": VMEM((tokens, wide), BF16),
        "dx": VMEM((tokens, width), BF16), "lt": VMEM((2, wide // 2, tokens), BF16),
        "dt": VMEM((tokens, heads), F32), "slope": VMEM((tokens, heads), F32), "a": VMEM((tokens, heads), F32),
        "within": VMEM((tokens, heads), F32), "last": VMEM((8, heads), F32), "cols": VMEM((tokens, 3 * heads), F32),
        "rows": VMEM((groups, 3 * heads, GROUP), F32), "cross": VMEM((groups, GROUP, GROUP), F32),
        "decay": VMEM((8, width), F32), "spread": VMEM((heads, width), BF16),
        "parts": VMEM((2 * groups - 2, STATE, width), F32), "ends": VMEM((2 * STATE, width + 128), F32),
        "pair": VMEM((2, half, width + 128), F32), "out": VMEM((16, 8, width + 128), F32),
        "got": VMEM((16, 8, width + 128), F32), "scanned": VMEM((16, 8, width), F32),
        "back": VMEM((16, 8, width), F32), "mine": VMEM((2, half, width), F32), "yours": VMEM((2, half, width), F32),
        "carry": VMEM((2 * STATE, width), F32), "gains": VMEM((32, width), F32),
        "v": VMEM((groups, GROUP, GROUP), F32), "mix": VMEM((2, GROUP, GROUP), BF16),
        "flow": VMEM((groups, 2 * heads, GROUP), F32), "sp": VMEM((groups, STATE, 256), F32),
        "gp": VMEM((groups, STATE, 256), F32), "dbc": VMEM((tokens, 2 * STATE), F32),
        "sums": VMEM((tokens, 128), F32), "inner": VMEM((8, width), F32), "stats": VMEM((8, 128), F32),
        "packed": VMEM((4, tokens // 2, 128), F32), "dbc_in": VMEM((3, tokens // 2, 128), F32),
        "work": VMEM((3, chunks, 2, 4, 4, block, 128), F32), "relay": VMEM((2, chunks, 2, 2, block, 128), F32),
        "final": VMEM((2, chunks, 2, 4, block, 128), F32), "mid": VMEM((chunks, 2, 4, block, 128), F32),
        "relay2": VMEM((2, chunks, 2, block // 2, 128), F32), "final2": VMEM((2, chunks, 2, block, 128), F32),
        "w_work": VMEM((3, 4, 4, W_ROWS, 128), F32), "w_relay": VMEM((2, 2, W_ROWS, 128), F32),
        "w_final": VMEM((2, 4, W_ROWS, 128), F32), "w_mid": VMEM((4, W_ROWS, 128), F32),
        "w_relay2": VMEM((2, W_ROWS // 2, 128), F32), "w_final2": VMEM((2, W_ROWS, 128), F32),
        "load_sems": dma((3,)), "pair_sems": dma((2, 3)), "chip_sems": dma((4, 16)),
        "core_sems": dma((2, chunks + 1)), "mp_sems": dma((2, 3)),
        "ring_send": dma((2 * chunks + 1, 12)), "ring_recv": dma((2 * chunks + 1, 12)),
    }


def on_device(layer_in, ssm_input, b_matrix, c_matrix, dt_raw, dt_bias, a_log, d_skip, grad_out):
    tokens, heads = dt_raw.shape
    wide = layer_in.shape[1]
    width = heads * HEAD_DIM
    block = wide // math.prod(lax.axis_size(axis) for axis in SEQ)
    sds = jax.ShapeDtypeStruct
    shapes = scratch(tokens, heads, block, wide)

    def kernel(*refs):
        whole_kernel(refs[:9], refs[9:12], dict(zip(shapes, refs[12:])))

    anywhere, local = pl.BlockSpec(memory_space=pl.ANY), pl.BlockSpec(memory_space=VMEM)
    grad_wx, grad_wbc, totals = pl.pallas_call(
        kernel,
        out_shape=(sds((block, width), F32), sds((block, 64), F32), sds((8, 128), F32)),
        in_specs=[anywhere] * 3 + [local] * 6,
        out_specs=(local,) * 3,
        scratch_shapes=list(shapes.values()),
        name="whole",
        cost_estimate=pl.CostEstimate(flops=4 * 10**10, bytes_accessed=10**7, transcendentals=0),
        compiler_params=pltpu.CompilerParams(
            collective_id=0, has_side_effects=True, vmem_limit_bytes=67043328
        ),
    )(ssm_input, grad_out, layer_in, b_matrix, c_matrix, dt_raw, dt_bias[None, :], a_log[None, :],
      jnp.repeat(d_skip, HEAD_DIM)[None, :])
    return (grad_wx, grad_wbc, totals[0, :heads], totals[1, :heads], totals[2, :heads])


def solution(mesh):
    n_seq, n_mp = mesh.shape["seq"], mesh.shape["mp"]
    split = Mesh(mesh.devices.reshape(n_seq // 8, 4, 2, n_mp), SEQ + ("mp",))
    in_specs = (
        P(SEQ, None),
        P(SEQ, "mp"),
        P(SEQ, None),
        P(SEQ, None),
        P(SEQ, "mp"),
        P("mp"),
        P("mp"),
        P("mp"),
        P(SEQ, "mp"),
    )
    out_specs = (P(SEQ, "mp"), P(SEQ, "mp"), P("mp"), P("mp"), P("mp"))
    return jax.shard_map(
        on_device, mesh=split, in_specs=in_specs, out_specs=out_specs, check_vma=False
    )
```

```python
import functools
import math

import jax
import jax.numpy as jnp
from jax import lax
from jax.experimental import pallas as pl
from jax.experimental.pallas import tpu as pltpu
from jax.sharding import Mesh
from jax.sharding import PartitionSpec as P

GROUP = 256
HEAD_DIM = 64
STATE = 128
LOG2E = 1.0 / math.log(2.0)
SEQ = ("seq_0", "seq_1", "seq_2")
F32 = jnp.float32
BF16 = jnp.bfloat16
VMEM = pltpu.VMEM


def dot(left, right):
    return jnp.dot(left, right, preferred_element_type=F32)


def dot_nt(left, right):
    return lax.dot_general(left, right, (((1,), (1,)), ((), ())), preferred_element_type=F32)


def dot_tn(left, right):
    return lax.dot_general(left, right, (((0,), (0,)), ((), ())), preferred_element_type=F32)


def dot_exact(left, right):
    return jnp.dot(left, right, preferred_element_type=F32, precision=lax.Precision.HIGHEST)


def lane_iota(shape, dim):
    return lax.broadcasted_iota(jnp.int32, shape, dim)


def spread_matrix(heads, dtype):
    rows = lane_iota((heads, heads * HEAD_DIM), 0)
    cols = lane_iota((heads, heads * HEAD_DIM), 1)
    inside = (cols >= rows * HEAD_DIM) & (cols < (rows + 1) * HEAD_DIM)
    return jnp.where(inside, 1.0, 0.0).astype(dtype)


def gather_matrix(heads, dtype):
    rows = lane_iota((heads * HEAD_DIM, heads), 0)
    cols = lane_iota((heads * HEAD_DIM, heads), 1)
    inside = (rows >= cols * HEAD_DIM) & (rows < (cols + 1) * HEAD_DIM)
    return jnp.where(inside, 1.0, 0.0).astype(dtype)


def lower_ones(size):
    return jnp.where(lane_iota((size, size), 0) >= lane_iota((size, size), 1), 1.0, 0.0)


def spread(values, matrix):
    high = values.astype(BF16)
    low = (values - high.astype(F32)).astype(BF16)
    return dot(high, matrix) + dot(low, matrix)


MESH = pl.DeviceIdType.MESH
W_ROWS = 48


def around(axis, shift):
    return {axis: lax.rem(lax.axis_index(axis) + shift, 4)}


def remote(source, target, send, recv, device):
    return pltpu.make_async_remote_copy(
        src_ref=source, dst_ref=target, send_sem=send, recv_sem=recv, device_id=device, device_id_type=MESH
    )


class RingSum:
    def __init__(self, axis, part, relay, final, send, recv, base):
        self.axis, self.part, self.relay, self.final = axis, part, relay, final
        self.send, self.recv, self.base = send, recv, base
        me = lax.axis_index(axis)
        self.me = me
        self.ahead, self.behind, self.across = (lax.rem(me + k, 4) for k in (1, 3, 2))
        self.up, self.down = around(axis, 1), around(axis, 3)
        self.copies = {}

    def copy(self, n, source, target, device):
        at = self.base + n
        self.copies[n] = remote(source, target, self.send(at), self.recv(at), device)
        self.copies[n].start()

    def first(self):
        self.copy(0, self.part(self.across, 0), self.relay(0), self.up)
        self.copy(1, self.part(self.across, 1), self.relay(1), self.down)
        self.copy(2, self.part(self.ahead, 1), self.final(0, 1), self.up)
        self.copy(3, self.part(self.behind, 0), self.final(1, 0), self.down)

    def second(self):
        self.copies[0].wait_recv()
        ahead = self.part(self.ahead, 0)
        ahead[...] += self.relay(0)[...]
        self.copy(4, ahead, self.final(0, 0), self.up)
        self.copies[1].wait_recv()
        behind = self.part(self.behind, 1)
        behind[...] += self.relay(1)[...]
        self.copy(5, behind, self.final(1, 1), self.down)

    def result(self, half):
        (self.copies[4] if half == 0 else self.copies[2]).wait_recv()
        (self.copies[3] if half == 0 else self.copies[5]).wait_recv()
        return self.part(self.me, half)[...] + self.final(0, half)[...] + self.final(1, half)[...]

    def drain(self):
        for copy in self.copies.values():
            copy.wait_send()


class PlaneSum:
    def __init__(self, first_axis, second_axis, swap, own, relay, final, mid, relay2, final2, send, recv, store):
        rows = mid.shape[1]
        self.store, self.mid, self.rows = store, mid, rows

        def part(d, half):
            pair = pl.ds(2 * half, 2)
            return own.at[pair, d] if swap else own.at[d, pair]

        def part2(d, half):
            return mid.at[d, pl.ds(half * (rows // 2), rows // 2)]

        self.one = RingSum(first_axis, part, lambda h: relay.at[h], lambda w, h: final.at[w, pl.ds(2 * h, 2)],
                           send, recv, 0)
        self.two = RingSum(second_axis, part2, lambda h: relay2.at[h],
                           lambda w, h: final2.at[w, pl.ds(h * (rows // 2), rows // 2)], send, recv, 6)

    def run(self, stage):
        if stage == 0:
            self.one.first()
        elif stage == 1:
            self.one.second()
        elif stage == 2:
            for half in range(2):
                self.mid[pl.ds(2 * half, 2)] = self.one.result(half)
            self.two.first()
        elif stage == 3:
            self.two.second()
        elif stage == 4:
            for half in range(2):
                self.store(half, self.two.result(half))

    def drain(self):
        self.one.drain()
        self.two.drain()


STRIP = 64


def scalars(raw_ref, bias_ref, log_ref, dt_ref, slope_ref, a_ref):
    shifted = jnp.transpose(raw_ref[...]) + bias_ref[...]
    small = jnp.exp(-jnp.abs(shifted))
    one = 1.0 + small
    log_one = jnp.where(one == 1.0, small, jnp.log(one) * small / jnp.where(one == 1.0, 1.0, one - 1.0))
    dt = jnp.maximum(shifted, 0.0) + log_one
    dt_ref[...] = dt
    slope_ref[...] = jnp.where(shifted >= 0.0, 1.0, small) / one
    a_ref[...] = dt * -jnp.exp(log_ref[...])


def states(x, dy, b_ref, c_ref, dt_ref, slope_ref, a_ref, within_ref, last_ref, cols_ref, rows_ref, cross_ref,
           decay_ref, spread_ref, parts, ends, tile, skip_ref, skip_wide):
    tokens, heads = dt_ref.shape
    groups = tokens // GROUP
    width = heads * HEAD_DIM
    tri = lower_ones(GROUP)
    spread_m = spread_matrix(heads, BF16)
    spread_ref[...] = spread_m
    spread_e = spread_matrix(heads, F32)
    skip_wide[...] = dot_exact(jnp.broadcast_to(skip_ref[...], (8, heads)), spread_e)
    block_end = jnp.zeros((1, heads), F32)
    for g in range(groups):
        rows = slice(g * GROUP, (g + 1) * GROUP)
        dt = dt_ref[rows, :]
        sums = dot_exact(tri, jnp.concatenate([a_ref[rows, :], dt, slope_ref[rows, :]], axis=1))
        within = sums[:, 0:heads]
        last = within[GROUP - 1 : GROUP, :]
        block_end = block_end + last
        within_ref[rows, :] = within
        last_ref[g : g + 1, :] = last
        decay = dot_exact(jnp.broadcast_to(jnp.exp(last), (8, heads)), spread_e)[0:1, :]
        decay_ref[g : g + 1, :] = decay
        fall = spread(dt * jnp.exp(last - within), spread_m)
        xw = (x[rows, :].astype(F32) * fall).astype(BF16)
        state = dot_tn(b_ref[rows, :], xw)
        rise = spread(jnp.exp(within), spread_m)
        yw = (dy[rows, :].astype(F32) * rise).astype(BF16)
        grad = dot_tn(c_ref[rows, :], yw)
        if g < groups - 1:
            parts[g] = state
        if g > 0:
            parts[groups - 2 + g] = grad
        if g == 0:
            ends[0:STATE, 0:width] = state
            ends[STATE : 2 * STATE, 0:width] = grad
            gain = decay
        else:
            ends[0:STATE, 0:width] = decay * ends[0:STATE, 0:width] + state
            ends[STATE : 2 * STATE, 0:width] = ends[STATE : 2 * STATE, 0:width] + gain * grad
            gain = gain * decay
        packed = jnp.concatenate([within * LOG2E - jnp.log2(dt), sums[:, heads : 3 * heads]], axis=1)
        cols_ref[rows, :] = packed
        rows_ref[g] = jnp.transpose(jnp.concatenate([within * LOG2E, sums[:, heads : 3 * heads]], axis=1))
        cross_ref[g] = dot_nt(b_ref[rows, :], c_ref[rows, :])
    pad = jnp.concatenate([jnp.exp(block_end), jnp.zeros((1, 128 - heads), F32)], axis=1)
    tile[...] = jnp.broadcast_to(pad, (8, 128))


class Decays:
    def __init__(self, tile, pair, chip_tile, got, gains, heads, sems):
        self.tile, self.pair, self.chip_tile, self.got, self.gains = tile, pair, chip_tile, got, gains
        self.heads, self.sems = heads, sems
        self.core = lax.axis_index("seq_2")
        self.me = lax.axis_index("seq_0") * 4 + lax.axis_index("seq_1")

    def chip(self, offset):
        index = lax.rem(self.me + offset, 16)
        return index, {"seq_0": index // 4, "seq_1": lax.rem(index, 4)}

    def spread_rows(self, tile):
        return dot_exact(tile[:, 0 : self.heads], spread_matrix(self.heads, F32))

    def give_pair(self):
        self.copies = [remote(self.tile, self.pair, self.sems.at[0, 0], self.sems.at[1, 0], {"seq_2": 1 - self.core})]
        self.copies[0].start()

    def give_chips(self):
        self.copies[0].wait_recv()
        first = self.core == 0
        mine, theirs = self.tile[...], self.pair[...]
        tile0, tile1 = jnp.where(first, mine, theirs), jnp.where(first, theirs, mine)
        self.chip_tile[...] = tile0 * tile1
        self.got[0] = tile0 * tile1
        for k in range(1, 16):
            copy = remote(self.chip_tile, self.got.at[k], self.sems.at[0, k], self.sems.at[1, k], self.chip(k)[1])
            copy.start()
            self.copies.append(copy)
        self.gains[0:8, :] = self.spread_rows(tile0)
        self.gains[8:16, :] = self.spread_rows(tile1)

    def take(self):
        for copy in self.copies[1:]:
            copy.wait_recv()
        self.gains[16:32, :] = self.spread_rows(self.got[:, 0, :])


class Carry:
    def __init__(self, decays, left, ends, carry, pair, out, got, scanned, back, mine, yours, core_sems, sems):
        self.ends, self.pair, self.out, self.got, self.scanned = ends, pair, out, got, scanned
        self.back, self.mine, self.yours, self.carry, self.gains = back, mine, yours, carry, decays.gains
        self.core_sems, self.sems, self.decays = core_sems, sems, decays
        self.core, self.me, self.chip = decays.core, decays.me, decays.chip
        self.other = {"seq_2": 1 - self.core}
        self.width = out.shape[2]
        self.cols = pl.ds(left, self.width)

    def own_rows(self, kind, core):
        return pl.ds(pl.multiple_of(kind * STATE + core * (STATE // 2), STATE // 2), STATE // 2)

    def gain(self, row):
        return self.gains[pl.ds(row, 1), self.cols]

    def give_pair(self):
        self.pair_copies = []
        for kind in range(2):
            copy = remote(self.ends.at[self.own_rows(kind, 1 - self.core), self.cols], self.pair.at[kind],
                          self.core_sems.at[0, kind], self.core_sems.at[1, kind], self.other)
            copy.start()
            self.pair_copies.append(copy)

    def both(self, kind):
        own = self.ends[self.own_rows(kind, self.core), self.cols]
        other = self.pair[kind]
        first = self.core == 0
        return jnp.where(first, own, other), jnp.where(first, other, own)

    def give_chips(self):
        for copy in self.pair_copies:
            copy.wait_recv()
        s0, s1 = self.both(0)
        self.out[0:8] = (self.gain(8) * s0 + s1).reshape(8, 8, self.width)
        g0, g1 = self.both(1)
        self.out[8:16] = (g0 + self.gain(0) * g1).reshape(8, 8, self.width)
        self.got[0] = self.out[self.me]
        self.copies = []
        for k in range(1, 16):
            index, device = self.chip(k)
            copy = remote(self.out.at[index], self.got.at[k], self.sems.at[0, k], self.sems.at[1, k], device)
            copy.start()
            self.copies.append(copy)

    def scan(self):
        for copy in self.copies:
            copy.wait_recv()
        backward = self.me >= 8

        def step(i, running):
            chip = jnp.where(backward, 15 - i, i)
            slot = lax.rem(self.me - chip + 16, 16)
            self.scanned[slot] = running
            return self.gain(16 + slot) * running + self.got[slot]

        lax.fori_loop(0, 16, step, jnp.zeros((8, self.width), F32))
        self.back[self.me] = self.scanned[0]
        self.back_copies = []
        for k in range(1, 16):
            index, device = self.chip(16 - k)
            copy = remote(self.scanned.at[k], self.back.at[self.me], self.sems.at[2, k], self.sems.at[3, k], device)
            copy.start()
            self.back_copies.append(copy)

    def give_back(self):
        half = STATE // 2
        for copy in self.back_copies:
            copy.wait_recv()
        first = self.core == 0
        s_in = self.back[0:8].reshape(half, self.width)
        s0, _ = self.both(0)
        s_next = self.gain(0) * s_in + s0
        self.mine[0] = jnp.where(first, s_next, s_in)
        g_in = self.back[8:16].reshape(half, self.width)
        _, g1 = self.both(1)
        g_before = g1 + self.gain(8) * g_in
        self.mine[1] = jnp.where(first, g_in, g_before)
        self.last = remote(self.mine, self.yours, self.core_sems.at[0, 2], self.core_sems.at[1, 2], self.other)
        self.last.start()
        self.carry[self.own_rows(0, self.core), self.cols] = jnp.where(first, s_in, s_next)
        self.carry[self.own_rows(1, self.core), self.cols] = jnp.where(first, g_before, g_in)

    def finish(self):
        self.last.wait_recv()
        for kind in range(2):
            self.carry[self.own_rows(kind, 1 - self.core), self.cols] = self.yours[kind]

    def drain(self):
        for copy in self.pair_copies + self.copies + self.back_copies + [self.last]:
            copy.wait_send()


def intra(j, x, dy, cols_ref, rows_ref, cross_ref, v_ref, mix_ref, gi, flow_ref, heads):
    half = GROUP // 2

    def group(g, unused):
        at = pl.multiple_of(g * GROUP, GROUP)
        for pair in range(2 * j, 2 * j + 2):
            zs, sides = [], []
            for sub in range(2):
                h = 2 * pair + sub
                lanes = slice(h * HEAD_DIM, (h + 1) * HEAD_DIM)
                x_h = x[pl.ds(at, GROUP), lanes]
                dy_h = dy[pl.ds(at, GROUP), lanes]
                top = dot_nt(x_h[0:half], dy_h)
                low = dot_nt(x_h[half:GROUP], dy_h[half:GROUP])
                acc = [jnp.zeros((8, GROUP), F32) for _ in range(3)]
                z_strips = []
                for k in range(GROUP // STRIP):
                    first = (k * STRIP // half) * half
                    wide = GROUP - first
                    rows = slice(k * STRIP, (k + 1) * STRIP)
                    here = pl.ds(at + k * STRIP, STRIP)
                    gap = rows_ref[g, h : h + 1, first:GROUP] - cols_ref[here, h : h + 1]
                    reach = lane_iota((STRIP, wide), 1) + first >= lane_iota((STRIP, wide), 0) + k * STRIP
                    decay = jnp.where(reach, jnp.exp2(gap), 0.0)
                    bc = cross_ref[g, rows, first:GROUP]
                    mix_ref[sub, rows, first:GROUP] = (decay * bc).astype(BF16)
                    z = decay * (top[rows, :] if first == 0 else low[k * STRIP - half : (k + 1) * STRIP - half, :])
                    z_strips.append(z)
                    box = z * bc
                    w_dt = cols_ref[here, heads + h : heads + h + 1]
                    w_sl = cols_ref[here, 2 * heads + h : 2 * heads + h + 1]
                    for n, term in enumerate((box, box * w_dt, box * w_sl)):
                        part = jnp.sum(term.reshape(STRIP // 8, 8, wide), axis=0)
                        if first > 0:
                            acc[n] = jnp.concatenate([acc[n][:, 0:first], acc[n][:, first:GROUP] + part], axis=1)
                        else:
                            acc[n] = acc[n] + part
                zs.append(z_strips)
                sides.append(dot(mix_ref[sub], dy_h))
                flow_dt = acc[0] * rows_ref[g, heads + h : heads + h + 1, :] - acc[1]
                flow_sl = acc[0] * rows_ref[g, 2 * heads + h : 2 * heads + h + 1, :] - acc[2]
                flow_ref[g, h : h + 1, :] = jnp.sum(flow_dt, axis=0, keepdims=True)
                flow_ref[g, heads + h : heads + h + 1, :] = jnp.sum(flow_sl, axis=0, keepdims=True)
            for k in range(GROUP // STRIP):
                first = (k * STRIP // half) * half
                rows = slice(k * STRIP, (k + 1) * STRIP)
                both = zs[0][k] + zs[1][k]
                if pair == 0:
                    v_ref[g, rows, first:GROUP] = both
                else:
                    v_ref[g, rows, first:GROUP] += both
            gi[pl.ds(at, GROUP), pair * 128 : (pair + 1) * 128] = jnp.concatenate(sides, axis=1).astype(BF16)
        return unused

    lax.fori_loop(0, x.shape[0] // GROUP, group, 0)


def combine(j, x, dy, b_ref, c_ref, dt_ref, within_ref, last_ref, decay_ref, spread_ref, skip_ref, parts, carry,
            sp_ref, gp_ref, dx, dbc, sums_ref, inner_ref):
    tokens, heads = dt_ref.shape
    groups = tokens // GROUP
    cols = slice(j * 256, (j + 1) * 256)
    sp_ref[0] = carry[0:STATE, cols]
    gp_ref[groups - 1] = carry[STATE : 2 * STATE, cols]
    for g in range(groups - 1):
        sp_ref[g + 1] = decay_ref[g : g + 1, cols] * sp_ref[g] + parts[g, :, cols]
    for g in range(groups - 1, 0, -1):
        gp_ref[g - 1] = parts[groups - 2 + g, :, cols] + decay_ref[g : g + 1, cols] * gp_ref[g]
    spread_m = spread_ref[:, cols]
    head = (lane_iota((256, 128), 0) + j * 256) // HEAD_DIM
    lane = lane_iota((256, 128), 1)

    def gather(k):
        return jnp.where(lane == head + k * heads, 1.0, 0.0).astype(BF16)

    for g in range(groups):
        rows = slice(g * GROUP, (g + 1) * GROUP)
        within = within_ref[rows, :]
        fall = spread(dt_ref[rows, :] * jnp.exp(last_ref[g : g + 1, :] - within), spread_m)
        rise = spread(jnp.exp(within), spread_m)
        xs = x[rows, cols].astype(F32)
        dys = dy[rows, cols].astype(F32)
        sp = sp_ref[g]
        gp = gp_ref[g]
        inner_ref[g : g + 1, cols] = jnp.sum(sp * gp, axis=0, keepdims=True)
        sp_low = sp.astype(BF16)
        gp_low = gp.astype(BF16)
        from_end = dot(b_ref[rows, :], gp_low)
        from_start = dot(c_ref[rows, :], sp_low)
        raw = dx[rows, cols].astype(F32) + fall * from_end
        total = dot((xs * raw).astype(BF16), gather(0))
        total += dot((xs * from_end).astype(BF16), gather(1))
        total += dot((xs * dys).astype(BF16), gather(2))
        total += dot((dys * from_start).astype(BF16), gather(3))
        dx[rows, cols] = (raw + skip_ref[0:1, cols] * dys).astype(BF16)
        d_b = dot_nt((xs * fall).astype(BF16), gp_low)
        d_c = dot_nt((dys * rise).astype(BF16), sp_low)
        if j == 0:
            sums_ref[rows, :] = total
            dbc[rows, 0:STATE] = d_b
            dbc[rows, STATE : 2 * STATE] = d_c
        else:
            sums_ref[rows, :] += total
            dbc[rows, 0:STATE] += d_b
            dbc[rows, STATE : 2 * STATE] += d_c


def mixed_grads(b_ref, c_ref, v_ref, dbc, packed):
    groups = v_ref.shape[0]
    for g in range(groups):
        rows = slice(g * GROUP, (g + 1) * GROUP)
        mixed = v_ref[g].astype(BF16)
        grads = (dbc[rows, 0:STATE] + dot(mixed, c_ref[rows, :]),
                 dbc[rows, STATE : 2 * STATE] + dot_tn(mixed, b_ref[rows, :]))
        for piece in range(GROUP // 128):
            at = g * (GROUP // 128) + piece
            side, base = divmod(at * 128, packed.shape[1])
            for m in range(packed.shape[0]):
                source, left = divmod(m * 64, STATE)
                packed[m, base : base + 128, side * 64 : side * 64 + 64] = grads[source][
                    piece * 128 : (piece + 1) * 128, left : left + 64
                ]


def statistics(dt_ref, slope_ref, log_ref, within_ref, last_ref, cols_ref, sums_ref, inner_ref, flow_ref, stat_ref):
    tokens, heads = dt_ref.shape
    groups = tokens // GROUP
    gather_e = gather_matrix(heads, F32)
    rate = -jnp.exp(log_ref[...])
    flow_dt = jnp.zeros((1, heads), F32)
    flow_sl = jnp.zeros((1, heads), F32)
    bias = jnp.zeros((1, heads), F32)
    skips = jnp.zeros((1, heads), F32)
    inner = dot_exact(inner_ref[...], gather_e)
    for g in range(groups):
        rows = slice(g * GROUP, (g + 1) * GROUP)
        dt = dt_ref[rows, :]
        within = within_ref[rows, :]
        last = last_ref[g : g + 1, :]
        back = jnp.exp(within) * sums_ref[rows, 3 * heads : 4 * heads]
        fore = dt * jnp.exp(last - within) * sums_ref[rows, heads : 2 * heads]
        meet = jnp.exp(last) * inner[g : g + 1, :]
        for which in range(2):
            sums = cols_ref[rows, (which + 1) * heads : (which + 2) * heads]
            whole = sums[GROUP - 1 : GROUP, :]
            flow = jnp.sum(back * sums + fore * (whole - sums), axis=0, keepdims=True) + meet * whole
            if which == 0:
                flow_dt += flow
            else:
                flow_sl += flow
        bias += jnp.sum(slope_ref[rows, :] / dt * sums_ref[rows, 0:heads], axis=0, keepdims=True)
        skips += jnp.sum(sums_ref[rows, 2 * heads : 3 * heads], axis=0, keepdims=True)
    flows = flow_ref[0]
    for g in range(1, groups):
        flows = flows + flow_ref[g]
    totals = jnp.transpose(jnp.sum(flows, axis=1, keepdims=True) + jnp.zeros((2 * heads, 128), F32))[0:1, :]
    stat_ref[...] = jnp.zeros_like(stat_ref)
    stat_ref[0:1, 0:heads] = rate * (flow_dt + totals[:, 0:heads])
    stat_ref[1:2, 0:heads] = bias + rate * (flow_sl + totals[:, heads : 2 * heads])
    stat_ref[2:3, 0:heads] = skips


def flip(li, lt, block):
    def group(g, unused):
        at = pl.multiple_of(g * GROUP, GROUP)
        wide = 8 * block
        for q in range(li.shape[1] // wide):
            turned = jnp.transpose(li[pl.ds(at, GROUP), q * wide : (q + 1) * wide])
            for k in range(8):
                n = q * 8 + k
                lt[n % 2, (n // 2) * block : (n // 2 + 1) * block, pl.ds(at, GROUP)] = turned[
                    k * block : (k + 1) * block, :
                ]
        return unused

    lax.fori_loop(0, li.shape[0] // GROUP, group, 0)


def whole_kernel(refs_in, refs_out, s):
    x_hbm, dy_hbm, li_hbm, b_ref, c_ref, raw_ref, bias_ref, log_ref, skip_ref = refs_in
    wx_ref, wbc_ref, total_ref = refs_out
    block = wx_ref.shape[0]
    heads = raw_ref.shape[0]
    x, dy, li, dx, lt = s["x"], s["dy"], s["li"], s["dx"], s["lt"]
    work, got_sems = s["work"], s["core_sems"]
    chunks = work.shape[1]
    core = lax.axis_index("seq_2")
    mp = lax.axis_index("mp")
    other = {"seq_2": 1 - core}

    loads = []
    for n, (source, target) in enumerate(((x_hbm, x), (dy_hbm, dy), (li_hbm, li))):
        load = pltpu.make_async_copy(source, target, s["load_sems"].at[n])
        load.start()
        loads.append(load)

    decays = Decays(s["tile"], s["tile_pair"], s["tile_chip"], s["tile_got"], s["gains"], heads, s["tile_sems"])
    carries = []
    for n, (left, right) in enumerate(parts_of(heads * HEAD_DIM)):
        buffers = [s[f"{name}{n}"] for name in ("pair", "out", "got", "scanned", "back", "mine", "yours")]
        carries.append(Carry(decays, left, s["ends"], s["carry"], *buffers, s["pair_sems"].at[n], s["chip_sems"].at[n]))
    partners = [other] + [decays.chip(k)[1] for k in range(1, 16)] + [around("mp", k) for k in (1, 2, 3)]
    barrier = pltpu.get_barrier_semaphore()
    for partner in partners:
        pl.semaphore_signal(barrier, inc=1, device_id=partner, device_id_type=MESH)

    scalars(raw_ref, bias_ref, log_ref, s["dt"], s["slope"], s["a"])
    s["mix"][:, GROUP // 2 : GROUP, 0 : GROUP // 2] = jnp.zeros((2, GROUP // 2, GROUP // 2), BF16)
    s["v"][:, GROUP // 2 : GROUP, 0 : GROUP // 2] = jnp.zeros((s["v"].shape[0], GROUP // 2, GROUP // 2), F32)
    s["inner"][...] = jnp.zeros_like(s["inner"])
    loads[0].wait()
    loads[1].wait()
    states(x, dy, b_ref, c_ref, s["dt"], s["slope"], s["a"], s["within"], s["last"], s["cols"], s["rows"],
           s["cross"], s["decay"], s["spread"], s["parts"], s["ends"], s["tile"], skip_ref, s["skip"])
    pl.semaphore_wait(barrier, len(partners))
    decays.give_pair()
    for one in carries:
        one.give_pair()

    def intra_part(j):
        intra(j, x, dy, s["cols"], s["rows"], s["cross"], s["v"], s["mix"], dx, s["flow"], heads)

    def combine_part(j):
        combine(j, x, dy, b_ref, c_ref, s["dt"], s["within"], s["last"], s["decay"], s["spread"], s["skip"],
                s["parts"], s["carry"], s["sp"], s["gp"], dx, s["dbc"], s["sums"], s["inner"])

    decays.give_chips()
    for one in carries:
        one.give_chips()
    loads[2].wait()
    flip(li, lt, block)
    decays.take()
    carries[0].scan()
    intra_part(0)
    carries[1].scan()
    intra_part(1)
    carries[0].give_back()

    send_own, got, own = (work.at[i] for i in range(3))
    core_copies = {}

    def give(j):
        cols = dx[:, j * 256 : (j + 1) * 256]

        def body(i, unused):
            start = pl.multiple_of(i * 4 * block, 16)
            res = dot(lt[1 - core, pl.ds(start, 4 * block), :], cols)
            for side in range(2):
                send_own[j, side, i] = res[:, side * 128 : (side + 1) * 128].reshape(4, block, 128)
            return unused

        lax.fori_loop(0, 4, body, 0)
        core_copies[j] = remote(send_own.at[j], got.at[j], got_sems.at[0, j], got_sems.at[1, j], other)
        core_copies[j].start()

    def keep(j):
        core_copies[j].wait_recv()
        cols = dx[:, j * 256 : (j + 1) * 256]

        def body(i, unused):
            start = pl.multiple_of(i * 4 * block, 16)
            res = dot(lt[core, pl.ds(start, 4 * block), :], cols)
            for side in range(2):
                own[j, side, i] = got[j, side, i] + res[:, side * 128 : (side + 1) * 128].reshape(4, block, 128)
            return unused

        lax.fori_loop(0, 4, body, 0)

    w_work = s["w_work"]
    dbc_in, packed = s["dbc_in"], s["packed"]

    def narrow(kind, i, cols):
        start = pl.multiple_of(i * 4 * block, 16)
        res = dot(lt[kind, pl.ds(start, 4 * block), :], cols).reshape(4, block, 64)
        grads = jnp.concatenate([res[:, 0 : block // 2], res[:, block // 2 : block]], axis=2)
        stats = jnp.broadcast_to(s["stats"][...][None], (4, 8, 128))
        return jnp.concatenate([grads, stats], axis=1)

    mp_copies = []

    def give_mp():
        mixed_grads(b_ref, c_ref, s["v"], s["dbc"], packed)
        for k in (1, 2, 3):
            target = around("mp", k)
            copy = remote(packed.at[target["mp"]], dbc_in.at[k - 1], s["mp_sems"].at[0, k - 1],
                          s["mp_sems"].at[1, k - 1], target)
            copy.start()
            mp_copies.append(copy)

    def owned_cols():
        for copy in mp_copies:
            copy.wait_recv()
        owned = packed[mp] + dbc_in[0] + dbc_in[1] + dbc_in[2]
        return jnp.concatenate([owned[:, 0:64], owned[:, 64:128]], axis=0).astype(BF16)

    def give_narrow(cols):
        def body(i, unused):
            w_work[0, i] = narrow(1 - core, i, cols)
            return unused

        lax.fori_loop(0, 4, body, 0)
        core_copies[chunks] = remote(
            w_work.at[0], w_work.at[1], got_sems.at[0, chunks], got_sems.at[1, chunks], other
        )
        core_copies[chunks].start()

    def keep_narrow(cols):
        core_copies[chunks].wait_recv()

        def body(i, unused):
            w_work[2, i] = w_work[1, i] + narrow(core, i, cols)
            return unused

        lax.fori_loop(0, 4, body, 0)

    def store_wide(j, side):
        left = j * 256 + side * 128

        def store(half, value):
            wx_ref[half * (block // 2) : (half + 1) * (block // 2), left : left + 128] = value

        return store

    def store_narrow(half, value):
        w_work[0, 0, 0, half * (W_ROWS // 2) : (half + 1) * (W_ROWS // 2)] = value

    send, recv = s["ring_send"], s["ring_recv"]

    def stream(j, side):
        axes = ("seq_0", "seq_1") if side == 0 else ("seq_1", "seq_0")
        n = 2 * j + side
        return PlaneSum(*axes, side == 1, own.at[j, side], s["relay"].at[:, j, side], s["final"].at[:, j, side],
                        s["mid"].at[j, side], s["relay2"].at[:, j, side], s["final2"].at[:, j, side],
                        lambda k: send.at[n, k], lambda k: recv.at[n, k], store_wide(j, side))

    streams = [[stream(j, 0), stream(j, 1)] for j in range(chunks)]
    end = 2 * chunks
    streams.append([PlaneSum("seq_0", "seq_1", False, w_work.at[2], s["w_relay"], s["w_final"], s["w_mid"],
                             s["w_relay2"], s["w_final2"],
                             lambda k: send.at[end, k], lambda k: recv.at[end, k], store_narrow)])

    second = parts_of(heads * HEAD_DIM)[1][0] // 256
    carries[0].finish()
    combine_part(0)
    give(0)
    carries[1].give_back()
    cols_low = []
    for t in range(chunks + 5):
        if t + 1 < chunks:
            if t + 1 >= 2:
                intra_part(t + 1)
            if t + 1 == second:
                carries[1].finish()
            combine_part(t + 1)
            give(t + 1)
        if t < chunks:
            keep(t)
        if t == chunks:
            keep_narrow(cols_low[0])
        for stage in range(5):
            j = t - stage
            if 0 <= j <= chunks:
                if stage == 4 and j == chunks:
                    core_copies[chunks].wait_send()
                for one in streams[j]:
                    one.run(stage)
        if t == chunks - 2:
            give_mp()
        if t == chunks - 1:
            statistics(s["dt"], s["slope"], log_ref, s["within"], s["last"], s["cols"], s["sums"], s["inner"],
                       s["flow"], s["stats"])
            cols_low.append(owned_cols())
            give_narrow(cols_low[0])

    half = block // 2
    turned = jnp.transpose(w_work[0, 0, 0, 0:half, :])
    wbc_ref[...] = jnp.concatenate([turned[0:64], turned[64:128]], axis=1)
    total_ref[...] = w_work[0, 0, 0, half : half + 8, :]
    for one in carries:
        one.drain()
    for copy in decays.copies + mp_copies:
        copy.wait_send()
    for j in range(chunks):
        core_copies[j].wait_send()
    for group in streams:
        for one in group:
            one.drain()


def parts_of(width):
    cut = 2 * 256
    return ((0, cut), (cut, width))


def carry_buffers(width):
    found = {}
    for n, (left, right) in enumerate(parts_of(width)):
        wide = right - left
        for name in ("out", "got", "scanned", "back"):
            found[f"{name}{n}"] = VMEM((16, 8, wide), F32)
        for name in ("pair", "mine", "yours"):
            found[f"{name}{n}"] = VMEM((2, STATE // 2, wide), F32)
    return found


def finish_kernel(wx_in, wbc_in, totals, wx_ref, wbc_ref, log_ref, bias_ref, skip_ref):
    wx_ref[...] = wx_in[...]
    wbc_ref[...] = wbc_in[...]
    for n, ref in enumerate((log_ref, bias_ref, skip_ref)):
        ref[...] = totals[n : n + 1, 0 : ref.shape[1]]


def scratch(tokens, heads, block, wide):
    width = heads * HEAD_DIM
    chunks = width // 256
    groups = tokens // GROUP
    half = STATE // 2
    dma = pltpu.SemaphoreType.DMA
    return {
        "x": VMEM((tokens, width), BF16), "dy": VMEM((tokens, width), BF16), "li": VMEM((tokens, wide), BF16),
        "dx": VMEM((tokens, width), BF16), "lt": VMEM((2, wide // 2, tokens), BF16),
        "dt": VMEM((tokens, heads), F32), "slope": VMEM((tokens, heads), F32), "a": VMEM((tokens, heads), F32),
        "within": VMEM((tokens, heads), F32), "last": VMEM((8, heads), F32), "cols": VMEM((tokens, 3 * heads), F32),
        "rows": VMEM((groups, 3 * heads, GROUP), F32), "cross": VMEM((groups, GROUP, GROUP), F32),
        "decay": VMEM((8, width), F32), "spread": VMEM((heads, width), BF16),
        "parts": VMEM((2 * groups - 2, STATE, width), F32), "ends": VMEM((2 * STATE, width), F32),
        **carry_buffers(width), "tile": VMEM((8, 128), F32), "tile_pair": VMEM((8, 128), F32),
        "tile_chip": VMEM((8, 128), F32), "tile_got": VMEM((16, 8, 128), F32), "skip": VMEM((8, width), F32),
        "tile_sems": dma((2, 16)),
        "carry": VMEM((2 * STATE, width), F32), "gains": VMEM((32, width), F32),
        "v": VMEM((groups, GROUP, GROUP), F32), "mix": VMEM((2, GROUP, GROUP), BF16),
        "flow": VMEM((groups, 2 * heads, GROUP), F32), "sp": VMEM((groups, STATE, 256), F32),
        "gp": VMEM((groups, STATE, 256), F32), "dbc": VMEM((tokens, 2 * STATE), F32),
        "sums": VMEM((tokens, 128), F32), "inner": VMEM((8, width), F32), "stats": VMEM((8, 128), F32),
        "packed": VMEM((4, tokens // 2, 128), F32), "dbc_in": VMEM((3, tokens // 2, 128), F32),
        "work": VMEM((3, chunks, 2, 4, 4, block, 128), F32), "relay": VMEM((2, chunks, 2, 2, block, 128), F32),
        "final": VMEM((2, chunks, 2, 4, block, 128), F32), "mid": VMEM((chunks, 2, 4, block, 128), F32),
        "relay2": VMEM((2, chunks, 2, block // 2, 128), F32), "final2": VMEM((2, chunks, 2, block, 128), F32),
        "w_work": VMEM((3, 4, 4, W_ROWS, 128), F32), "w_relay": VMEM((2, 2, W_ROWS, 128), F32),
        "w_final": VMEM((2, 4, W_ROWS, 128), F32), "w_mid": VMEM((4, W_ROWS, 128), F32),
        "w_relay2": VMEM((2, W_ROWS // 2, 128), F32), "w_final2": VMEM((2, W_ROWS, 128), F32),
        "load_sems": dma((3,)), "pair_sems": dma((2, 2, 3)), "chip_sems": dma((2, 4, 16)),
        "core_sems": dma((2, chunks + 1)), "mp_sems": dma((2, 3)),
        "ring_send": dma((2 * chunks + 1, 12)), "ring_recv": dma((2 * chunks + 1, 12)),
    }


def on_device(layer_in, ssm_input, b_matrix, c_matrix, dt_raw, dt_bias, a_log, d_skip, grad_out):
    tokens, heads = dt_raw.shape
    wide = layer_in.shape[1]
    width = heads * HEAD_DIM
    block = wide // math.prod(lax.axis_size(axis) for axis in SEQ)
    sds = jax.ShapeDtypeStruct
    shapes = scratch(tokens, heads, block, wide)

    def kernel(*refs):
        whole_kernel(refs[:9], refs[9:12], dict(zip(shapes, refs[12:])))

    anywhere, local = pl.BlockSpec(memory_space=pl.ANY), pl.BlockSpec(memory_space=VMEM)
    grad_wx, grad_wbc, totals = pl.pallas_call(
        kernel,
        out_shape=(sds((block, width), F32), sds((64, block), F32), sds((8, 128), F32)),
        in_specs=[anywhere] * 3 + [local] * 6,
        out_specs=(local,) * 3,
        scratch_shapes=list(shapes.values()),
        name="whole",
        cost_estimate=pl.CostEstimate(flops=4 * 10**10, bytes_accessed=10**7, transcendentals=0),
        compiler_params=pltpu.CompilerParams(
            collective_id=0, has_side_effects=True, vmem_limit_bytes=67043328
        ),
    )(ssm_input, grad_out, layer_in, b_matrix, c_matrix, dt_raw.T, dt_bias[None, :], a_log[None, :],
      d_skip[None, :])
    grad_wx, grad_wbc, *rows = pl.pallas_call(
        finish_kernel,
        out_shape=(sds((block, width), F32), sds((64, block), F32)) + (sds((1, heads), F32),) * 3,
        name="finish",
        cost_estimate=pl.CostEstimate(flops=10**6, bytes_accessed=10**6, transcendentals=0),
    )(grad_wx, grad_wbc, totals)
    return (grad_wx, grad_wbc.T, *(row.reshape(heads) for row in rows))


def solution(mesh):
    n_seq, n_mp = mesh.shape["seq"], mesh.shape["mp"]
    split = Mesh(mesh.devices.reshape(n_seq // 8, 4, 2, n_mp), SEQ + ("mp",))
    in_specs = (
        P(SEQ, None),
        P(SEQ, "mp"),
        P(SEQ, None),
        P(SEQ, None),
        P(SEQ, "mp"),
        P("mp"),
        P("mp"),
        P("mp"),
        P(SEQ, "mp"),
    )
    out_specs = (P(SEQ, "mp"), P(SEQ, "mp"), P("mp"), P("mp"), P("mp"))
    return jax.shard_map(
        on_device, mesh=split, in_specs=in_specs, out_specs=out_specs, check_vma=False
    )
```

```python
import functools
import math

import jax
import jax.numpy as jnp
from jax import lax
from jax.experimental import pallas as pl
from jax.experimental.pallas import tpu as pltpu
from jax.sharding import Mesh
from jax.sharding import PartitionSpec as P

GROUP = 256
HEAD_DIM = 64
STATE = 128
LOG2E = 1.0 / math.log(2.0)
SEQ = ("seq_0", "seq_1", "seq_2")
F32 = jnp.float32
BF16 = jnp.bfloat16
VMEM = pltpu.VMEM


def dot(left, right):
    return jnp.dot(left, right, preferred_element_type=F32)


def dot_nt(left, right):
    return lax.dot_general(left, right, (((1,), (1,)), ((), ())), preferred_element_type=F32)


def dot_tn(left, right):
    return lax.dot_general(left, right, (((0,), (0,)), ((), ())), preferred_element_type=F32)


def dot_exact(left, right):
    return jnp.dot(left, right, preferred_element_type=F32, precision=lax.Precision.HIGHEST)


def lane_iota(shape, dim):
    return lax.broadcasted_iota(jnp.int32, shape, dim)


def spread_matrix(heads, dtype):
    rows = lane_iota((heads, heads * HEAD_DIM), 0)
    cols = lane_iota((heads, heads * HEAD_DIM), 1)
    inside = (cols >= rows * HEAD_DIM) & (cols < (rows + 1) * HEAD_DIM)
    return jnp.where(inside, 1.0, 0.0).astype(dtype)


def gather_matrix(heads, dtype):
    rows = lane_iota((heads * HEAD_DIM, heads), 0)
    cols = lane_iota((heads * HEAD_DIM, heads), 1)
    inside = (rows >= cols * HEAD_DIM) & (rows < (cols + 1) * HEAD_DIM)
    return jnp.where(inside, 1.0, 0.0).astype(dtype)


def lower_ones(size):
    return jnp.where(lane_iota((size, size), 0) >= lane_iota((size, size), 1), 1.0, 0.0)


def halves(values):
    high = values.astype(BF16)
    low = (values - high.astype(F32)).astype(BF16)
    return jnp.concatenate([high, low], axis=1)


def spread(first, second, matrix):
    rows = first.shape[0]
    wide = dot(jnp.concatenate([halves(first), halves(second)], axis=0), matrix)
    return wide[0:rows], wide[rows : 2 * rows]


MESH = pl.DeviceIdType.MESH
ORDER = (
    "F", "S0", "I0", "S1", "I1", "B0", "I2", "E0", "C0", "G0", "C1", "G1", "K0", "r00", "B1", "K1", "r10",
    "E1", "C2", "r01", "G2", "I3", "K2", "r20", "r11", "r02", "C3", "G3", "I4", "K3", "r30", "r21", "r12",
    "r03", "C4", "G4", "M", "P0", "T", "K4", "r40", "r31", "P1", "r22", "r13", "O", "g", "r41", "k", "r50",
    "r04", "r32", "r23", "r51", "r14", "r42", "r33", "r52", "r24", "r43", "r34", "r53", "r44", "r54",
)
W_ROWS = 48


def around(axis, shift):
    return {axis: lax.rem(lax.axis_index(axis) + shift, 4)}


def remote(source, target, send, recv, device):
    return pltpu.make_async_remote_copy(
        src_ref=source, dst_ref=target, send_sem=send, recv_sem=recv, device_id=device, device_id_type=MESH
    )


class RingSum:
    def __init__(self, axis, part, relay, final, send, recv, base):
        self.axis, self.part, self.relay, self.final = axis, part, relay, final
        self.send, self.recv, self.base = send, recv, base
        me = lax.axis_index(axis)
        self.me = me
        self.ahead, self.behind, self.across = (lax.rem(me + k, 4) for k in (1, 3, 2))
        self.up, self.down = around(axis, 1), around(axis, 3)
        self.copies = {}

    def copy(self, n, source, target, device):
        at = self.base + n
        self.copies[n] = remote(source, target, self.send(at), self.recv(at), device)
        self.copies[n].start()

    def first(self):
        self.copy(0, self.part(self.across, 0), self.relay(0), self.up)
        self.copy(1, self.part(self.across, 1), self.relay(1), self.down)
        self.copy(2, self.part(self.ahead, 1), self.final(0, 1), self.up)
        self.copy(3, self.part(self.behind, 0), self.final(1, 0), self.down)

    def second(self):
        self.copies[0].wait_recv()
        ahead = self.part(self.ahead, 0)
        ahead[...] += self.relay(0)[...]
        self.copy(4, ahead, self.final(0, 0), self.up)
        self.copies[1].wait_recv()
        behind = self.part(self.behind, 1)
        behind[...] += self.relay(1)[...]
        self.copy(5, behind, self.final(1, 1), self.down)

    def result(self, half):
        (self.copies[4] if half == 0 else self.copies[2]).wait_recv()
        (self.copies[3] if half == 0 else self.copies[5]).wait_recv()
        return self.part(self.me, half)[...] + self.final(0, half)[...] + self.final(1, half)[...]

    def drain(self):
        for copy in self.copies.values():
            copy.wait_send()


class PlaneSum:
    def __init__(self, first_axis, second_axis, swap, own, relay, final, mid, relay2, final2, send, recv, store):
        rows = mid.shape[1]
        self.store, self.mid, self.rows = store, mid, rows

        def part(d, half):
            pair = pl.ds(2 * half, 2)
            return own.at[pair, d] if swap else own.at[d, pair]

        def part2(d, half):
            return mid.at[d, pl.ds(half * (rows // 2), rows // 2)]

        self.one = RingSum(first_axis, part, lambda h: relay.at[h], lambda w, h: final.at[w, pl.ds(2 * h, 2)],
                           send, recv, 0)
        self.two = RingSum(second_axis, part2, lambda h: relay2.at[h],
                           lambda w, h: final2.at[w, pl.ds(h * (rows // 2), rows // 2)], send, recv, 6)

    def run(self, stage):
        if stage == 0:
            self.one.first()
        elif stage == 1:
            self.one.second()
        elif stage == 2:
            for half in range(2):
                self.mid[pl.ds(2 * half, 2)] = self.one.result(half)
            self.two.first()
        elif stage == 3:
            self.two.second()
        elif stage == 4:
            for half in range(2):
                self.store(half, self.two.result(half))

    def drain(self):
        self.one.drain()
        self.two.drain()


STRIP = 64


def scalars(raw_ref, bias_ref, log_ref, dt_ref, slope_ref, a_ref):
    shifted = jnp.transpose(raw_ref[...]) + bias_ref[...]
    small = jnp.exp(-jnp.abs(shifted))
    one = 1.0 + small
    log_one = jnp.where(one == 1.0, small, jnp.log(one) * small / jnp.where(one == 1.0, 1.0, one - 1.0))
    dt = jnp.maximum(shifted, 0.0) + log_one
    dt_ref[...] = dt
    slope_ref[...] = jnp.where(shifted >= 0.0, 1.0, small) / one
    a_ref[...] = dt * -jnp.exp(log_ref[...])


def states(x, dy, b_ref, c_ref, dt_ref, a_ref, within_ref, last_ref, decay_ref, spread_ref, parts, ends, tile):
    tokens, heads = dt_ref.shape
    groups = tokens // GROUP
    width = heads * HEAD_DIM
    tri = lower_ones(GROUP)
    once = spread_matrix(heads, F32)
    spread_m = jnp.concatenate([once, once], axis=0).astype(BF16)
    spread_ref[...] = spread_m
    spread_e = spread_matrix(heads, F32)
    block_end = jnp.zeros((1, heads), F32)
    for g in range(groups):
        rows = slice(g * GROUP, (g + 1) * GROUP)
        dt = dt_ref[rows, :]
        within = dot_exact(tri, a_ref[rows, :])
        last = within[GROUP - 1 : GROUP, :]
        block_end = block_end + last
        within_ref[rows, :] = within
        last_ref[g : g + 1, :] = last
        decay = dot_exact(jnp.broadcast_to(jnp.exp(last), (8, heads)), spread_e)[0:1, :]
        decay_ref[g : g + 1, :] = decay
        fall, rise = spread(dt * jnp.exp(last - within), jnp.exp(within), spread_m)
        xw = (x[rows, :].astype(F32) * fall).astype(BF16)
        state = dot_tn(b_ref[rows, :], xw)
        yw = (dy[rows, :].astype(F32) * rise).astype(BF16)
        grad = dot_tn(c_ref[rows, :], yw)
        if g < groups - 1:
            parts[g] = state
        if g > 0:
            parts[groups - 2 + g] = grad
        if g == 0:
            ends[0:STATE, 0:width] = state
            ends[STATE : 2 * STATE, 0:width] = grad
            gain = decay
        else:
            ends[0:STATE, 0:width] = decay * ends[0:STATE, 0:width] + state
            ends[STATE : 2 * STATE, 0:width] = ends[STATE : 2 * STATE, 0:width] + gain * grad
            gain = gain * decay
    pad = jnp.concatenate([jnp.exp(block_end), jnp.zeros((1, 128 - heads), F32)], axis=1)
    tile[...] = jnp.broadcast_to(pad, (8, 128))


def tables(b_ref, c_ref, dt_ref, slope_ref, within_ref, cols_ref, rows_ref, cross_ref, skip_ref, skip_wide):
    tokens, heads = dt_ref.shape
    tri = lower_ones(GROUP)
    skip_wide[...] = dot_exact(jnp.broadcast_to(skip_ref[...], (8, heads)), spread_matrix(heads, F32))
    for g in range(tokens // GROUP):
        rows = slice(g * GROUP, (g + 1) * GROUP)
        dt = dt_ref[rows, :]
        rise2 = within_ref[rows, :] * LOG2E
        sums = dot_exact(tri, jnp.concatenate([dt, slope_ref[rows, :]], axis=1))
        cols_ref[rows, :] = jnp.concatenate([rise2 - jnp.log2(dt), sums], axis=1)
        rows_ref[g] = jnp.transpose(jnp.concatenate([rise2, sums], axis=1))
        cross_ref[g] = dot_nt(b_ref[rows, :], c_ref[rows, :])


class Decays:
    def __init__(self, tile, pair, chip_tile, got, gains, heads, sems):
        self.tile, self.pair, self.chip_tile, self.got, self.gains = tile, pair, chip_tile, got, gains
        self.heads, self.sems = heads, sems
        self.core = lax.axis_index("seq_2")
        self.me = lax.axis_index("seq_0") * 4 + lax.axis_index("seq_1")

    def chip(self, offset):
        index = lax.rem(self.me + offset, 16)
        return index, {"seq_0": index // 4, "seq_1": lax.rem(index, 4)}

    def spread_rows(self, tile):
        return dot_exact(tile[:, 0 : self.heads], spread_matrix(self.heads, F32))

    def give_pair(self):
        self.copies = [remote(self.tile, self.pair, self.sems.at[0, 0], self.sems.at[1, 0], {"seq_2": 1 - self.core})]
        self.copies[0].start()

    def give_chips(self):
        self.copies[0].wait_recv()
        first = self.core == 0
        mine, theirs = self.tile[...], self.pair[...]
        tile0, tile1 = jnp.where(first, mine, theirs), jnp.where(first, theirs, mine)
        self.chip_tile[...] = tile0 * tile1
        self.got[0] = tile0 * tile1
        for k in range(1, 16):
            copy = remote(self.chip_tile, self.got.at[k], self.sems.at[0, k], self.sems.at[1, k], self.chip(k)[1])
            copy.start()
            self.copies.append(copy)
        self.gains[0:8, :] = self.spread_rows(tile0)
        self.gains[8:16, :] = self.spread_rows(tile1)

    def take(self):
        for copy in self.copies[1:]:
            copy.wait_recv()
        self.gains[16:32, :] = self.spread_rows(self.got[:, 0, :])


class Carry:
    def __init__(self, decays, left, ends, carry, pair, out, got, scanned, back, mine, yours, core_sems, sems):
        self.ends, self.pair, self.out, self.got, self.scanned = ends, pair, out, got, scanned
        self.back, self.mine, self.yours, self.carry, self.gains = back, mine, yours, carry, decays.gains
        self.core_sems, self.sems, self.decays = core_sems, sems, decays
        self.core, self.me, self.chip = decays.core, decays.me, decays.chip
        self.other = {"seq_2": 1 - self.core}
        self.width = out.shape[2]
        self.cols = pl.ds(left, self.width)

    def own_rows(self, kind, core):
        return pl.ds(pl.multiple_of(kind * STATE + core * (STATE // 2), STATE // 2), STATE // 2)

    def gain(self, row):
        return self.gains[pl.ds(row, 1), self.cols]

    def give_pair(self):
        self.pair_copies = []
        for kind in range(2):
            copy = remote(self.ends.at[self.own_rows(kind, 1 - self.core), self.cols], self.pair.at[kind],
                          self.core_sems.at[0, kind], self.core_sems.at[1, kind], self.other)
            copy.start()
            self.pair_copies.append(copy)

    def both(self, kind):
        own = self.ends[self.own_rows(kind, self.core), self.cols]
        other = self.pair[kind]
        first = self.core == 0
        return jnp.where(first, own, other), jnp.where(first, other, own)

    def give_chips(self):
        for copy in self.pair_copies:
            copy.wait_recv()
        s0, s1 = self.both(0)
        self.out[0:8] = (self.gain(8) * s0 + s1).reshape(8, 8, self.width)
        g0, g1 = self.both(1)
        self.out[8:16] = (g0 + self.gain(0) * g1).reshape(8, 8, self.width)
        self.got[0] = self.out[self.me]
        self.copies = []
        for k in range(1, 16):
            index, device = self.chip(k)
            copy = remote(self.out.at[index], self.got.at[k], self.sems.at[0, k], self.sems.at[1, k], device)
            copy.start()
            self.copies.append(copy)

    def scan(self):
        for copy in self.copies:
            copy.wait_recv()
        backward = self.me >= 8

        def step(i, running):
            chip = jnp.where(backward, 15 - i, i)
            slot = lax.rem(self.me - chip + 16, 16)
            self.scanned[slot] = running
            return self.gain(16 + slot) * running + self.got[slot]

        lax.fori_loop(0, 16, step, jnp.zeros((8, self.width), F32))
        self.back[self.me] = self.scanned[0]
        self.back_copies = []
        for k in range(1, 16):
            index, device = self.chip(16 - k)
            copy = remote(self.scanned.at[k], self.back.at[self.me], self.sems.at[2, k], self.sems.at[3, k], device)
            copy.start()
            self.back_copies.append(copy)

    def give_back(self):
        half = STATE // 2
        for copy in self.back_copies:
            copy.wait_recv()
        first = self.core == 0
        s_in = self.back[0:8].reshape(half, self.width)
        s0, _ = self.both(0)
        s_next = self.gain(0) * s_in + s0
        self.mine[0] = jnp.where(first, s_next, s_in)
        g_in = self.back[8:16].reshape(half, self.width)
        _, g1 = self.both(1)
        g_before = g1 + self.gain(8) * g_in
        self.mine[1] = jnp.where(first, g_in, g_before)
        self.last = remote(self.mine, self.yours, self.core_sems.at[0, 2], self.core_sems.at[1, 2], self.other)
        self.last.start()
        self.carry[self.own_rows(0, self.core), self.cols] = jnp.where(first, s_in, s_next)
        self.carry[self.own_rows(1, self.core), self.cols] = jnp.where(first, g_before, g_in)

    def finish(self):
        self.last.wait_recv()
        for kind in range(2):
            self.carry[self.own_rows(kind, 1 - self.core), self.cols] = self.yours[kind]

    def drain(self):
        for copy in self.pair_copies + self.copies + self.back_copies + [self.last]:
            copy.wait_send()


def intra(j, x, dy, cols_ref, rows_ref, cross_ref, v_ref, mix_ref, gi, flow_ref, heads):
    half = GROUP // 2

    def group(g, unused):
        at = pl.multiple_of(g * GROUP, GROUP)
        for pair in range(2 * j, 2 * j + 2):
            zs, sides = [], []
            for sub in range(2):
                h = 2 * pair + sub
                lanes = slice(h * HEAD_DIM, (h + 1) * HEAD_DIM)
                x_h = x[pl.ds(at, GROUP), lanes]
                dy_h = dy[pl.ds(at, GROUP), lanes]
                top = dot_nt(x_h[0:half], dy_h)
                low = dot_nt(x_h[half:GROUP], dy_h[half:GROUP])
                acc = [jnp.zeros((8, GROUP), F32) for _ in range(3)]
                z_strips = []
                for k in range(GROUP // STRIP):
                    first = (k * STRIP // half) * half
                    wide = GROUP - first
                    rows = slice(k * STRIP, (k + 1) * STRIP)
                    here = pl.ds(at + k * STRIP, STRIP)
                    gap = rows_ref[g, h : h + 1, first:GROUP] - cols_ref[here, h : h + 1]
                    reach = lane_iota((STRIP, wide), 1) + first >= lane_iota((STRIP, wide), 0) + k * STRIP
                    decay = jnp.where(reach, jnp.exp2(gap), 0.0)
                    bc = cross_ref[g, rows, first:GROUP]
                    mix_ref[sub, rows, first:GROUP] = (decay * bc).astype(BF16)
                    z = decay * (top[rows, :] if first == 0 else low[k * STRIP - half : (k + 1) * STRIP - half, :])
                    z_strips.append(z)
                    box = z * bc
                    w_dt = cols_ref[here, heads + h : heads + h + 1]
                    w_sl = cols_ref[here, 2 * heads + h : 2 * heads + h + 1]
                    for n, term in enumerate((box, box * w_dt, box * w_sl)):
                        part = jnp.sum(term.reshape(STRIP // 8, 8, wide), axis=0)
                        if first > 0:
                            acc[n] = jnp.concatenate([acc[n][:, 0:first], acc[n][:, first:GROUP] + part], axis=1)
                        else:
                            acc[n] = acc[n] + part
                zs.append(z_strips)
                sides.append(dot(mix_ref[sub], dy_h))
                flow_dt = acc[0] * rows_ref[g, heads + h : heads + h + 1, :] - acc[1]
                flow_sl = acc[0] * rows_ref[g, 2 * heads + h : 2 * heads + h + 1, :] - acc[2]
                flow_ref[g, h : h + 1, :] = jnp.sum(flow_dt, axis=0, keepdims=True)
                flow_ref[g, heads + h : heads + h + 1, :] = jnp.sum(flow_sl, axis=0, keepdims=True)
            for k in range(GROUP // STRIP):
                first = (k * STRIP // half) * half
                rows = slice(k * STRIP, (k + 1) * STRIP)
                both = zs[0][k] + zs[1][k]
                if pair == 0:
                    v_ref[g, rows, first:GROUP] = both
                else:
                    v_ref[g, rows, first:GROUP] += both
            gi[pl.ds(at, GROUP), pair * 128 : (pair + 1) * 128] = jnp.concatenate(sides, axis=1).astype(BF16)
        return unused

    lax.fori_loop(0, x.shape[0] // GROUP, group, 0)


def combine(j, x, dy, b_ref, c_ref, dt_ref, within_ref, last_ref, decay_ref, spread_ref, skip_ref, parts, carry,
            sp_ref, gp_ref, dx, dbc, sums_ref, inner_ref):
    tokens, heads = dt_ref.shape
    groups = tokens // GROUP
    cols = slice(j * 256, (j + 1) * 256)
    sp_ref[0] = carry[0:STATE, cols]
    gp_ref[groups - 1] = carry[STATE : 2 * STATE, cols]
    for g in range(groups - 1):
        sp_ref[g + 1] = decay_ref[g : g + 1, cols] * sp_ref[g] + parts[g, :, cols]
    for g in range(groups - 1, 0, -1):
        gp_ref[g - 1] = parts[groups - 2 + g, :, cols] + decay_ref[g : g + 1, cols] * gp_ref[g]
    spread_m = spread_ref[:, cols]
    head = (lane_iota((256, 128), 0) + j * 256) // HEAD_DIM
    lane = lane_iota((256, 128), 1)

    def gather(k):
        return jnp.where(lane == head + k * heads, 1.0, 0.0).astype(BF16)

    for g in range(groups):
        rows = slice(g * GROUP, (g + 1) * GROUP)
        within = within_ref[rows, :]
        fall, rise = spread(dt_ref[rows, :] * jnp.exp(last_ref[g : g + 1, :] - within), jnp.exp(within), spread_m)
        xs = x[rows, cols].astype(F32)
        dys = dy[rows, cols].astype(F32)
        sp = sp_ref[g]
        gp = gp_ref[g]
        inner_ref[g : g + 1, cols] = jnp.sum(sp * gp, axis=0, keepdims=True)
        sp_low = sp.astype(BF16)
        gp_low = gp.astype(BF16)
        from_end = dot(b_ref[rows, :], gp_low)
        from_start = dot(c_ref[rows, :], sp_low)
        raw = dx[rows, cols].astype(F32) + fall * from_end
        total = dot((xs * raw).astype(BF16), gather(0))
        total += dot((xs * from_end).astype(BF16), gather(1))
        total += dot((xs * dys).astype(BF16), gather(2))
        total += dot((dys * from_start).astype(BF16), gather(3))
        dx[rows, cols] = (raw + skip_ref[0:1, cols] * dys).astype(BF16)
        d_b = dot_nt((xs * fall).astype(BF16), gp_low)
        d_c = dot_nt((dys * rise).astype(BF16), sp_low)
        if j == 0:
            sums_ref[rows, :] = total
            dbc[rows, 0:STATE] = d_b
            dbc[rows, STATE : 2 * STATE] = d_c
        else:
            sums_ref[rows, :] += total
            dbc[rows, 0:STATE] += d_b
            dbc[rows, STATE : 2 * STATE] += d_c


def mixed_grads(b_ref, c_ref, v_ref, dbc, packed):
    groups = v_ref.shape[0]
    for g in range(groups):
        rows = slice(g * GROUP, (g + 1) * GROUP)
        mixed = v_ref[g].astype(BF16)
        grads = (dbc[rows, 0:STATE] + dot(mixed, c_ref[rows, :]),
                 dbc[rows, STATE : 2 * STATE] + dot_tn(mixed, b_ref[rows, :]))
        for piece in range(GROUP // 128):
            at = g * (GROUP // 128) + piece
            side, base = divmod(at * 128, packed.shape[1])
            for m in range(packed.shape[0]):
                source, left = divmod(m * 64, STATE)
                packed[m, base : base + 128, side * 64 : side * 64 + 64] = grads[source][
                    piece * 128 : (piece + 1) * 128, left : left + 64
                ]


def statistics(dt_ref, slope_ref, log_ref, within_ref, last_ref, cols_ref, sums_ref, inner_ref, flow_ref, stat_ref):
    tokens, heads = dt_ref.shape
    groups = tokens // GROUP
    gather_e = gather_matrix(heads, F32)
    rate = -jnp.exp(log_ref[...])
    flow_dt = jnp.zeros((1, heads), F32)
    flow_sl = jnp.zeros((1, heads), F32)
    bias = jnp.zeros((1, heads), F32)
    skips = jnp.zeros((1, heads), F32)
    inner = dot_exact(inner_ref[...], gather_e)
    for g in range(groups):
        rows = slice(g * GROUP, (g + 1) * GROUP)
        dt = dt_ref[rows, :]
        within = within_ref[rows, :]
        last = last_ref[g : g + 1, :]
        back = jnp.exp(within) * sums_ref[rows, 3 * heads : 4 * heads]
        fore = dt * jnp.exp(last - within) * sums_ref[rows, heads : 2 * heads]
        meet = jnp.exp(last) * inner[g : g + 1, :]
        for which in range(2):
            sums = cols_ref[rows, (which + 1) * heads : (which + 2) * heads]
            whole = sums[GROUP - 1 : GROUP, :]
            flow = jnp.sum(back * sums + fore * (whole - sums), axis=0, keepdims=True) + meet * whole
            if which == 0:
                flow_dt += flow
            else:
                flow_sl += flow
        bias += jnp.sum(slope_ref[rows, :] / dt * sums_ref[rows, 0:heads], axis=0, keepdims=True)
        skips += jnp.sum(sums_ref[rows, 2 * heads : 3 * heads], axis=0, keepdims=True)
    flows = flow_ref[0]
    for g in range(1, groups):
        flows = flows + flow_ref[g]
    totals = jnp.transpose(jnp.sum(flows, axis=1, keepdims=True) + jnp.zeros((2 * heads, 128), F32))[0:1, :]
    stat_ref[...] = jnp.zeros_like(stat_ref)
    stat_ref[0:1, 0:heads] = rate * (flow_dt + totals[:, 0:heads])
    stat_ref[1:2, 0:heads] = bias + rate * (flow_sl + totals[:, heads : 2 * heads])
    stat_ref[2:3, 0:heads] = skips


def flip(li, lt, block):
    def group(g, unused):
        at = pl.multiple_of(g * GROUP, GROUP)
        wide = 8 * block
        for q in range(li.shape[1] // wide):
            turned = jnp.transpose(li[pl.ds(at, GROUP), q * wide : (q + 1) * wide])
            for k in range(8):
                n = q * 8 + k
                lt[n % 2, (n // 2) * block : (n // 2 + 1) * block, pl.ds(at, GROUP)] = turned[
                    k * block : (k + 1) * block, :
                ]
        return unused

    lax.fori_loop(0, li.shape[0] // GROUP, group, 0)


def whole_kernel(refs_in, refs_out, s):
    x_hbm, dy_hbm, li_hbm, b_ref, c_ref, raw_ref, bias_ref, log_ref, skip_ref = refs_in
    wx_ref, wbc_ref, total_ref = refs_out
    block = wx_ref.shape[0]
    heads = raw_ref.shape[0]
    x, dy, li, dx, lt = s["x"], s["dy"], s["li"], s["dx"], s["lt"]
    work, got_sems = s["work"], s["core_sems"]
    chunks = work.shape[1]
    core = lax.axis_index("seq_2")
    mp = lax.axis_index("mp")
    other = {"seq_2": 1 - core}

    loads = []
    for n, (source, target) in enumerate(((x_hbm, x), (dy_hbm, dy), (li_hbm, li))):
        load = pltpu.make_async_copy(source, target, s["load_sems"].at[n])
        load.start()
        loads.append(load)

    decays = Decays(s["tile"], s["tile_pair"], s["tile_chip"], s["tile_got"], s["gains"], heads, s["tile_sems"])
    carries = []
    for n, (left, right) in enumerate(parts_of(heads * HEAD_DIM)):
        buffers = [s[f"{name}{n}"] for name in ("pair", "out", "got", "scanned", "back", "mine", "yours")]
        carries.append(Carry(decays, left, s["ends"], s["carry"], *buffers, s["pair_sems"].at[n], s["chip_sems"].at[n]))
    partners = [other] + [decays.chip(k)[1] for k in range(1, 16)] + [around("mp", k) for k in (1, 2, 3)]
    barrier = pltpu.get_barrier_semaphore()
    for partner in partners:
        pl.semaphore_signal(barrier, inc=1, device_id=partner, device_id_type=MESH)

    scalars(raw_ref, bias_ref, log_ref, s["dt"], s["slope"], s["a"])
    loads[0].wait()
    loads[1].wait()
    states(x, dy, b_ref, c_ref, s["dt"], s["a"], s["within"], s["last"], s["decay"], s["spread"], s["parts"],
           s["ends"], s["tile"])
    pl.semaphore_wait(barrier, len(partners))
    decays.give_pair()
    for one in carries:
        one.give_pair()

    def intra_part(j):
        intra(j, x, dy, s["cols"], s["rows"], s["cross"], s["v"], s["mix"], dx, s["flow"], heads)

    def combine_part(j):
        combine(j, x, dy, b_ref, c_ref, s["dt"], s["within"], s["last"], s["decay"], s["spread"], s["skip"],
                s["parts"], s["carry"], s["sp"], s["gp"], dx, s["dbc"], s["sums"], s["inner"])

    decays.give_chips()
    for one in carries:
        one.give_chips()
    loads[2].wait()
    send_own, got, own = (work.at[i] for i in range(3))
    core_copies = {}

    def give(j):
        cols = dx[:, j * 256 : (j + 1) * 256]

        def body(i, unused):
            start = pl.multiple_of(i * 8 * block, 16)
            res = dot(lt[1 - core, pl.ds(start, 8 * block), :], cols)
            for side in range(2):
                send_own[j, side, pl.ds(2 * i, 2)] = res[:, side * 128 : (side + 1) * 128].reshape(2, 4, block, 128)
            return unused

        lax.fori_loop(0, 2, body, 0)
        core_copies[j] = remote(send_own.at[j], got.at[j], got_sems.at[0, j], got_sems.at[1, j], other)
        core_copies[j].start()

    def keep(j):
        core_copies[j].wait_recv()
        cols = dx[:, j * 256 : (j + 1) * 256]

        def body(i, unused):
            start = pl.multiple_of(i * 8 * block, 16)
            res = dot(lt[core, pl.ds(start, 8 * block), :], cols)
            for side in range(2):
                part = res[:, side * 128 : (side + 1) * 128].reshape(2, 4, block, 128)
                own[j, side, pl.ds(2 * i, 2)] = got[j, side, pl.ds(2 * i, 2)] + part
            return unused

        lax.fori_loop(0, 2, body, 0)

    w_work = s["w_work"]
    dbc_in, packed = s["dbc_in"], s["packed"]

    def narrow(kind, i, cols):
        start = pl.multiple_of(i * 4 * block, 16)
        res = dot(lt[kind, pl.ds(start, 4 * block), :], cols).reshape(4, block, 64)
        grads = jnp.concatenate([res[:, 0 : block // 2], res[:, block // 2 : block]], axis=2)
        stats = jnp.broadcast_to(s["stats"][...][None], (4, 8, 128))
        return jnp.concatenate([grads, stats], axis=1)

    quarter = packed.shape[1] // 2
    mp_ring = RingSum("mp", lambda d, h: packed.at[d, pl.ds(h * quarter, quarter)], lambda h: s["mp_relay"].at[h],
                      lambda w, h: dbc_in.at[w, pl.ds(h * quarter, quarter)],
                      lambda k: s["mp_sems"].at[0, k], lambda k: s["mp_sems"].at[1, k], 0)

    def owned_cols():
        owned = jnp.concatenate([mp_ring.result(0), mp_ring.result(1)], axis=0)
        return jnp.concatenate([owned[:, 0:64], owned[:, 64:128]], axis=0).astype(BF16)

    def give_narrow(cols):
        def body(i, unused):
            w_work[0, i] = narrow(1 - core, i, cols)
            return unused

        lax.fori_loop(0, 4, body, 0)
        core_copies[chunks] = remote(
            w_work.at[0], w_work.at[1], got_sems.at[0, chunks], got_sems.at[1, chunks], other
        )
        core_copies[chunks].start()

    def keep_narrow(cols):
        core_copies[chunks].wait_recv()

        def body(i, unused):
            w_work[2, i] = w_work[1, i] + narrow(core, i, cols)
            return unused

        lax.fori_loop(0, 4, body, 0)

    def store_wide(j, side):
        left = j * 256 + side * 128

        def store(half, value):
            wx_ref[half * (block // 2) : (half + 1) * (block // 2), left : left + 128] = value

        return store

    def store_narrow(half, value):
        w_work[0, 0, 0, half * (W_ROWS // 2) : (half + 1) * (W_ROWS // 2)] = value

    send, recv = s["ring_send"], s["ring_recv"]

    def stream(j, side):
        axes = ("seq_0", "seq_1") if side == 0 else ("seq_1", "seq_0")
        n = 2 * j + side
        return PlaneSum(*axes, side == 1, own.at[j, side], s["relay"].at[:, j, side], s["final"].at[:, j, side],
                        s["mid"].at[j, side], s["relay2"].at[:, j, side], s["final2"].at[:, j, side],
                        lambda k: send.at[n, k], lambda k: recv.at[n, k], store_wide(j, side))

    streams = [[stream(j, 0), stream(j, 1)] for j in range(chunks)]
    end = 2 * chunks
    streams.append([PlaneSum("seq_0", "seq_1", False, w_work.at[2], s["w_relay"], s["w_final"], s["w_mid"],
                             s["w_relay2"], s["w_final2"],
                             lambda k: send.at[end, k], lambda k: recv.at[end, k], store_narrow)])

    cols_low = []

    def ring(j, stage):
        if stage == 4 and j == chunks:
            core_copies[chunks].wait_send()
        for one in streams[j]:
            one.run(stage)

    def stats_part(n):
        statistics(s["dt"], s["slope"], log_ref, s["within"], s["last"], s["cols"], s["sums"], s["inner"],
                   s["flow"], s["stats"])

    def flip_part(n):
        s["mix"][:, GROUP // 2 : GROUP, 0 : GROUP // 2] = jnp.zeros((2, GROUP // 2, GROUP // 2), BF16)
        s["v"][:, GROUP // 2 : GROUP, 0 : GROUP // 2] = jnp.zeros((s["v"].shape[0], GROUP // 2, GROUP // 2), F32)
        s["inner"][...] = jnp.zeros_like(s["inner"])
        flip(li, lt, block)
        tables(b_ref, c_ref, s["dt"], s["slope"], s["within"], s["cols"], s["rows"], s["cross"], skip_ref, s["skip"])
        decays.take()

    steps = {
        "F": flip_part,
        "S": lambda n: carries[n].scan(),
        "B": lambda n: carries[n].give_back(),
        "E": lambda n: carries[n].finish(),
        "I": intra_part,
        "C": combine_part,
        "G": give,
        "K": keep,
        "M": lambda n: mixed_grads(b_ref, c_ref, s["v"], s["dbc"], packed),
        "P": lambda n: mp_ring.first() if n == 0 else mp_ring.second(),
        "T": stats_part,
        "O": lambda n: cols_low.append(owned_cols()),
        "g": lambda n: give_narrow(cols_low[0]),
        "k": lambda n: keep_narrow(cols_low[0]),
    }
    for step in ORDER:
        if step[0] == "r":
            ring(int(step[1]), int(step[2]))
        else:
            steps[step[0]](int(step[1:] or 0))

    half = block // 2
    turned = jnp.transpose(w_work[0, 0, 0, 0:half, :])
    wbc_ref[...] = jnp.concatenate([turned[0:64], turned[64:128]], axis=1)
    total_ref[...] = w_work[0, 0, 0, half : half + 8, :]
    for one in carries:
        one.drain()
    mp_ring.drain()
    for copy in decays.copies:
        copy.wait_send()
    for j in range(chunks):
        core_copies[j].wait_send()
    for group in streams:
        for one in group:
            one.drain()


def parts_of(width):
    cut = 2 * 256
    return ((0, cut), (cut, width))


def carry_buffers(width):
    found = {}
    for n, (left, right) in enumerate(parts_of(width)):
        wide = right - left
        for name in ("out", "got", "scanned", "back"):
            found[f"{name}{n}"] = VMEM((16, 8, wide), F32)
        for name in ("pair", "mine", "yours"):
            found[f"{name}{n}"] = VMEM((2, STATE // 2, wide), F32)
    return found


def finish_kernel(wx_in, wbc_in, totals, wx_ref, wbc_ref, log_ref, bias_ref, skip_ref):
    wx_ref[...] = wx_in[...]
    wbc_ref[...] = wbc_in[...]
    for n, ref in enumerate((log_ref, bias_ref, skip_ref)):
        ref[...] = totals[n : n + 1, 0 : ref.shape[1]]


def scratch(tokens, heads, block, wide):
    width = heads * HEAD_DIM
    chunks = width // 256
    groups = tokens // GROUP
    half = STATE // 2
    dma = pltpu.SemaphoreType.DMA
    return {
        "x": VMEM((tokens, width), BF16), "dy": VMEM((tokens, width), BF16), "li": VMEM((tokens, wide), BF16),
        "dx": VMEM((tokens, width), BF16), "lt": VMEM((2, wide // 2, tokens), BF16),
        "dt": VMEM((tokens, heads), F32), "slope": VMEM((tokens, heads), F32), "a": VMEM((tokens, heads), F32),
        "within": VMEM((tokens, heads), F32), "last": VMEM((8, heads), F32), "cols": VMEM((tokens, 3 * heads), F32),
        "rows": VMEM((groups, 3 * heads, GROUP), F32), "cross": VMEM((groups, GROUP, GROUP), F32),
        "decay": VMEM((8, width), F32), "spread": VMEM((2 * heads, width), BF16),
        "parts": VMEM((2 * groups - 2, STATE, width), F32), "ends": VMEM((2 * STATE, width), F32),
        **carry_buffers(width), "tile": VMEM((8, 128), F32), "tile_pair": VMEM((8, 128), F32),
        "tile_chip": VMEM((8, 128), F32), "tile_got": VMEM((16, 8, 128), F32), "skip": VMEM((8, width), F32),
        "tile_sems": dma((2, 16)),
        "carry": VMEM((2 * STATE, width), F32), "gains": VMEM((32, width), F32),
        "v": VMEM((groups, GROUP, GROUP), F32), "mix": VMEM((2, GROUP, GROUP), BF16),
        "flow": VMEM((groups, 2 * heads, GROUP), F32), "sp": VMEM((groups, STATE, 256), F32),
        "gp": VMEM((groups, STATE, 256), F32), "dbc": VMEM((tokens, 2 * STATE), F32),
        "sums": VMEM((tokens, 128), F32), "inner": VMEM((8, width), F32), "stats": VMEM((8, 128), F32),
        "packed": VMEM((4, tokens // 2, 128), F32), "dbc_in": VMEM((2, tokens // 2, 128), F32),
        "work": VMEM((3, chunks, 2, 4, 4, block, 128), F32), "relay": VMEM((2, chunks, 2, 2, block, 128), F32),
        "final": VMEM((2, chunks, 2, 4, block, 128), F32), "mid": VMEM((chunks, 2, 4, block, 128), F32),
        "relay2": VMEM((2, chunks, 2, block // 2, 128), F32), "final2": VMEM((2, chunks, 2, block, 128), F32),
        "w_work": VMEM((3, 4, 4, W_ROWS, 128), F32), "w_relay": VMEM((2, 2, W_ROWS, 128), F32),
        "w_final": VMEM((2, 4, W_ROWS, 128), F32), "w_mid": VMEM((4, W_ROWS, 128), F32),
        "w_relay2": VMEM((2, W_ROWS // 2, 128), F32), "w_final2": VMEM((2, W_ROWS, 128), F32),
        "load_sems": dma((3,)), "pair_sems": dma((2, 2, 3)), "chip_sems": dma((2, 4, 16)),
        "core_sems": dma((2, chunks + 1)), "mp_sems": dma((2, 6)), "mp_relay": VMEM((2, tokens // 4, 128), F32),
        "ring_send": dma((2 * chunks + 1, 12)), "ring_recv": dma((2 * chunks + 1, 12)),
    }


def on_device(layer_in, ssm_input, b_matrix, c_matrix, dt_raw, dt_bias, a_log, d_skip, grad_out):
    tokens, heads = dt_raw.shape
    wide = layer_in.shape[1]
    width = heads * HEAD_DIM
    block = wide // math.prod(lax.axis_size(axis) for axis in SEQ)
    sds = jax.ShapeDtypeStruct
    shapes = scratch(tokens, heads, block, wide)

    def kernel(*refs):
        whole_kernel(refs[:9], refs[9:12], dict(zip(shapes, refs[12:])))

    anywhere, local = pl.BlockSpec(memory_space=pl.ANY), pl.BlockSpec(memory_space=VMEM)
    grad_wx, grad_wbc, totals = pl.pallas_call(
        kernel,
        out_shape=(sds((block, width), F32), sds((64, block), F32), sds((8, 128), F32)),
        in_specs=[anywhere] * 3 + [local] * 6,
        out_specs=(local,) * 3,
        scratch_shapes=list(shapes.values()),
        name="whole",
        cost_estimate=pl.CostEstimate(flops=4 * 10**10, bytes_accessed=10**7, transcendentals=0),
        compiler_params=pltpu.CompilerParams(
            collective_id=0, has_side_effects=True, vmem_limit_bytes=67043328
        ),
    )(ssm_input, grad_out, layer_in, b_matrix, c_matrix, dt_raw.T, dt_bias[None, :], a_log[None, :],
      d_skip[None, :])
    grad_wx, grad_wbc, *rows = pl.pallas_call(
        finish_kernel,
        out_shape=(sds((block, width), F32), sds((64, block), F32)) + (sds((1, heads), F32),) * 3,
        name="finish",
        cost_estimate=pl.CostEstimate(flops=10**6, bytes_accessed=10**6, transcendentals=0),
    )(grad_wx, grad_wbc, totals)
    return (grad_wx, grad_wbc.T, *(row.reshape(heads) for row in rows))


def solution(mesh):
    n_seq, n_mp = mesh.shape["seq"], mesh.shape["mp"]
    split = Mesh(mesh.devices.reshape(n_seq // 8, 4, 2, n_mp), SEQ + ("mp",))
    in_specs = (
        P(SEQ, None),
        P(SEQ, "mp"),
        P(SEQ, None),
        P(SEQ, None),
        P(SEQ, "mp"),
        P("mp"),
        P("mp"),
        P("mp"),
        P(SEQ, "mp"),
    )
    out_specs = (P(SEQ, "mp"), P(SEQ, "mp"), P("mp"), P("mp"), P("mp"))
    return jax.shard_map(
        on_device, mesh=split, in_specs=in_specs, out_specs=out_specs, check_vma=False
    )
```

```python
import math
from types import SimpleNamespace

import jax
import jax.numpy as jnp
from jax import lax
from jax.experimental import pallas as pl
from jax.experimental.pallas import tpu as pltpu
from jax.sharding import Mesh
from jax.sharding import PartitionSpec as P

GROUP = 256
HEAD_DIM = 64
STATE = 128
LOG2E = 1.0 / math.log(2.0)
SEQ = ("seq_0", "seq_1", "seq_2")
F32 = jnp.float32
BF16 = jnp.bfloat16
VMEM = pltpu.VMEM


def dot(left, right):
    return jnp.dot(left, right, preferred_element_type=F32)


def dot_nt(left, right):
    return lax.dot_general(left, right, (((1,), (1,)), ((), ())), preferred_element_type=F32)


def dot_tn(left, right):
    return lax.dot_general(left, right, (((0,), (0,)), ((), ())), preferred_element_type=F32)


def dot_exact(left, right):
    return jnp.dot(left, right, preferred_element_type=F32, precision=lax.Precision.HIGHEST)


def lane_iota(shape, dim):
    return lax.broadcasted_iota(jnp.int32, shape, dim)


def spread_matrix(heads, dtype):
    rows = lane_iota((heads, heads * HEAD_DIM), 0)
    cols = lane_iota((heads, heads * HEAD_DIM), 1)
    inside = (cols >= rows * HEAD_DIM) & (cols < (rows + 1) * HEAD_DIM)
    return jnp.where(inside, 1.0, 0.0).astype(dtype)


def gather_matrix(heads, dtype):
    rows = lane_iota((heads * HEAD_DIM, heads), 0)
    cols = lane_iota((heads * HEAD_DIM, heads), 1)
    inside = (rows >= cols * HEAD_DIM) & (rows < (cols + 1) * HEAD_DIM)
    return jnp.where(inside, 1.0, 0.0).astype(dtype)


def lower_ones(size):
    return jnp.where(lane_iota((size, size), 0) >= lane_iota((size, size), 1), 1.0, 0.0)


def halves(values):
    high = values.astype(BF16)
    low = (values - high.astype(F32)).astype(BF16)
    return jnp.concatenate([high, low], axis=1)


def spread(first, second, matrix):
    rows = first.shape[0]
    wide = dot(jnp.concatenate([halves(first), halves(second)], axis=0), matrix)
    return wide[0:rows], wide[rows : 2 * rows]


MESH = pl.DeviceIdType.MESH
W_ROWS = 48


def around(axis, shift):
    return {axis: lax.rem(lax.axis_index(axis) + shift, 4)}


def remote(source, target, send, recv, device):
    return pltpu.make_async_remote_copy(
        src_ref=source, dst_ref=target, send_sem=send, recv_sem=recv, device_id=device, device_id_type=MESH
    )


class RingSum:
    def __init__(self, axis, part, relay, final, send, recv, base):
        self.axis, self.part, self.relay, self.final = axis, part, relay, final
        self.send, self.recv, self.base = send, recv, base
        me = lax.axis_index(axis)
        self.me = me
        self.ahead, self.behind, self.across = (lax.rem(me + k, 4) for k in (1, 3, 2))
        self.up, self.down = around(axis, 1), around(axis, 3)
        self.copies = {}

    def copy(self, n, source, target, device):
        at = self.base + n
        self.copies[n] = remote(source, target, self.send(at), self.recv(at), device)
        self.copies[n].start()

    def first(self):
        self.copy(0, self.part(self.across, 0), self.relay(0), self.up)
        self.copy(1, self.part(self.across, 1), self.relay(1), self.down)
        self.copy(2, self.part(self.ahead, 1), self.final(0, 1), self.up)
        self.copy(3, self.part(self.behind, 0), self.final(1, 0), self.down)

    def second(self):
        self.copies[0].wait_recv()
        ahead = self.part(self.ahead, 0)
        ahead[...] += self.relay(0)[...]
        self.copy(4, ahead, self.final(0, 0), self.up)
        self.copies[1].wait_recv()
        behind = self.part(self.behind, 1)
        behind[...] += self.relay(1)[...]
        self.copy(5, behind, self.final(1, 1), self.down)

    def result(self, half):
        (self.copies[4] if half == 0 else self.copies[2]).wait_recv()
        (self.copies[3] if half == 0 else self.copies[5]).wait_recv()
        return self.part(self.me, half)[...] + self.final(0, half)[...] + self.final(1, half)[...]

    def drain(self):
        for copy in self.copies.values():
            copy.wait_send()


class PlaneSum:
    def __init__(self, first_axis, second_axis, swap, own, relay, final, mid, relay2, final2, send, recv, store):
        rows = mid.shape[1]
        self.store, self.mid, self.rows = store, mid, rows

        def part(d, half):
            pair = pl.ds(2 * half, 2)
            return own.at[pair, d] if swap else own.at[d, pair]

        def part2(d, half):
            return mid.at[d, pl.ds(half * (rows // 2), rows // 2)]

        self.one = RingSum(first_axis, part, lambda h: relay.at[h], lambda w, h: final.at[w, pl.ds(2 * h, 2)],
                           send, recv, 0)
        self.two = RingSum(second_axis, part2, lambda h: relay2.at[h],
                           lambda w, h: final2.at[w, pl.ds(h * (rows // 2), rows // 2)], send, recv, 6)

    def run(self, stage):
        if stage == 0:
            self.one.first()
        elif stage == 1:
            self.one.second()
        elif stage == 2:
            for half in range(2):
                self.mid[pl.ds(2 * half, 2)] = self.one.result(half)
            self.two.first()
        elif stage == 3:
            self.two.second()
        elif stage == 4:
            for half in range(2):
                self.store(half, self.two.result(half))

    def drain(self):
        self.one.drain()
        self.two.drain()


STRIP = 64


def scalars(raw_ref, bias_ref, log_ref, dt_ref, slope_ref, a_ref):
    shifted = jnp.transpose(raw_ref[...]) + bias_ref[...]
    small = jnp.exp(-jnp.abs(shifted))
    one = 1.0 + small
    log_one = jnp.where(one == 1.0, small, jnp.log(one) * small / jnp.where(one == 1.0, 1.0, one - 1.0))
    dt = jnp.maximum(shifted, 0.0) + log_one
    dt_ref[...] = dt
    slope_ref[...] = jnp.where(shifted >= 0.0, 1.0, small) / one
    a_ref[...] = dt * -jnp.exp(log_ref[...])


def block_decay(a_ref, within_ref, last_ref, tile):
    tokens, heads = a_ref.shape
    tri = lower_ones(GROUP)
    block_end = jnp.zeros((1, heads), F32)
    for g in range(tokens // GROUP):
        rows = slice(g * GROUP, (g + 1) * GROUP)
        within = dot_exact(tri, a_ref[rows, :])
        last = within[GROUP - 1 : GROUP, :]
        block_end = block_end + last
        within_ref[rows, :] = within
        last_ref[g : g + 1, :] = last
    pad = jnp.concatenate([jnp.exp(block_end), jnp.zeros((1, 128 - heads), F32)], axis=1)
    tile[...] = jnp.broadcast_to(pad, (8, 128))


def states(x, dy, b_ref, c_ref, dt_ref, within_ref, last_ref, decay_ref, spread_ref, parts, ends):
    tokens, heads = dt_ref.shape
    groups = tokens // GROUP
    width = heads * HEAD_DIM
    once = spread_matrix(heads, F32)
    spread_m = jnp.concatenate([once, once], axis=0).astype(BF16)
    spread_ref[...] = spread_m
    spread_e = spread_matrix(heads, F32)
    for g in range(groups):
        rows = slice(g * GROUP, (g + 1) * GROUP)
        dt = dt_ref[rows, :]
        within = within_ref[rows, :]
        last = last_ref[g : g + 1, :]
        decay = dot_exact(jnp.broadcast_to(jnp.exp(last), (8, heads)), spread_e)[0:1, :]
        decay_ref[g : g + 1, :] = decay
        fall, rise = spread(dt * jnp.exp(last - within), jnp.exp(within), spread_m)
        xw = (x[rows, :].astype(F32) * fall).astype(BF16)
        state = dot_tn(b_ref[rows, :], xw)
        yw = (dy[rows, :].astype(F32) * rise).astype(BF16)
        grad = dot_tn(c_ref[rows, :], yw)
        if g < groups - 1:
            parts[g] = state
        if g > 0:
            parts[groups - 2 + g] = grad
        if g == 0:
            ends[0:STATE, 0:width] = state
            ends[STATE : 2 * STATE, 0:width] = grad
            gain = decay
        else:
            ends[0:STATE, 0:width] = decay * ends[0:STATE, 0:width] + state
            ends[STATE : 2 * STATE, 0:width] = ends[STATE : 2 * STATE, 0:width] + gain * grad
            gain = gain * decay


def tables(b_ref, c_ref, dt_ref, slope_ref, within_ref, cols_ref, rows_ref, cross_ref, skip_ref, skip_wide):
    tokens, heads = dt_ref.shape
    tri = lower_ones(GROUP)
    skip_wide[...] = dot_exact(jnp.broadcast_to(skip_ref[...], (8, heads)), spread_matrix(heads, F32))
    for g in range(tokens // GROUP):
        rows = slice(g * GROUP, (g + 1) * GROUP)
        dt = dt_ref[rows, :]
        rise2 = within_ref[rows, :] * LOG2E
        sums = dot_exact(tri, jnp.concatenate([dt, slope_ref[rows, :]], axis=1))
        cols_ref[rows, :] = jnp.concatenate([rise2 - jnp.log2(dt), sums], axis=1)
        rows_ref[g] = jnp.transpose(jnp.concatenate([rise2, sums], axis=1))
        cross_ref[g] = dot_nt(b_ref[rows, :], c_ref[rows, :])


class Decays:
    def __init__(self, tile, pair, chip_tile, got, gains, heads, sems):
        self.tile, self.pair, self.chip_tile, self.got, self.gains = tile, pair, chip_tile, got, gains
        self.heads, self.sems = heads, sems
        self.core = lax.axis_index(SEQ[2])
        self.me = lax.axis_index(SEQ[0]) * 4 + lax.axis_index(SEQ[1])

    def chip(self, offset):
        index = lax.rem(self.me + offset, 16)
        return index, {SEQ[0]: index // 4, SEQ[1]: lax.rem(index, 4)}

    def spread_rows(self, tile):
        return dot_exact(tile[:, 0 : self.heads], spread_matrix(self.heads, F32))

    def give_pair(self):
        self.copies = [remote(self.tile, self.pair, self.sems.at[0, 0], self.sems.at[1, 0], {SEQ[2]: 1 - self.core})]
        self.copies[0].start()

    def give_chips(self):
        self.copies[0].wait_recv()
        first = self.core == 0
        mine, theirs = self.tile[...], self.pair[...]
        tile0, tile1 = jnp.where(first, mine, theirs), jnp.where(first, theirs, mine)
        self.chip_tile[...] = tile0 * tile1
        self.got[0] = tile0 * tile1
        for k in range(1, 16):
            copy = remote(self.chip_tile, self.got.at[k], self.sems.at[0, k], self.sems.at[1, k], self.chip(k)[1])
            copy.start()
            self.copies.append(copy)
        self.gains[0:8, :] = self.spread_rows(tile0)
        self.gains[8:16, :] = self.spread_rows(tile1)

    def take(self):
        for copy in self.copies[1:]:
            copy.wait_recv()
        self.gains[16:32, :] = self.spread_rows(self.got[:, 0, :])


class Carry:
    def __init__(self, decays, left, ends, carry, pair, out, got, scanned, back, mine, yours, core_sems, sems):
        self.ends, self.pair, self.out, self.got, self.scanned = ends, pair, out, got, scanned
        self.back, self.mine, self.yours, self.carry, self.gains = back, mine, yours, carry, decays.gains
        self.core_sems, self.sems, self.decays = core_sems, sems, decays
        self.core, self.me, self.chip = decays.core, decays.me, decays.chip
        self.other = {SEQ[2]: 1 - self.core}
        self.width = out.shape[2]
        self.cols = pl.ds(left, self.width)

    def own_rows(self, kind, core):
        return pl.ds(pl.multiple_of(kind * STATE + core * (STATE // 2), STATE // 2), STATE // 2)

    def gain(self, row):
        return self.gains[pl.ds(row, 1), self.cols]

    def give_pair(self):
        self.pair_copies = []
        for kind in range(2):
            copy = remote(self.ends.at[self.own_rows(kind, 1 - self.core), self.cols], self.pair.at[kind],
                          self.core_sems.at[0, kind], self.core_sems.at[1, kind], self.other)
            copy.start()
            self.pair_copies.append(copy)

    def both(self, kind):
        own = self.ends[self.own_rows(kind, self.core), self.cols]
        other = self.pair[kind]
        first = self.core == 0
        return jnp.where(first, own, other), jnp.where(first, other, own)

    def give_chips(self):
        for copy in self.pair_copies:
            copy.wait_recv()
        s0, s1 = self.both(0)
        self.out[0:8] = (self.gain(8) * s0 + s1).reshape(8, 8, self.width)
        g0, g1 = self.both(1)
        self.out[8:16] = (g0 + self.gain(0) * g1).reshape(8, 8, self.width)
        self.got[0] = self.out[self.me]
        self.copies = []
        for k in range(1, 16):
            index, device = self.chip(k)
            copy = remote(self.out.at[index], self.got.at[k], self.sems.at[0, k], self.sems.at[1, k], device)
            copy.start()
            self.copies.append(copy)

    def scan(self):
        for copy in self.copies:
            copy.wait_recv()
        backward = self.me >= 8

        def step(i, running):
            chip = jnp.where(backward, 15 - i, i)
            slot = lax.rem(self.me - chip + 16, 16)
            self.scanned[slot] = running
            return self.gain(16 + slot) * running + self.got[slot]

        lax.fori_loop(0, 16, step, jnp.zeros((8, self.width), F32))
        self.back[self.me] = self.scanned[0]
        self.back_copies = []
        for k in range(1, 16):
            index, device = self.chip(16 - k)
            copy = remote(self.scanned.at[k], self.back.at[self.me], self.sems.at[2, k], self.sems.at[3, k], device)
            copy.start()
            self.back_copies.append(copy)

    def give_back(self):
        half = STATE // 2
        for copy in self.back_copies:
            copy.wait_recv()
        first = self.core == 0
        s_in = self.back[0:8].reshape(half, self.width)
        s0, _ = self.both(0)
        s_next = self.gain(0) * s_in + s0
        self.mine[0] = jnp.where(first, s_next, s_in)
        g_in = self.back[8:16].reshape(half, self.width)
        _, g1 = self.both(1)
        g_before = g1 + self.gain(8) * g_in
        self.mine[1] = jnp.where(first, g_in, g_before)
        self.last = remote(self.mine, self.yours, self.core_sems.at[0, 2], self.core_sems.at[1, 2], self.other)
        self.last.start()
        self.carry[self.own_rows(0, self.core), self.cols] = jnp.where(first, s_in, s_next)
        self.carry[self.own_rows(1, self.core), self.cols] = jnp.where(first, g_before, g_in)

    def finish(self):
        self.last.wait_recv()
        for kind in range(2):
            self.carry[self.own_rows(kind, 1 - self.core), self.cols] = self.yours[kind]

    def drain(self):
        for copy in self.pair_copies + self.copies + self.back_copies + [self.last]:
            copy.wait_send()


def intra(j, x, dy, cols_ref, rows_ref, cross_ref, v_ref, mix_ref, gi, flow_ref, heads):
    half = GROUP // 2

    def group(g, unused):
        at = pl.multiple_of(g * GROUP, GROUP)
        for pair in range(2 * j, 2 * j + 2):
            zs, sides = [], []
            for sub in range(2):
                h = 2 * pair + sub
                lanes = slice(h * HEAD_DIM, (h + 1) * HEAD_DIM)
                x_h = x[pl.ds(at, GROUP), lanes]
                dy_h = dy[pl.ds(at, GROUP), lanes]
                top = dot_nt(x_h[0:half], dy_h)
                low = dot_nt(x_h[half:GROUP], dy_h[half:GROUP])
                acc = [jnp.zeros((8, GROUP), F32) for _ in range(3)]
                z_strips = []
                for k in range(GROUP // STRIP):
                    first = (k * STRIP // half) * half
                    wide = GROUP - first
                    rows = slice(k * STRIP, (k + 1) * STRIP)
                    here = pl.ds(at + k * STRIP, STRIP)
                    gap = rows_ref[g, h : h + 1, first:GROUP] - cols_ref[here, h : h + 1]
                    reach = lane_iota((STRIP, wide), 1) + first >= lane_iota((STRIP, wide), 0) + k * STRIP
                    decay = jnp.where(reach, jnp.exp2(gap), 0.0)
                    bc = cross_ref[g, rows, first:GROUP]
                    mix_ref[sub, rows, first:GROUP] = (decay * bc).astype(BF16)
                    z = decay * (top[rows, :] if first == 0 else low[k * STRIP - half : (k + 1) * STRIP - half, :])
                    z_strips.append(z)
                    box = z * bc
                    w_dt = cols_ref[here, heads + h : heads + h + 1]
                    w_sl = cols_ref[here, 2 * heads + h : 2 * heads + h + 1]
                    for n, term in enumerate((box, box * w_dt, box * w_sl)):
                        part = jnp.sum(term.reshape(STRIP // 8, 8, wide), axis=0)
                        if first > 0:
                            acc[n] = jnp.concatenate([acc[n][:, 0:first], acc[n][:, first:GROUP] + part], axis=1)
                        else:
                            acc[n] = acc[n] + part
                zs.append(z_strips)
                sides.append(dot(mix_ref[sub], dy_h))
                flow_dt = acc[0] * rows_ref[g, heads + h : heads + h + 1, :] - acc[1]
                flow_sl = acc[0] * rows_ref[g, 2 * heads + h : 2 * heads + h + 1, :] - acc[2]
                flow_ref[g, h : h + 1, :] = jnp.sum(flow_dt, axis=0, keepdims=True)
                flow_ref[g, heads + h : heads + h + 1, :] = jnp.sum(flow_sl, axis=0, keepdims=True)
            for k in range(GROUP // STRIP):
                first = (k * STRIP // half) * half
                rows = slice(k * STRIP, (k + 1) * STRIP)
                both = zs[0][k] + zs[1][k]
                if pair == 0:
                    v_ref[g, rows, first:GROUP] = both
                else:
                    v_ref[g, rows, first:GROUP] += both
            gi[pl.ds(at, GROUP), pair * 128 : (pair + 1) * 128] = jnp.concatenate(sides, axis=1).astype(BF16)
        return unused

    lax.fori_loop(0, x.shape[0] // GROUP, group, 0)


def combine(j, x, dy, b_ref, c_ref, dt_ref, within_ref, last_ref, decay_ref, spread_ref, skip_ref, parts, carry,
            sp_ref, gp_ref, dx, dbc, sums_ref, inner_ref):
    tokens, heads = dt_ref.shape
    groups = tokens // GROUP
    cols = slice(j * 256, (j + 1) * 256)
    sp_ref[0] = carry[0:STATE, cols]
    gp_ref[groups - 1] = carry[STATE : 2 * STATE, cols]
    for g in range(groups - 1):
        sp_ref[g + 1] = decay_ref[g : g + 1, cols] * sp_ref[g] + parts[g, :, cols]
    for g in range(groups - 1, 0, -1):
        gp_ref[g - 1] = parts[groups - 2 + g, :, cols] + decay_ref[g : g + 1, cols] * gp_ref[g]
    spread_m = spread_ref[:, cols]
    head = (lane_iota((256, 128), 0) + j * 256) // HEAD_DIM
    lane = lane_iota((256, 128), 1)

    def gather(k):
        return jnp.where(lane == head + k * heads, 1.0, 0.0).astype(BF16)

    for g in range(groups):
        rows = slice(g * GROUP, (g + 1) * GROUP)
        within = within_ref[rows, :]
        fall, rise = spread(dt_ref[rows, :] * jnp.exp(last_ref[g : g + 1, :] - within), jnp.exp(within), spread_m)
        xs = x[rows, cols].astype(F32)
        dys = dy[rows, cols].astype(F32)
        sp = sp_ref[g]
        gp = gp_ref[g]
        inner_ref[g : g + 1, cols] = jnp.sum(sp * gp, axis=0, keepdims=True)
        sp_low = sp.astype(BF16)
        gp_low = gp.astype(BF16)
        from_end = dot(b_ref[rows, :], gp_low)
        from_start = dot(c_ref[rows, :], sp_low)
        raw = dx[rows, cols].astype(F32) + fall * from_end
        total = dot((xs * raw).astype(BF16), gather(0))
        total += dot((xs * from_end).astype(BF16), gather(1))
        total += dot((xs * dys).astype(BF16), gather(2))
        total += dot((dys * from_start).astype(BF16), gather(3))
        dx[rows, cols] = (raw + skip_ref[0:1, cols] * dys).astype(BF16)
        d_b = dot_nt((xs * fall).astype(BF16), gp_low)
        d_c = dot_nt((dys * rise).astype(BF16), sp_low)
        if j == 0:
            sums_ref[rows, :] = total
            dbc[rows, 0:STATE] = d_b
            dbc[rows, STATE : 2 * STATE] = d_c
        else:
            sums_ref[rows, :] += total
            dbc[rows, 0:STATE] += d_b
            dbc[rows, STATE : 2 * STATE] += d_c


def mixed_grads(b_ref, c_ref, v_ref, dbc, packed):
    groups = v_ref.shape[0]
    for g in range(groups):
        rows = slice(g * GROUP, (g + 1) * GROUP)
        mixed = v_ref[g].astype(BF16)
        grads = (dbc[rows, 0:STATE] + dot(mixed, c_ref[rows, :]),
                 dbc[rows, STATE : 2 * STATE] + dot_tn(mixed, b_ref[rows, :]))
        for piece in range(GROUP // 128):
            at = g * (GROUP // 128) + piece
            side, base = divmod(at * 128, packed.shape[1])
            for m in range(packed.shape[0]):
                source, left = divmod(m * 64, STATE)
                packed[m, base : base + 128, side * 64 : side * 64 + 64] = grads[source][
                    piece * 128 : (piece + 1) * 128, left : left + 64
                ]


def statistics(dt_ref, slope_ref, log_ref, within_ref, last_ref, cols_ref, sums_ref, inner_ref, flow_ref, stat_ref):
    tokens, heads = dt_ref.shape
    groups = tokens // GROUP
    gather_e = gather_matrix(heads, F32)
    rate = -jnp.exp(log_ref[...])
    flow_dt = jnp.zeros((1, heads), F32)
    flow_sl = jnp.zeros((1, heads), F32)
    bias = jnp.zeros((1, heads), F32)
    skips = jnp.zeros((1, heads), F32)
    inner = dot_exact(inner_ref[...], gather_e)
    for g in range(groups):
        rows = slice(g * GROUP, (g + 1) * GROUP)
        dt = dt_ref[rows, :]
        within = within_ref[rows, :]
        last = last_ref[g : g + 1, :]
        back = jnp.exp(within) * sums_ref[rows, 3 * heads : 4 * heads]
        fore = dt * jnp.exp(last - within) * sums_ref[rows, heads : 2 * heads]
        meet = jnp.exp(last) * inner[g : g + 1, :]
        for which in range(2):
            sums = cols_ref[rows, (which + 1) * heads : (which + 2) * heads]
            whole = sums[GROUP - 1 : GROUP, :]
            flow = jnp.sum(back * sums + fore * (whole - sums), axis=0, keepdims=True) + meet * whole
            if which == 0:
                flow_dt += flow
            else:
                flow_sl += flow
        bias += jnp.sum(slope_ref[rows, :] / dt * sums_ref[rows, 0:heads], axis=0, keepdims=True)
        skips += jnp.sum(sums_ref[rows, 2 * heads : 3 * heads], axis=0, keepdims=True)
    flows = flow_ref[0]
    for g in range(1, groups):
        flows = flows + flow_ref[g]
    totals = jnp.transpose(jnp.sum(flows, axis=1, keepdims=True) + jnp.zeros((2 * heads, 128), F32))[0:1, :]
    stat_ref[...] = jnp.zeros_like(stat_ref)
    stat_ref[0:1, 0:heads] = rate * (flow_dt + totals[:, 0:heads])
    stat_ref[1:2, 0:heads] = bias + rate * (flow_sl + totals[:, heads : 2 * heads])
    stat_ref[2:3, 0:heads] = skips


def flip(li, lt, block):
    def group(g, unused):
        at = pl.multiple_of(g * GROUP, GROUP)
        wide = 8 * block
        for q in range(li.shape[1] // wide):
            turned = jnp.transpose(li[pl.ds(at, GROUP), q * wide : (q + 1) * wide])
            for k in range(8):
                n = q * 8 + k
                lt[n % 2, (n // 2) * block : (n // 2 + 1) * block, pl.ds(at, GROUP)] = turned[
                    k * block : (k + 1) * block, :
                ]
        return unused

    lax.fori_loop(0, li.shape[0] // GROUP, group, 0)


def whole_kernel(refs_in, refs_out, s):
    x_hbm, dy_hbm, li_hbm, b_ref, c_ref, raw_ref, bias_ref, log_ref, skip_ref = refs_in
    wx_ref, wbc_ref, total_ref = refs_out
    block = wx_ref.shape[0]
    heads = raw_ref.shape[0]
    x, dy, li, dx, lt = s.x, s.dy, s.li, s.dx, s.lt
    work, got_sems = s.work, s.core_sems
    chunks = work.shape[1]
    core = lax.axis_index(SEQ[2])
    mp = lax.axis_index("mp")
    other = {SEQ[2]: 1 - core}

    loads = []
    for n, (source, target) in enumerate(((x_hbm, x), (dy_hbm, dy), (li_hbm, li))):
        load = pltpu.make_async_copy(source, target, s.load_sems.at[n])
        load.start()
        loads.append(load)

    decays = Decays(s.tile, s.tile_pair, s.tile_chip, s.tile_got, s.gains, heads, s.tile_sems)
    carries = []
    for n, (left, right) in enumerate(parts_of(heads * HEAD_DIM)):
        buffers = s.carry_parts[n]
        carries.append(Carry(decays, left, s.ends, s.carry, *buffers, s.pair_sems.at[n], s.chip_sems.at[n]))
    partners = [other] + [decays.chip(k)[1] for k in range(1, 16)] + [around("mp", k) for k in (1, 2, 3)]
    barrier = pltpu.get_barrier_semaphore()
    for partner in partners:
        pl.semaphore_signal(barrier, inc=1, device_id=partner, device_id_type=MESH)

    scalars(raw_ref, bias_ref, log_ref, s.dt, s.slope, s.a)
    block_decay(s.a, s.within, s.last, s.tile)
    pl.semaphore_wait(barrier, len(partners))
    decays.give_pair()
    loads[0].wait()
    loads[1].wait()
    states(x, dy, b_ref, c_ref, s.dt, s.within, s.last, s.decay, s.spread, s.parts, s.ends)
    for one in carries:
        one.give_pair()

    def intra_part(j):
        intra(j, x, dy, s.cols, s.rows, s.cross, s.v, s.mix, dx, s.flow, heads)

    def combine_part(j):
        combine(j, x, dy, b_ref, c_ref, s.dt, s.within, s.last, s.decay, s.spread, s.skip,
                s.parts, s.carry, s.sp, s.gp, dx, s.dbc, s.sums, s.inner)

    decays.give_chips()
    for one in carries:
        one.give_chips()
    loads[2].wait()
    send_own, got, own = (work.at[i] for i in range(3))
    core_copies = {}

    def give(j):
        cols = dx[:, j * 256 : (j + 1) * 256]

        def body(i, unused):
            start = pl.multiple_of(i * 8 * block, 16)
            res = dot(lt[1 - core, pl.ds(start, 8 * block), :], cols)
            for side in range(2):
                send_own[j, side, pl.ds(2 * i, 2)] = res[:, side * 128 : (side + 1) * 128].reshape(2, 4, block, 128)
            return unused

        lax.fori_loop(0, 2, body, 0)
        core_copies[j] = remote(send_own.at[j], got.at[j], got_sems.at[0, j], got_sems.at[1, j], other)
        core_copies[j].start()

    def keep(j):
        core_copies[j].wait_recv()
        cols = dx[:, j * 256 : (j + 1) * 256]

        def body(i, unused):
            start = pl.multiple_of(i * 8 * block, 16)
            res = dot(lt[core, pl.ds(start, 8 * block), :], cols)
            for side in range(2):
                part = res[:, side * 128 : (side + 1) * 128].reshape(2, 4, block, 128)
                own[j, side, pl.ds(2 * i, 2)] = got[j, side, pl.ds(2 * i, 2)] + part
            return unused

        lax.fori_loop(0, 2, body, 0)

    w_work = s.w_work
    dbc_in, packed = s.dbc_in, s.packed

    def narrow(kind, i, cols):
        start = pl.multiple_of(i * 4 * block, 16)
        res = dot(lt[kind, pl.ds(start, 4 * block), :], cols).reshape(4, block, 64)
        grads = jnp.concatenate([res[:, 0 : block // 2], res[:, block // 2 : block]], axis=2)
        stats = jnp.broadcast_to(s.stats[...][None], (4, 8, 128))
        return jnp.concatenate([grads, stats], axis=1)

    quarter = packed.shape[1] // 2
    mp_ring = RingSum("mp", lambda d, h: packed.at[d, pl.ds(h * quarter, quarter)], lambda h: s.mp_relay.at[h],
                      lambda w, h: dbc_in.at[w, pl.ds(h * quarter, quarter)],
                      lambda k: s.mp_sems.at[0, k], lambda k: s.mp_sems.at[1, k], 0)

    def owned_cols():
        owned = jnp.concatenate([mp_ring.result(0), mp_ring.result(1)], axis=0)
        return jnp.concatenate([owned[:, 0:64], owned[:, 64:128]], axis=0).astype(BF16)

    def give_narrow(cols):
        def body(i, unused):
            w_work[0, i] = narrow(1 - core, i, cols)
            return unused

        lax.fori_loop(0, 4, body, 0)
        core_copies[chunks] = remote(
            w_work.at[0], w_work.at[1], got_sems.at[0, chunks], got_sems.at[1, chunks], other
        )
        core_copies[chunks].start()

    def keep_narrow(cols):
        core_copies[chunks].wait_recv()

        def body(i, unused):
            w_work[2, i] = w_work[1, i] + narrow(core, i, cols)
            return unused

        lax.fori_loop(0, 4, body, 0)

    def store_wide(j, side):
        left = j * 256 + side * 128

        def store(half, value):
            wx_ref[half * (block // 2) : (half + 1) * (block // 2), left : left + 128] = value

        return store

    def store_narrow(half, value):
        w_work[0, 0, 0, half * (W_ROWS // 2) : (half + 1) * (W_ROWS // 2)] = value

    send, recv = s.ring_send, s.ring_recv

    def stream(j, side):
        axes = SEQ[:2] if side == 0 else SEQ[1::-1]
        n = 2 * j + side
        return PlaneSum(*axes, side == 1, own.at[j, side], s.relay.at[:, j, side], s.final.at[:, j, side],
                        s.mid.at[j, side], s.relay2.at[:, j, side], s.final2.at[:, j, side],
                        lambda k: send.at[n, k], lambda k: recv.at[n, k], store_wide(j, side))

    streams = [[stream(j, 0), stream(j, 1)] for j in range(chunks)]
    end = 2 * chunks
    streams.append([PlaneSum(*SEQ[:2], False, w_work.at[2], s.w_relay, s.w_final, s.w_mid,
                             s.w_relay2, s.w_final2,
                             lambda k: send.at[end, k], lambda k: recv.at[end, k], store_narrow)])

    def ring(j, stage):
        if stage == 4 and j == chunks:
            core_copies[chunks].wait_send()
        for one in streams[j]:
            one.run(stage)

    def stats_part(n):
        statistics(s.dt, s.slope, log_ref, s.within, s.last, s.cols, s.sums, s.inner,
                   s.flow, s.stats)

    def flip_part(n):
        s.mix[:, GROUP // 2 : GROUP, 0 : GROUP // 2] = jnp.zeros((2, GROUP // 2, GROUP // 2), BF16)
        s.v[:, GROUP // 2 : GROUP, 0 : GROUP // 2] = jnp.zeros((s.v.shape[0], GROUP // 2, GROUP // 2), F32)
        s.inner[...] = jnp.zeros_like(s.inner)
        flip(li, lt, block)
        tables(b_ref, c_ref, s.dt, s.slope, s.within, s.cols, s.rows, s.cross, skip_ref, s.skip)
        decays.take()

    flip_part(0)
    carries[0].scan()
    intra_part(0)
    carries[1].scan()
    intra_part(1)
    carries[0].give_back()
    intra_part(2)
    carries[0].finish()
    combine_part(0)
    give(0)
    combine_part(1)
    give(1)
    carries[1].give_back()
    keep(0)
    ring(0, 0)
    keep(1)
    ring(1, 0)
    carries[1].finish()
    combine_part(2)
    ring(0, 1)
    give(2)
    intra_part(3)
    keep(2)
    ring(2, 0)
    ring(1, 1)
    combine_part(3)
    give(3)
    ring(0, 2)
    intra_part(4)
    keep(3)
    ring(3, 0)
    ring(2, 1)
    combine_part(4)
    give(4)
    mixed_grads(b_ref, c_ref, s.v, s.dbc, packed)
    mp_ring.first()
    ring(1, 2)
    ring(0, 3)
    keep(4)
    ring(4, 0)
    stats_part(0)
    ring(3, 1)
    mp_ring.second()
    ring(2, 2)
    ring(1, 3)
    owned = owned_cols()
    give_narrow(owned)
    ring(4, 1)
    keep_narrow(owned)
    ring(5, 0)
    ring(0, 4)
    ring(3, 2)
    ring(2, 3)
    ring(5, 1)
    ring(1, 4)
    ring(4, 2)
    ring(3, 3)
    ring(5, 2)
    ring(2, 4)
    ring(4, 3)
    ring(3, 4)
    ring(5, 3)
    ring(4, 4)
    ring(5, 4)

    half = block // 2
    turned = jnp.transpose(w_work[0, 0, 0, 0:half, :])
    wbc_ref[...] = jnp.concatenate([turned[0:64], turned[64:128]], axis=1)
    total_ref[...] = w_work[0, 0, 0, half : half + 8, :]
    for one in carries:
        one.drain()
    mp_ring.drain()
    for copy in decays.copies:
        copy.wait_send()
    for j in range(chunks):
        core_copies[j].wait_send()
    for group in streams:
        for one in group:
            one.drain()


def parts_of(width):
    cut = 2 * 256
    return ((0, cut), (cut, width))


def carry_buffers(left, right):
    rows, tiles = VMEM((2, STATE // 2, right - left), F32), VMEM((16, 8, right - left), F32)
    return (rows, tiles, tiles, tiles, tiles, rows, rows)


def finish_kernel(wx_in, wbc_in, totals, wx_ref, wbc_ref, log_ref, bias_ref, skip_ref):
    wx_ref[...] = wx_in[...]
    wbc_ref[...] = wbc_in[...]
    for n, ref in enumerate((log_ref, bias_ref, skip_ref)):
        ref[...] = totals[n : n + 1, 0 : ref.shape[1]]


def scratch(tokens, heads, block, wide):
    width = heads * HEAD_DIM
    chunks = width // 256
    groups = tokens // GROUP
    half = STATE // 2
    dma = pltpu.SemaphoreType.DMA
    return dict(
        x=VMEM((tokens, width), BF16), dy=VMEM((tokens, width), BF16), li=VMEM((tokens, wide), BF16),
        dx=VMEM((tokens, width), BF16), lt=VMEM((2, wide // 2, tokens), BF16),
        dt=VMEM((tokens, heads), F32), slope=VMEM((tokens, heads), F32), a=VMEM((tokens, heads), F32),
        within=VMEM((tokens, heads), F32), last=VMEM((8, heads), F32), cols=VMEM((tokens, 3 * heads), F32),
        rows=VMEM((groups, 3 * heads, GROUP), F32), cross=VMEM((groups, GROUP, GROUP), F32),
        decay=VMEM((8, width), F32), spread=VMEM((2 * heads, width), BF16),
        parts=VMEM((2 * groups - 2, STATE, width), F32), ends=VMEM((2 * STATE, width), F32),
        tile=VMEM((8, 128), F32), tile_pair=VMEM((8, 128), F32),
        tile_chip=VMEM((8, 128), F32), tile_got=VMEM((16, 8, 128), F32), skip=VMEM((8, width), F32),
        tile_sems=dma((2, 16)),
        carry=VMEM((2 * STATE, width), F32), gains=VMEM((32, width), F32),
        v=VMEM((groups, GROUP, GROUP), F32), mix=VMEM((2, GROUP, GROUP), BF16),
        flow=VMEM((groups, 2 * heads, GROUP), F32), sp=VMEM((groups, STATE, 256), F32),
        gp=VMEM((groups, STATE, 256), F32), dbc=VMEM((tokens, 2 * STATE), F32),
        sums=VMEM((tokens, 128), F32), inner=VMEM((8, width), F32), stats=VMEM((8, 128), F32),
        packed=VMEM((4, tokens // 2, 128), F32), dbc_in=VMEM((2, tokens // 2, 128), F32),
        work=VMEM((3, chunks, 2, 4, 4, block, 128), F32), relay=VMEM((2, chunks, 2, 2, block, 128), F32),
        final=VMEM((2, chunks, 2, 4, block, 128), F32), mid=VMEM((chunks, 2, 4, block, 128), F32),
        relay2=VMEM((2, chunks, 2, block // 2, 128), F32), final2=VMEM((2, chunks, 2, block, 128), F32),
        w_work=VMEM((3, 4, 4, W_ROWS, 128), F32), w_relay=VMEM((2, 2, W_ROWS, 128), F32),
        w_final=VMEM((2, 4, W_ROWS, 128), F32), w_mid=VMEM((4, W_ROWS, 128), F32),
        w_relay2=VMEM((2, W_ROWS // 2, 128), F32), w_final2=VMEM((2, W_ROWS, 128), F32),
        load_sems=dma((3,)), pair_sems=dma((2, 2, 3)), chip_sems=dma((2, 4, 16)),
        core_sems=dma((2, chunks + 1)), mp_sems=dma((2, 6)), mp_relay=VMEM((2, tokens // 4, 128), F32),
        ring_send=dma((2 * chunks + 1, 12)), ring_recv=dma((2 * chunks + 1, 12)),
    )


def on_device(layer_in, ssm_input, b_matrix, c_matrix, dt_raw, dt_bias, a_log, d_skip, grad_out):
    tokens, heads = dt_raw.shape
    wide = layer_in.shape[1]
    width = heads * HEAD_DIM
    block = wide // math.prod(lax.axis_size(axis) for axis in SEQ)
    sds = jax.ShapeDtypeStruct
    shapes = scratch(tokens, heads, block, wide)

    held = [carry_buffers(*part) for part in parts_of(width)]
    count = len(held[0])

    def kernel(*refs):
        space = SimpleNamespace(**dict(zip(shapes, refs[12:])))
        rest = refs[12 + len(shapes) :]
        space.carry_parts = [rest[n * count : (n + 1) * count] for n in range(len(held))]
        whole_kernel(refs[:9], refs[9:12], space)

    anywhere, local = pl.BlockSpec(memory_space=pl.ANY), pl.BlockSpec(memory_space=VMEM)
    grad_wx, grad_wbc, totals = pl.pallas_call(
        kernel,
        out_shape=(sds((block, width), F32), sds((64, block), F32), sds((8, 128), F32)),
        in_specs=[anywhere] * 3 + [local] * 6,
        out_specs=(local,) * 3,
        scratch_shapes=list(shapes.values()) + [one for part in held for one in part],
        name="whole",
        cost_estimate=pl.CostEstimate(flops=4 * 10**10, bytes_accessed=10**7, transcendentals=0),
        compiler_params=pltpu.CompilerParams(
            collective_id=0, has_side_effects=True, vmem_limit_bytes=67043328
        ),
    )(ssm_input, grad_out, layer_in, b_matrix, c_matrix, dt_raw.T, dt_bias[None, :], a_log[None, :],
      d_skip[None, :])
    grad_wx, grad_wbc, *rows = pl.pallas_call(
        finish_kernel,
        out_shape=(sds((block, width), F32), sds((64, block), F32)) + (sds((1, heads), F32),) * 3,
        name="finish",
        cost_estimate=pl.CostEstimate(flops=10**6, bytes_accessed=10**6, transcendentals=0),
    )(grad_wx, grad_wbc, totals)
    return (grad_wx, grad_wbc.T, *(row.reshape(heads) for row in rows))


def solution(mesh):
    n_seq, n_mp = mesh.shape["seq"], mesh.shape["mp"]
    split = Mesh(mesh.devices.reshape(n_seq // 8, 4, 2, n_mp), SEQ + ("mp",))
    in_specs = (
        P(SEQ, None),
        P(SEQ, "mp"),
        P(SEQ, None),
        P(SEQ, None),
        P(SEQ, "mp"),
        P("mp"),
        P("mp"),
        P("mp"),
        P(SEQ, "mp"),
    )
    out_specs = (P(SEQ, "mp"), P(SEQ, "mp"), P("mp"), P("mp"), P("mp"))
    return jax.shard_map(
        on_device, mesh=split, in_specs=in_specs, out_specs=out_specs, check_vma=False
    )
```
